8 devices in a mesh: fsdp: 8 (over z, y, x, core).
Axes of the slice: x: 2, y: 2, z: 1, core: 2. Of those that a mesh axis runs over, the one named last changes fastest.
Arguments:
- token_ids: int32 [128, 256], P('fsdp')
- grad_y: bfloat16 [128, 256, 960], P('fsdp')
- table: bfloat16 [49152, 960], P('fsdp')
- norm1_gain: bfloat16 [960], P('fsdp')
- norm2_gain: bfloat16 [960], P('fsdp')
- w_query: bfloat16 [960, 15, 64], P('fsdp')
- w_key: bfloat16 [960, 5, 64], P('fsdp')
- w_value: bfloat16 [960, 5, 64], P('fsdp')
- w_out: bfloat16 [960, 960], P('fsdp')
- w_gate: bfloat16 [960, 2560], P('fsdp')
- w_up: bfloat16 [960, 2560], P('fsdp')
- w_down: bfloat16 [2560, 960], P('fsdp')
Outputs:
- output 1: bfloat16 [128, 256, 960], P('fsdp')
- output 2: bfloat16 [49152, 960], P('fsdp')
- output 3: bfloat16 [960], P('fsdp')
- output 4: bfloat16 [960], P('fsdp')
- output 5: bfloat16 [960, 15, 64], P('fsdp')
- output 6: bfloat16 [960, 5, 64], P('fsdp')
- output 7: bfloat16 [960, 5, 64], P('fsdp')
- output 8: bfloat16 [960, 960], P('fsdp')
- output 9: bfloat16 [960, 2560], P('fsdp')
- output 10: bfloat16 [960, 2560], P('fsdp')
- output 11: bfloat16 [2560, 960], P('fsdp')
All inputs are finite; a program needn't handle non-finite values.
Results may differ from the reference program's by a relative error of at most 0.0162377.
Values are sent between devices in bfloat16 or wider.
A program may use at most 1 GiB of HBM per device.

```python
import jax
import jax.numpy as jnp
from jax import lax

VOCAB_SIZE = 49152
MODEL_DIM = 960
Q_HEADS = 15
KV_HEADS = 5
HEAD_DIM = 64
FFN_DIM = 2560
GLOBAL_BATCH = 128
SEQ_LEN = 256

NORM_EPS = 1e-5
ROPE_THETA = 500000.0
VOCAB_BITS = (VOCAB_SIZE - 1).bit_length()
TOKENS_ALL = GLOBAL_BATCH * SEQ_LEN


def draw_ids(rng_key):
    k_level, k_rank, k_flat, k_pick, k_perm = jax.random.split(rng_key, 5)
    id_shape = (GLOBAL_BATCH, SEQ_LEN)
    levels = jax.random.randint(k_level, id_shape, 0, VOCAB_BITS + 1)
    level_span = jnp.minimum(jnp.left_shift(jnp.ones(id_shape, jnp.int32), levels), VOCAB_SIZE)
    id_ranks = jax.random.randint(k_rank, id_shape, 0, level_span)
    flat_ids = jax.random.randint(k_flat, id_shape, 0, VOCAB_SIZE)
    use_flat = jax.random.randint(k_pick, id_shape, 0, 4) == 0
    id_ranks = jnp.where(use_flat, flat_ids, id_ranks)
    row_order = jax.random.permutation(k_perm, VOCAB_SIZE)
    return jnp.take(row_order, id_ranks).astype(jnp.int32)


def normal_weight(rng_key, w_shape, fan_in):
    return (jax.random.normal(rng_key, w_shape, jnp.float32) * fan_in ** -0.5).astype(jnp.bfloat16)


def setup_inputs(seed: int = 0) -> dict:
    keys = jax.random.split(jax.random.key(seed), 12)
    attn_width = Q_HEADS * HEAD_DIM
    return {
        "token_ids": draw_ids(keys[0]),
        "grad_y": (jax.random.normal(keys[1], (GLOBAL_BATCH, SEQ_LEN, MODEL_DIM), jnp.float32) * TOKENS_ALL ** -0.5).astype(jnp.bfloat16),
        "table": jax.random.normal(keys[2], (VOCAB_SIZE, MODEL_DIM), jnp.float32).astype(jnp.bfloat16),
        "norm1_gain": jax.random.uniform(keys[3], (MODEL_DIM,), jnp.float32, 0.5, 1.5).astype(jnp.bfloat16),
        "norm2_gain": jax.random.uniform(keys[4], (MODEL_DIM,), jnp.float32, 0.5, 1.5).astype(jnp.bfloat16),
        "w_query": normal_weight(keys[5], (MODEL_DIM, Q_HEADS, HEAD_DIM), MODEL_DIM),
        "w_key": normal_weight(keys[6], (MODEL_DIM, KV_HEADS, HEAD_DIM), MODEL_DIM),
        "w_value": normal_weight(keys[7], (MODEL_DIM, KV_HEADS, HEAD_DIM), MODEL_DIM),
        "w_out": normal_weight(keys[8], (attn_width, MODEL_DIM), attn_width),
        "w_gate": normal_weight(keys[9], (MODEL_DIM, FFN_DIM), MODEL_DIM),
        "w_up": normal_weight(keys[10], (MODEL_DIM, FFN_DIM), MODEL_DIM),
        "w_down": normal_weight(keys[11], (FFN_DIM, MODEL_DIM), FFN_DIM),
    }


def rms_norm(x_f32, gain_f32):
    inv_rms = lax.rsqrt(jnp.mean(x_f32 * x_f32, axis=-1, keepdims=True) + NORM_EPS)
    return (x_f32 * inv_rms * gain_f32).astype(jnp.bfloat16)


def rotary(x_f32):
    head_dim = x_f32.shape[-1]
    half_dim = head_dim // 2
    seq_len = x_f32.shape[-3]
    inv_freq = ROPE_THETA ** (-2.0 * jnp.arange(half_dim, dtype=jnp.float32) / head_dim)
    angles = jnp.arange(seq_len, dtype=jnp.float32)[:, None] * inv_freq[None, :]
    cos_tab = jnp.cos(angles)[:, None, :]
    sin_tab = jnp.sin(angles)[:, None, :]
    lo_half = x_f32[..., :half_dim]
    hi_half = x_f32[..., half_dim:]
    return jnp.concatenate([lo_half * cos_tab - hi_half * sin_tab, hi_half * cos_tab + lo_half * sin_tab], axis=-1)


def attend(q_f32, k_f32, v_bf16):
    q_rot = rotary(q_f32).astype(jnp.bfloat16).reshape(SEQ_LEN, KV_HEADS, Q_HEADS // KV_HEADS, HEAD_DIM)
    k_rot = rotary(k_f32).astype(jnp.bfloat16)
    scores = jnp.einsum("qkgd,skd->kgqs", q_rot.astype(jnp.float32), k_rot.astype(jnp.float32)) * HEAD_DIM ** -0.5
    positions = jnp.arange(SEQ_LEN)
    causal = positions[:, None] >= positions[None, :]
    scores = jnp.where(causal, scores, -1e30)
    prob_bf = jax.nn.softmax(scores, axis=-1).astype(jnp.bfloat16)
    attn_out = jnp.einsum("kgqs,skd->qkgd", prob_bf.astype(jnp.float32), v_bf16.astype(jnp.float32))
    return attn_out.astype(jnp.bfloat16).reshape(SEQ_LEN, Q_HEADS * HEAD_DIM)


def layer(emb_rows, gain_one, gain_two, w_query, w_key, w_value, w_out, w_gate, w_up, w_down):
    x_f32 = emb_rows.astype(jnp.float32)
    h_one = rms_norm(x_f32, gain_one).astype(jnp.float32)
    q_f32 = jnp.einsum("sd,dhe->she", h_one, w_query)
    k_f32 = jnp.einsum("sd,dhe->she", h_one, w_key)
    v_bf16 = jnp.einsum("sd,dhe->she", h_one, w_value).astype(jnp.bfloat16)
    attn_out = attend(q_f32, k_f32, v_bf16)
    resid_f32 = x_f32 + jnp.dot(attn_out.astype(jnp.float32), w_out, preferred_element_type=jnp.float32)
    resid_two = resid_f32.astype(jnp.bfloat16).astype(jnp.float32)
    h_two = rms_norm(resid_two, gain_two).astype(jnp.float32)
    gate_f32 = jnp.dot(h_two, w_gate, preferred_element_type=jnp.float32)
    up_f32 = jnp.dot(h_two, w_up, preferred_element_type=jnp.float32)
    act_f32 = (jax.nn.silu(gate_f32) * up_f32).astype(jnp.bfloat16).astype(jnp.float32)
    return (resid_two + jnp.dot(act_f32, w_down, preferred_element_type=jnp.float32)).astype(jnp.bfloat16)


def reference(token_ids, grad_y, table, norm1_gain, norm2_gain, w_query, w_key, w_value, w_out, w_gate, w_up, w_down):
    params = tuple(weight.astype(jnp.float32) for weight in (norm1_gain, norm2_gain, w_query, w_key, w_value, w_out, w_gate, w_up, w_down))

    def one_sequence(grad_acc, seq_in):
        seq_ids, seq_dy = seq_in
        emb_rows = jnp.take(table, seq_ids, axis=0)
        layer_out, pullback = jax.vjp(layer, emb_rows, *params)
        cotangents = pullback(seq_dy)
        new_acc = tuple(acc_old + cot_new for acc_old, cot_new in zip(grad_acc, cotangents[1:]))
        return new_acc, (layer_out, cotangents[0])

    zero_acc = tuple(jnp.zeros_like(weight) for weight in params)
    grad_acc, (y_out, d_emb) = lax.scan(one_sequence, zero_acc, (token_ids, grad_y))
    grad_table = jax.ops.segment_sum(d_emb.reshape(-1, MODEL_DIM).astype(jnp.float32), token_ids.reshape(-1), num_segments=VOCAB_SIZE).astype(jnp.bfloat16)
    grads = [acc_val.astype(jnp.bfloat16) for acc_val in grad_acc]
    return (y_out, grad_table, grads[0], grads[1], grads[2], grads[3], grads[4], grads[5], grads[6], grads[7], grads[8])
```

```python
import functools

import jax
import jax.numpy as jnp
from jax import lax
from jax.experimental import pallas as pl
from jax.experimental.pallas import tpu as pltpu
from jax.experimental.layout import Layout, with_layout_constraint
from jax.sharding import PartitionSpec as P


AXIS_NAME = "fsdp"
NORM_EPS = 1e-5
ROPE_THETA = 500000.0
N_DEV = 8
CAP = 384
N_SLOT = N_DEV * CAP
HEAD_DIM = 64
Q_HEADS = 15
KV_HEADS = 5
QK_COLS = (Q_HEADS + KV_HEADS) * HEAD_DIM
QKV_COLS = (Q_HEADS + 2 * KV_HEADS) * HEAD_DIM
PACK_COLS = 1664
LANES = 128
WIDE = 1024
VMEM_LIMIT = 60 * 1024 * 1024
BF = jnp.bfloat16
F32 = jnp.float32


def params(limit=VMEM_LIMIT):
    return pltpu.CompilerParams(vmem_limit_bytes=limit, dimension_semantics=("arbitrary",))


def route_kernel(rows_dev, me_ref, ids_ref, slot_ref, req_ref, col_a, col_b):
    n_tok = ids_ref.shape[1]
    me = me_ref[0]
    big = jnp.int32(2**30)

    def fill(col, row):
        for c in range(n_tok // LANES):
            part = jnp.broadcast_to(row[:, c * LANES:(c + 1) * LANES], (LANES, LANES))
            col[c * LANES:(c + 1) * LANES, :] = part.T

    ids = ids_ref[...]
    tok = lax.broadcasted_iota(jnp.int32, (1, n_tok), 1)
    fill(col_a, ids)
    width = 1024
    wide = (8, LANES)

    groups = width // LANES
    unroll = 4

    def sweep(n_out, n_rows, init, rows_of, step):
        outs = []
        for g in range(n_out // width):
            rows = [rows_of(g * width + c * LANES) for c in range(groups)]
            accs = tuple(jnp.full(wide, init, jnp.int32) for _ in range(groups))

            def body(i, accs, rows=rows):
                for u in range(unroll):
                    accs = step(i * unroll + u, accs, rows)
                return accs

            outs.extend(lax.fori_loop(0, n_rows(g) // (8 * unroll), body, accs))
        return outs

    def id_row(lane0):
        return jnp.broadcast_to(ids_ref[:, lane0:lane0 + LANES], wide)

    def block(i):
        return pl.ds(pl.multiple_of(i * 8, 8), 8)

    def first_step(i, accs, rows):
        col = col_a[block(i), :]
        pos = i * 8 + lax.broadcasted_iota(jnp.int32, wide, 0)
        return tuple(jnp.minimum(acc, jnp.where(col == row, pos, big)) for acc, row in zip(accs, rows))

    reps = sweep(n_tok, lambda g: (g + 1) * width, big, id_row, first_step)
    rep = jnp.concatenate([jnp.min(r, axis=0, keepdims=True) for r in reps], axis=1)
    first = rep == tok
    key = jnp.where(first, ids, big)
    fill(col_b, key)

    def rank_step(i, accs, rows):
        col = col_b[block(i), :]
        return tuple(acc + jnp.where(col < row, 1, 0) for acc, row in zip(accs, rows))

    ranks = sweep(n_tok, lambda g: n_tok, 0, id_row, rank_step)
    below = jnp.concatenate([jnp.sum(r, axis=0, keepdims=True) for r in ranks], axis=1)
    owner = jnp.zeros_like(ids)
    start = jnp.zeros_like(ids)
    prev = jnp.zeros((1, 1), jnp.int32)
    most = jnp.zeros((1, 1), jnp.int32)
    for o in range(1, N_DEV + 1):
        base = jnp.sum(jnp.where(key < o * rows_dev, 1, 0), axis=1, keepdims=True)
        most = jnp.maximum(most, base - prev)
        prev = base
        if o < N_DEV:
            past = ids >= o * rows_dev
            owner = jnp.where(past, o, owner)
            start = jnp.where(past, base, start)
    rank = below - start
    slot = (owner ^ me) * CAP + jnp.minimum(rank, CAP - 1)
    slot_ref[...] = slot
    fits = jnp.logical_and(first, rank < CAP)
    fill(col_b, jnp.where(fits, slot, -1))
    fill(col_a, ids - owner * rows_dev - rows_dev)

    def req_step(i, accs, rows):
        col, val = col_b[block(i), :], col_a[block(i), :]
        return tuple(acc + jnp.where(col == row, val, 0) for acc, row in zip(accs, rows))

    reqs = sweep(N_SLOT, lambda g: n_tok, 0, lambda lane0: lane0 + lax.broadcasted_iota(jnp.int32, wide, 1), req_step)
    req = jnp.concatenate([jnp.sum(r, axis=0, keepdims=True) for r in reqs], axis=1) + rows_dev
    for k in range(N_DEV):
        req_ref[k:k + 1, :CAP] = req[:, k * CAP:(k + 1) * CAP]
        req_ref[k:k + 1, CAP:] = jnp.broadcast_to(most, (1, LANES))


def route(ids, rows_dev):
    n_tok = ids.shape[0]
    me = lax.axis_index(AXIS_NAME).astype(jnp.int32).reshape(1)
    slot, req = pl.pallas_call(
        functools.partial(route_kernel, rows_dev),
        out_shape=(jax.ShapeDtypeStruct((1, n_tok), jnp.int32), jax.ShapeDtypeStruct((N_DEV, CAP + LANES), jnp.int32)),
        in_specs=[pl.BlockSpec(memory_space=pltpu.SMEM), pl.BlockSpec(memory_space=pltpu.VMEM)],
        out_specs=(pl.BlockSpec(memory_space=pltpu.VMEM), pl.BlockSpec(memory_space=pltpu.VMEM)),
        scratch_shapes=[pltpu.VMEM((n_tok, LANES), jnp.int32)] * 2,
        compiler_params=pltpu.CompilerParams(vmem_limit_bytes=16 * 1024 * 1024),
        name="route",
    )(me, ids.reshape(1, n_tok))
    return slot, req


def swap(parts):
    out = [parts[0]]
    for k in range(1, N_DEV):
        out.append(lax.ppermute(parts[k], AXIS_NAME, [(i, i ^ k) for i in range(N_DEV)]))
    return out


ROW_UNROLL = 16


def copy_rows(src, idx_ref, idx0, dst, n_rows):
    def body(i, carry):
        vals = []
        for u in range(ROW_UNROLL):
            vals.append(src[pl.ds(idx_ref[idx0 + i * ROW_UNROLL + u], 1), :])
        for u in range(ROW_UNROLL):
            dst[pl.ds(i * ROW_UNROLL + u, 1), :] = vals[u]
        return carry

    lax.fori_loop(0, n_rows // ROW_UNROLL, body, 0)


GATHER_CHUNK = 768


def pick_kernel(idx_ref, tab_ref, *refs):
    outs, wide, stage = refs[:N_DEV], refs[N_DEV], refs[N_DEV + 1]
    step = pl.program_id(0)
    n_load = wide.shape[0] // GATHER_CHUNK

    @pl.when(step < n_load)
    def _():
        at = pl.ds(pl.multiple_of(step * GATHER_CHUNK, 8), GATHER_CHUNK)
        dim = tab_ref.shape[0]
        for c in range(WIDE // LANES):
            part = tab_ref[c * LANES:min((c + 1) * LANES, dim), :].astype(F32)
            if part.shape[0] < LANES:
                part = jnp.concatenate([part, jnp.zeros((LANES - part.shape[0], GATHER_CHUNK), F32)], axis=0)
            wide[at, c * LANES:(c + 1) * LANES] = part.T

    for k in range(N_DEV):
        @pl.when(step == n_load + k)
        def _(k=k):
            copy_rows(wide, idx_ref, k * CAP, stage, CAP)
            outs[k][...] = stage[...].astype(BF)


def pick_rows(table, idx):
    rows_dev, dim = table.shape
    n_load = rows_dev // GATHER_CHUNK
    idx = jnp.minimum(idx.reshape(-1), rows_dev - 1)
    return pl.pallas_call(
        pick_kernel,
        grid_spec=pltpu.PrefetchScalarGridSpec(
            num_scalar_prefetch=1,
            grid=(n_load + N_DEV,),
            in_specs=[pl.BlockSpec((dim, GATHER_CHUNK), lambda s, _: (0, jnp.minimum(s, n_load - 1)))],
            out_specs=[pl.BlockSpec((CAP, WIDE), lambda s, _: (0, 0))] * N_DEV,
            scratch_shapes=[pltpu.VMEM((rows_dev, WIDE), F32), pltpu.VMEM((CAP, WIDE), F32)],
        ),
        out_shape=[jax.ShapeDtypeStruct((CAP, WIDE), BF)] * N_DEV,
        compiler_params=params(),
        cost_estimate=pl.CostEstimate(flops=10**9, bytes_accessed=2 * rows_dev * dim, transcendentals=0),
        name="pick_rows",
    )(idx, table.T)


EXPAND_ROWS = 512


def expand_kernel(idx_ref, gain_ref, *refs):
    parts, e_ref, h_ref, wide, stage = refs[:N_DEV], *refs[N_DEV:]
    step = pl.program_id(0)

    @pl.when(step == 0)
    def _():
        for k in range(N_DEV):
            wide[k * CAP:(k + 1) * CAP, :] = parts[k][...].astype(F32)

    copy_rows(wide, idx_ref, step * EXPAND_ROWS, stage, EXPAND_ROWS)
    x = stage[:, :e_ref.shape[1]]
    e_ref[...] = x.astype(BF)
    inv = lax.rsqrt(jnp.mean(x * x, axis=-1, keepdims=True) + NORM_EPS)
    h_ref[...] = (x * inv * gain_ref[...]).astype(BF)


def expand_rows(parts, slot, gain):
    n_tok, dim = slot.shape[0], gain.shape[0]
    return pl.pallas_call(
        expand_kernel,
        grid_spec=pltpu.PrefetchScalarGridSpec(
            num_scalar_prefetch=1,
            grid=(n_tok // EXPAND_ROWS,),
            in_specs=[pl.BlockSpec((1, dim), lambda s, _: (0, 0))] + [pl.BlockSpec((CAP, WIDE), lambda s, _: (0, 0))] * N_DEV,
            out_specs=[pl.BlockSpec((EXPAND_ROWS, dim), lambda s, _: (s, 0))] * 2,
            scratch_shapes=[pltpu.VMEM((N_SLOT, WIDE), F32), pltpu.VMEM((EXPAND_ROWS, WIDE), F32)],
        ),
        out_shape=[jax.ShapeDtypeStruct((n_tok, dim), BF)] * 2,
        compiler_params=params(),
        name="expand_rows",
    )(slot, gain.reshape(1, dim), *parts)


def fold_kernel(slot_ref, d_ref, out_ref):
    step = pl.program_id(0)
    block = out_ref.shape[0]
    n_tok = slot_ref.shape[1]
    total = None
    width = 1024
    for c in range(n_tok // width):
        ids = jnp.broadcast_to(slot_ref[:, c * width:(c + 1) * width], (block, width))
        mine = step * block + lax.broadcasted_iota(jnp.int32, (block, width), 0)
        hot = jnp.where(ids == mine, 1.0, 0.0).astype(BF)
        term = jnp.dot(hot, d_ref[c * width:(c + 1) * width, :], preferred_element_type=F32)
        total = term if total is None else total + term
    out_ref[:, :d_ref.shape[1]] = total
    out_ref[:, d_ref.shape[1]:] = jnp.zeros((block, WIDE - d_ref.shape[1]), F32)


def fold_rows(d_emb, slot):
    n_tok, dim = d_emb.shape
    block = CAP
    return pl.pallas_call(
        fold_kernel,
        grid=(N_SLOT // block,),
        in_specs=[pl.BlockSpec((1, n_tok), lambda s: (0, 0)), pl.BlockSpec((n_tok, dim), lambda s: (0, 0))],
        out_specs=pl.BlockSpec((block, WIDE), lambda s: (s, 0)),
        out_shape=jax.ShapeDtypeStruct((N_SLOT, WIDE), F32),
        compiler_params=params(),
        cost_estimate=pl.CostEstimate(flops=2 * N_SLOT * n_tok * dim, bytes_accessed=4 * N_SLOT * dim, transcendentals=0),
        name="fold_rows",
    )(slot, d_emb)


ADD_UNROLL = 8


def spread_kernel(rows_dev, idx_ref, *refs):
    parts, out_ref, total = refs[:N_DEV], refs[N_DEV], refs[N_DEV + 1]
    step = pl.program_id(0)
    n_out = rows_dev // GATHER_CHUNK

    @pl.when(step == 0)
    def _():
        total[...] = jnp.zeros_like(total)

    for k in range(N_DEV):
        @pl.when(step == k)
        def _(k=k):
            def body(i, carry):
                sums = []
                rows = [idx_ref[k * CAP + i * ADD_UNROLL + u] for u in range(ADD_UNROLL)]
                for u in range(ADD_UNROLL):
                    sums.append(total[pl.ds(rows[u], 1), :] + parts[k][pl.ds(i * ADD_UNROLL + u, 1), :])
                for u in range(ADD_UNROLL):
                    total[pl.ds(rows[u], 1), :] = sums[u]
                return carry

            lax.fori_loop(0, CAP // ADD_UNROLL, body, 0)

    @pl.when(step >= N_DEV)
    def _():
        at = pl.multiple_of((step - N_DEV) * GATHER_CHUNK, 8)
        dim = out_ref.shape[0]
        for c in range(WIDE // LANES):
            n_lane = min(LANES, dim - c * LANES)
            part = total[pl.ds(at, GATHER_CHUNK), c * LANES:(c + 1) * LANES].T
            out_ref[c * LANES:c * LANES + n_lane, :] = part[:n_lane].astype(BF)


def spread_rows(parts, idx, rows_dev, dim):
    n_out = rows_dev // GATHER_CHUNK
    return pl.pallas_call(
        functools.partial(spread_kernel, rows_dev),
        grid_spec=pltpu.PrefetchScalarGridSpec(
            num_scalar_prefetch=1,
            grid=(N_DEV + n_out,),
            in_specs=[pl.BlockSpec((CAP, WIDE), lambda s, _: (0, 0))] * N_DEV,
            out_specs=pl.BlockSpec((dim, GATHER_CHUNK), lambda s, _: (0, jnp.maximum(s - N_DEV, 0))),
            scratch_shapes=[pltpu.VMEM((rows_dev + 8, WIDE), F32)],
        ),
        out_shape=jax.ShapeDtypeStruct((dim, rows_dev), BF),
        compiler_params=params(),
        name="spread_rows",
    )(idx.reshape(-1), *parts).T


def rope_tables(seq_len):
    half = HEAD_DIM // 2
    inv_freq = ROPE_THETA ** (-2.0 * jnp.arange(half, dtype=F32) / HEAD_DIM)
    angles = jnp.arange(seq_len, dtype=F32)[:, None] * inv_freq[None, :]
    cos_tab, sin_tab = jnp.cos(angles), jnp.sin(angles)
    cos_all = jnp.concatenate([cos_tab] * 4, axis=1)
    sin_all = jnp.concatenate([-sin_tab, sin_tab] * 2, axis=1)
    return cos_all, sin_all


def turn(x, cos_all, sin_all, low):
    other = jnp.where(low, pltpu.roll(x, LANES - HEAD_DIM // 2, 1), pltpu.roll(x, HEAD_DIM // 2, 1))
    return x * cos_all + other * sin_all


def low_lanes(seq_len):
    lane = lax.broadcasted_iota(jnp.int32, (seq_len, LANES), 1)
    return lax.rem(lane, HEAD_DIM) < HEAD_DIM // 2


CONTRACT_LAST = (((1,), (1,)), ((), ()))
CONTRACT_FIRST = (((0,), (0,)), ((), ()))


def lanes_of(ref, at, first_head):
    return jnp.concatenate([ref[at, h * HEAD_DIM:(h + 1) * HEAD_DIM] for h in range(first_head, first_head + 3)], axis=0)


def hidden(half):
    key = lax.broadcasted_iota(jnp.int32, (half, 3 * half), 0)
    query = lax.rem(lax.broadcasted_iota(jnp.int32, (half, 3 * half), 1), half)
    return key > query


def dot_last(a, b):
    return lax.dot_general(a, b, CONTRACT_LAST, preferred_element_type=F32)


def dot_first(a, b):
    return lax.dot_general(a, b, CONTRACT_FIRST, preferred_element_type=F32)


def dot_mid(a, b):
    return jnp.dot(a, b, preferred_element_type=F32)


def probabilities(q_lo, q_hi, k, mask):
    half, n_lo = k.shape[0] // 2, q_lo.shape[0]
    s_all = dot_last(k[:half], jnp.concatenate([q_lo, q_hi], axis=0))
    s_a = jnp.where(mask, -1e30, s_all[:, :n_lo])
    s_b = s_all[:, n_lo:]
    s_c = jnp.where(mask, -1e30, dot_last(k[half:], q_hi))
    m_lo = jnp.max(s_a, axis=0, keepdims=True)
    m_hi = jnp.maximum(jnp.max(s_b, axis=0, keepdims=True), jnp.max(s_c, axis=0, keepdims=True))
    p_a, p_b, p_c = jnp.exp(s_a - m_lo), jnp.exp(s_b - m_hi), jnp.exp(s_c - m_hi)
    inv_lo = 1.0 / jnp.sum(p_a, axis=0, keepdims=True)
    inv_hi = 1.0 / (jnp.sum(p_b, axis=0, keepdims=True) + jnp.sum(p_c, axis=0, keepdims=True))
    return p_a * inv_lo, p_b * inv_hi, p_c * inv_hi


def attend_kernel(cos_ref, sin_ref, qkv_ref, rot_ref, out_ref):
    seq_len = qkv_ref.shape[0]
    low = low_lanes(seq_len)
    cos_all, sin_all = cos_ref[...], sin_ref[...]
    scale_q = Q_HEADS * HEAD_DIM
    for c in range(QK_COLS // LANES):
        x = turn(qkv_ref[:, c * LANES:(c + 1) * LANES], cos_all, sin_all, low)
        col = c * LANES + lax.broadcasted_iota(jnp.int32, x.shape, 1)
        if (c + 1) * LANES <= scale_q:
            x = x * HEAD_DIM ** -0.5
        elif c * LANES < scale_q:
            x = jnp.where(col < scale_q, x * HEAD_DIM ** -0.5, x)
        rot_ref[:, c * LANES:(c + 1) * LANES] = x.astype(BF)
    rot_ref[:, QK_COLS:] = qkv_ref[:, QK_COLS:].astype(BF)
    half = seq_len // 2
    lo, hi = slice(0, half), slice(half, seq_len)
    mask = hidden(half)
    for g in range(KV_HEADS):
        k0, v0 = scale_q + g * HEAD_DIM, QK_COLS + g * HEAD_DIM
        k = rot_ref[:, k0:k0 + HEAD_DIM]
        v = rot_ref[:, v0:v0 + HEAD_DIM]
        p_a, p_b, p_c = probabilities(lanes_of(rot_ref, lo, 3 * g), lanes_of(rot_ref, hi, 3 * g), k, mask)
        o_lo = dot_first(p_a.astype(BF), v[lo]).astype(BF)
        o_hi = dot_first(jnp.concatenate([p_b.astype(BF), p_c.astype(BF)], axis=0), v).astype(BF)
        for j in range(3):
            h = 3 * g + j
            out_ref[lo, h * HEAD_DIM:(h + 1) * HEAD_DIM] = o_lo[j * half:(j + 1) * half]
            out_ref[hi, h * HEAD_DIM:(h + 1) * HEAD_DIM] = o_hi[j * half:(j + 1) * half]


def attend(qkv, seq_len, tables):
    n_tok = qkv.shape[0]
    width = Q_HEADS * HEAD_DIM
    return pl.pallas_call(
        attend_kernel,
        grid=(n_tok // seq_len,),
        in_specs=[pl.BlockSpec((seq_len, LANES), lambda s: (0, 0))] * 2 + [pl.BlockSpec((seq_len, QKV_COLS), lambda s: (s, 0))],
        out_specs=[pl.BlockSpec((seq_len, QKV_COLS), lambda s: (s, 0)), pl.BlockSpec((seq_len, width), lambda s: (s, 0))],
        out_shape=[jax.ShapeDtypeStruct((n_tok, QKV_COLS), BF), jax.ShapeDtypeStruct((n_tok, width), BF)],
        compiler_params=params(32 * 1024 * 1024),
        cost_estimate=pl.CostEstimate(flops=4 * n_tok * seq_len * width, bytes_accessed=12 * n_tok * width, transcendentals=n_tok * seq_len * Q_HEADS),
        name="attend",
    )(*tables, qkv)


def attend_back_kernel(cos_ref, sin_ref, rot_ref, d_ref, out_ref, d_rot):
    seq_len = rot_ref.shape[0]
    scale_q = Q_HEADS * HEAD_DIM
    half = seq_len // 2
    lo, hi = slice(0, half), slice(half, seq_len)
    mask = hidden(half)
    for g in range(KV_HEADS):
        k0, v0 = scale_q + g * HEAD_DIM, QK_COLS + g * HEAD_DIM
        k = rot_ref[:, k0:k0 + HEAD_DIM]
        v = rot_ref[:, v0:v0 + HEAD_DIM]
        q_lo, q_hi = lanes_of(rot_ref, lo, 3 * g), lanes_of(rot_ref, hi, 3 * g)
        d_lo, d_hi = lanes_of(d_ref, lo, 3 * g), lanes_of(d_ref, hi, 3 * g)
        n_lo = q_lo.shape[0]
        p_a, p_b, p_c = probabilities(q_lo, q_hi, k, mask)
        d_all = jnp.concatenate([d_lo, d_hi], axis=0)
        dp_all = dot_last(v[lo], d_all).astype(BF).astype(F32)
        dp_c = dot_last(v[hi], d_hi).astype(BF).astype(F32)
        p_lo = jnp.concatenate([p_a.astype(BF), p_b.astype(BF)], axis=1)
        out_ref[lo, v0:v0 + HEAD_DIM] = dot_mid(p_lo, d_all).astype(BF)
        out_ref[hi, v0:v0 + HEAD_DIM] = dot_mid(p_c.astype(BF), d_hi).astype(BF)
        pd_a, pd_b, pd_c = p_a * dp_all[:, :n_lo], p_b * dp_all[:, n_lo:], p_c * dp_c
        t_lo = jnp.sum(pd_a, axis=0, keepdims=True)
        t_hi = jnp.sum(pd_b, axis=0, keepdims=True) + jnp.sum(pd_c, axis=0, keepdims=True)
        ds_a = (pd_a - p_a * t_lo).astype(BF)
        ds_b = (pd_b - p_b * t_hi).astype(BF)
        ds_c = (pd_c - p_c * t_hi).astype(BF)
        q_all = jnp.concatenate([q_lo, q_hi], axis=0)
        ds_all = jnp.concatenate([ds_a, ds_b], axis=1)
        d_rot[lo, k0:k0 + HEAD_DIM] = dot_mid(ds_all, q_all).astype(BF).astype(F32)
        d_rot[hi, k0:k0 + HEAD_DIM] = dot_mid(ds_c, q_hi).astype(BF).astype(F32)
        scale = HEAD_DIM ** -0.5
        dq_lo = (dot_first(ds_a, k[lo]) * scale).astype(BF).astype(F32)
        dq_hi = (dot_first(jnp.concatenate([ds_b, ds_c], axis=0), k) * scale).astype(BF).astype(F32)
        for j in range(3):
            h = 3 * g + j
            d_rot[lo, h * HEAD_DIM:(h + 1) * HEAD_DIM] = dq_lo[j * half:(j + 1) * half]
            d_rot[hi, h * HEAD_DIM:(h + 1) * HEAD_DIM] = dq_hi[j * half:(j + 1) * half]
    low = low_lanes(seq_len)
    cos_all, sin_all = cos_ref[...], -sin_ref[...]
    for c in range(QK_COLS // LANES):
        at = slice(c * LANES, (c + 1) * LANES)
        out_ref[:, at] = turn(d_rot[:, at], cos_all, sin_all, low).astype(BF)


def attend_back(rot, d_attn, seq_len, tables):
    n_tok = rot.shape[0]
    width = Q_HEADS * HEAD_DIM
    return pl.pallas_call(
        attend_back_kernel,
        grid=(n_tok // seq_len,),
        in_specs=[pl.BlockSpec((seq_len, LANES), lambda s: (0, 0))] * 2
        + [pl.BlockSpec((seq_len, QKV_COLS), lambda s: (s, 0)), pl.BlockSpec((seq_len, width), lambda s: (s, 0))],
        out_specs=pl.BlockSpec((seq_len, QKV_COLS), lambda s: (s, 0)),
        out_shape=jax.ShapeDtypeStruct((n_tok, QKV_COLS), BF),
        scratch_shapes=[pltpu.VMEM((seq_len, QK_COLS), F32)],
        compiler_params=params(32 * 1024 * 1024),
        cost_estimate=pl.CostEstimate(flops=10 * n_tok * seq_len * width, bytes_accessed=9 * n_tok * width, transcendentals=n_tok * seq_len * Q_HEADS),
        name="attend_back",
    )(*tables, rot, d_attn)


def rms_norm(x_f32, gain_f32):
    inv_rms = lax.rsqrt(jnp.mean(x_f32 * x_f32, axis=-1, keepdims=True) + NORM_EPS)
    return (x_f32 * inv_rms * gain_f32).astype(BF)


def gated(gate_f32, up_f32):
    return (jax.nn.silu(gate_f32) * up_f32).astype(BF)


def mm(a, b):
    return jnp.einsum("bsd,df->bsf", a, b, preferred_element_type=F32)


def mm_t(a, b):
    return jnp.einsum("bsf,df->bsd", a, b, preferred_element_type=F32)


def mm_w(a, b):
    return jnp.einsum("bsd,bsf->df", a, b, preferred_element_type=F32)


def row_major(x):
    return with_layout_constraint(x, Layout(major_to_minor=(0, 1)))


def from_peer(x, k):
    return lax.ppermute(x, AXIS_NAME, [(i, i ^ k) for i in range(N_DEV)]) if k else x


def owned_ids(token_ids, rows_dev, k):
    rel_ids = from_peer(token_ids, k).reshape(-1) - lax.axis_index(AXIS_NAME) * rows_dev
    return rel_ids, (rel_ids >= 0) & (rel_ids < rows_dev)


def slow_rows(token_ids, table):
    total = None
    for k in range(N_DEV):
        rel_ids, owned = owned_ids(token_ids, table.shape[0], k)
        picked = jnp.take(table, jnp.where(owned, rel_ids, 0), axis=0)
        part = from_peer(jnp.where(owned[:, None], picked, jnp.zeros((), BF)), k)
        total = part if total is None else total + part
    return total


def slow_grad(token_ids, d_emb, rows_dev):
    total = None
    for k in range(N_DEV):
        rel_ids, owned = owned_ids(token_ids, rows_dev, k)
        d_all = from_peer(d_emb, k).astype(F32)
        seg_ids = jnp.where(owned, rel_ids, rows_dev)
        part = jax.ops.segment_sum(d_all, seg_ids, num_segments=rows_dev)
        total = part if total is None else total + part
    return total.astype(BF)


def gather_all(shard):
    return lax.all_gather(shard, AXIS_NAME, axis=0, tiled=True)


def scatter_sum(partial):
    return lax.psum_scatter(partial, AXIS_NAME, scatter_dimension=0, tiled=True)


def solution(mesh):
    spec_1d = P(AXIS_NAME)
    spec_2d = P(AXIS_NAME, None)
    spec_3d = P(AXIS_NAME, None, None)
    in_specs = (spec_2d, spec_3d, spec_2d, spec_1d, spec_1d, spec_3d, spec_3d, spec_3d, spec_2d, spec_2d, spec_2d, spec_2d)
    out_specs = (spec_3d, spec_2d, spec_1d, spec_1d, spec_3d, spec_3d, spec_3d, spec_2d, spec_2d, spec_2d, spec_2d)

    def device_step(token_ids, grad_y, table, g_one, g_two, w_query, w_key, w_value, w_out, w_gate, w_up, w_down):
        rows_dev, dim = table.shape
        batch, seq_len = token_ids.shape
        n_tok = batch * seq_len
        rows_w = w_query.shape[0]

        pad = jnp.zeros((rows_w, PACK_COLS - QKV_COLS - 2), BF)
        shards = [w.reshape(rows_w, -1) for w in (w_query, w_key, w_value)]
        pack = jnp.concatenate(shards + [g_one[:, None], g_two[:, None], pad], axis=1)
        full_down = gather_all(w_down)
        full_pack = gather_all(pack)
        full_out = gather_all(w_out)
        full_gate = gather_all(w_gate)
        full_up = gather_all(w_up)
        w_qkv = full_pack[:, :QKV_COLS]
        gain_one = full_pack[:, QKV_COLS].astype(F32)
        gain_two = full_pack[:, QKV_COLS + 1].astype(F32)

        slot, req = route(token_ids.reshape(n_tok), rows_dev)
        asked = swap([req[k:k + 1] for k in range(N_DEV)])
        asked = jnp.concatenate(asked, axis=0)
        overflow = jnp.max(asked[:, CAP]) > CAP
        asked = asked[:, :CAP]
        parts = swap(pick_rows(table, asked))
        emb, h_one = expand_rows(parts, slot.reshape(n_tok), gain_one)

        def slow_start():
            rows = slow_rows(token_ids, table)
            return rows, rms_norm(rows.astype(F32), gain_one)

        emb, h_one = lax.cond(overflow, slow_start, lambda: (emb, h_one))
        emb, h_one = row_major(emb), row_major(h_one)

        tables = rope_tables(seq_len)
        cube = (batch, seq_len, -1)
        d_act = mm_t(grad_y, full_down).astype(BF)
        h_one = h_one.reshape(cube)
        x_f32 = emb.reshape(cube).astype(F32)
        qkv = mm(h_one, w_qkv)
        rot, attn = attend(qkv.reshape(n_tok, -1), seq_len, tables)
        attn = attn.reshape(cube)
        resid = (x_f32 + mm(attn, full_out)).astype(BF)
        resid_f32 = resid.astype(F32)
        h_two, norm2_pull = jax.vjp(rms_norm, resid_f32, gain_two)
        gate_f32 = mm(h_two, full_gate)
        up_f32 = mm(h_two, full_up)
        act, act_pull = jax.vjp(gated, gate_f32, up_f32)
        y_out = (resid_f32 + mm(act, full_down)).astype(BF)

        g_down = mm_w(act, grad_y)
        d_gate, d_up = act_pull(d_act)
        d_gate, d_up = d_gate.astype(BF), d_up.astype(BF)
        d_gate, d_up, g_down, y_out = lax.optimization_barrier((d_gate, d_up, g_down, y_out))
        sum_down = scatter_sum(g_down)
        g_gate, g_up = mm_w(h_two, d_gate), mm_w(h_two, d_up)
        d_gate, d_up, g_gate, g_up = lax.optimization_barrier((d_gate, d_up, g_gate, g_up))
        sum_gate, sum_up = scatter_sum(g_gate), scatter_sum(g_up)
        d_h_two = (mm_t(d_gate, full_gate) + mm_t(d_up, full_up)).astype(BF)
        d_resid_two, d_gain_two = norm2_pull(d_h_two)
        d_resid = (grad_y.astype(F32) + d_resid_two).astype(BF)
        g_out = mm_w(attn, d_resid)
        d_attn = mm_t(d_resid, full_out).astype(BF).reshape(n_tok, -1)
        d_attn, g_out, sum_down = lax.optimization_barrier((d_attn, g_out, sum_down))
        sum_out = scatter_sum(g_out)
        d_qkv = attend_back(rot, row_major(d_attn), seq_len, tables).reshape(cube)
        d_qkv, sum_gate, sum_up = lax.optimization_barrier((d_qkv, sum_gate, sum_up))
        d_h_one = mm_t(d_qkv, w_qkv).astype(BF)
        _, norm1_pull = jax.vjp(rms_norm, x_f32, gain_one)
        d_x, d_gain_one = norm1_pull(d_h_one)
        d_emb = (d_resid.astype(F32) + d_x).astype(BF).reshape(n_tok, dim)

        d_emb, sum_out = lax.optimization_barrier((d_emb, sum_out))
        folded = fold_rows(d_emb, slot)
        sent = swap([folded[k * CAP:(k + 1) * CAP] for k in range(N_DEV)])
        g_pad = jnp.zeros((dim, PACK_COLS - QKV_COLS - 2), F32)
        sum_pack = scatter_sum(jnp.concatenate([mm_w(h_one, d_qkv), d_gain_one[:, None], d_gain_two[:, None], g_pad], axis=1)).astype(BF)
        d_table = spread_rows(sent, asked, rows_dev, dim)
        d_table, sum_pack, sum_out, sum_gate, sum_up, sum_down = lax.optimization_barrier(
            (d_table, sum_pack, sum_out, sum_gate, sum_up, sum_down))
        d_table = lax.cond(overflow, lambda: slow_grad(token_ids, d_emb, rows_dev), lambda: d_table)

        cols = [0, Q_HEADS * HEAD_DIM, QK_COLS, QKV_COLS]
        d_w = [sum_pack[:, a:b].reshape(rows_w, -1, HEAD_DIM) for a, b in zip(cols[:-1], cols[1:])]
        return (
            y_out, d_table, sum_pack[:, QKV_COLS], sum_pack[:, QKV_COLS + 1],
            d_w[0], d_w[1], d_w[2], sum_out.astype(BF), sum_gate.astype(BF), sum_up.astype(BF), sum_down.astype(BF),
        )

    return jax.shard_map(device_step, mesh=mesh, in_specs=in_specs, out_specs=out_specs, check_vma=False)
```

```python
import functools

import jax
import jax.numpy as jnp
from jax import lax
from jax.experimental import pallas as pl
from jax.experimental.pallas import tpu as pltpu
from jax.experimental.layout import Layout, with_layout_constraint
from jax.sharding import PartitionSpec as P


AXIS_NAME = "fsdp"
NORM_EPS = 1e-5
ROPE_THETA = 500000.0
N_DEV = 8
CAP = 384
N_SLOT = N_DEV * CAP
HEAD_DIM = 64
Q_HEADS = 15
KV_HEADS = 5
QK_COLS = (Q_HEADS + KV_HEADS) * HEAD_DIM
QKV_COLS = (Q_HEADS + 2 * KV_HEADS) * HEAD_DIM
PACK_COLS = 1664
LANES = 128
WIDE = 1024
VMEM_LIMIT = 60 * 1024 * 1024
BF = jnp.bfloat16
F32 = jnp.float32


def params(limit=VMEM_LIMIT):
    return pltpu.CompilerParams(vmem_limit_bytes=limit, dimension_semantics=("arbitrary",))


def route_kernel(rows_dev, me_ref, ids_ref, slot_ref, req_ref, col_a, col_b):
    n_tok = ids_ref.shape[1]
    me = me_ref[0]
    big = jnp.int32(2**30)

    def fill(col, row):
        for c in range(n_tok // LANES):
            part = jnp.broadcast_to(row[:, c * LANES:(c + 1) * LANES], (LANES, LANES))
            col[c * LANES:(c + 1) * LANES, :] = part.T

    ids = ids_ref[...]
    tok = lax.broadcasted_iota(jnp.int32, (1, n_tok), 1)
    fill(col_a, ids)
    width = 1024
    wide = (8, LANES)

    groups = width // LANES
    unroll = 4

    def sweep(n_out, n_rows, init, rows_of, step):
        outs = []
        for g in range(n_out // width):
            rows = [rows_of(g * width + c * LANES) for c in range(groups)]
            accs = tuple(jnp.full(wide, init, jnp.int32) for _ in range(groups))

            def body(i, accs, rows=rows):
                for u in range(unroll):
                    accs = step(i * unroll + u, accs, rows)
                return accs

            outs.extend(lax.fori_loop(0, n_rows(g) // (8 * unroll), body, accs))
        return outs

    def id_row(lane0):
        return jnp.broadcast_to(ids_ref[:, lane0:lane0 + LANES], wide)

    def block(i):
        return pl.ds(pl.multiple_of(i * 8, 8), 8)

    def first_step(i, accs, rows):
        col = col_a[block(i), :]
        pos = i * 8 + lax.broadcasted_iota(jnp.int32, wide, 0)
        return tuple(jnp.minimum(acc, jnp.where(col == row, pos, big)) for acc, row in zip(accs, rows))

    reps = sweep(n_tok, lambda g: (g + 1) * width, big, id_row, first_step)
    rep = jnp.concatenate([jnp.min(r, axis=0, keepdims=True) for r in reps], axis=1)
    first = rep == tok
    key = jnp.where(first, ids, big)
    fill(col_b, key)

    def rank_step(i, accs, rows):
        col = col_b[block(i), :]
        return tuple(acc + jnp.where(col < row, 1, 0) for acc, row in zip(accs, rows))

    ranks = sweep(n_tok, lambda g: n_tok, 0, id_row, rank_step)
    below = jnp.concatenate([jnp.sum(r, axis=0, keepdims=True) for r in ranks], axis=1)
    owner = jnp.zeros_like(ids)
    start = jnp.zeros_like(ids)
    prev = jnp.zeros((1, 1), jnp.int32)
    most = jnp.zeros((1, 1), jnp.int32)
    for o in range(1, N_DEV + 1):
        base = jnp.sum(jnp.where(key < o * rows_dev, 1, 0), axis=1, keepdims=True)
        most = jnp.maximum(most, base - prev)
        prev = base
        if o < N_DEV:
            past = ids >= o * rows_dev
            owner = jnp.where(past, o, owner)
            start = jnp.where(past, base, start)
    rank = below - start
    slot = (owner ^ me) * CAP + jnp.minimum(rank, CAP - 1)
    slot_ref[...] = slot
    fits = jnp.logical_and(first, rank < CAP)
    fill(col_b, jnp.where(fits, slot, -1))
    fill(col_a, ids - owner * rows_dev - rows_dev)

    def req_step(i, accs, rows):
        col, val = col_b[block(i), :], col_a[block(i), :]
        return tuple(acc + jnp.where(col == row, val, 0) for acc, row in zip(accs, rows))

    reqs = sweep(N_SLOT, lambda g: n_tok, 0, lambda lane0: lane0 + lax.broadcasted_iota(jnp.int32, wide, 1), req_step)
    req = jnp.concatenate([jnp.sum(r, axis=0, keepdims=True) for r in reqs], axis=1) + rows_dev
    for k in range(N_DEV):
        req_ref[k:k + 1, :CAP] = req[:, k * CAP:(k + 1) * CAP]
        req_ref[k:k + 1, CAP:] = jnp.broadcast_to(most, (1, LANES))


def route(ids, rows_dev):
    n_tok = ids.shape[0]
    me = lax.axis_index(AXIS_NAME).astype(jnp.int32).reshape(1)
    slot, req = pl.pallas_call(
        functools.partial(route_kernel, rows_dev),
        out_shape=(jax.ShapeDtypeStruct((1, n_tok), jnp.int32), jax.ShapeDtypeStruct((N_DEV, CAP + LANES), jnp.int32)),
        in_specs=[pl.BlockSpec(memory_space=pltpu.SMEM), pl.BlockSpec(memory_space=pltpu.VMEM)],
        out_specs=(pl.BlockSpec(memory_space=pltpu.VMEM), pl.BlockSpec(memory_space=pltpu.VMEM)),
        scratch_shapes=[pltpu.VMEM((n_tok, LANES), jnp.int32)] * 2,
        compiler_params=pltpu.CompilerParams(vmem_limit_bytes=16 * 1024 * 1024),
        name="route",
    )(me, ids.reshape(1, n_tok))
    return slot, req


def swap(parts):
    out = [parts[0]]
    for k in range(1, N_DEV):
        out.append(lax.ppermute(parts[k], AXIS_NAME, [(i, i ^ k) for i in range(N_DEV)]))
    return out


ROW_UNROLL = 16


def copy_rows(src, idx_ref, idx0, dst, n_rows):
    def body(i, carry):
        vals = []
        for u in range(ROW_UNROLL):
            vals.append(src[pl.ds(idx_ref[idx0 + i * ROW_UNROLL + u], 1), :])
        for u in range(ROW_UNROLL):
            dst[pl.ds(i * ROW_UNROLL + u, 1), :] = vals[u]
        return carry

    lax.fori_loop(0, n_rows // ROW_UNROLL, body, 0)


GATHER_CHUNK = 768


def pick_kernel(idx_ref, tab_ref, *refs):
    outs, wide, stage = refs[:N_DEV], refs[N_DEV], refs[N_DEV + 1]
    step = pl.program_id(0)
    n_load = wide.shape[0] // GATHER_CHUNK

    @pl.when(step < n_load)
    def _():
        at = pl.ds(pl.multiple_of(step * GATHER_CHUNK, 8), GATHER_CHUNK)
        dim = tab_ref.shape[0]
        for c in range(WIDE // LANES):
            part = tab_ref[c * LANES:min((c + 1) * LANES, dim), :].astype(F32)
            if part.shape[0] < LANES:
                part = jnp.concatenate([part, jnp.zeros((LANES - part.shape[0], GATHER_CHUNK), F32)], axis=0)
            wide[at, c * LANES:(c + 1) * LANES] = part.T

    for k in range(N_DEV):
        @pl.when(step == n_load + k)
        def _(k=k):
            copy_rows(wide, idx_ref, k * CAP, stage, CAP)
            outs[k][...] = stage[...].astype(BF)


def pick_rows(table, idx):
    rows_dev, dim = table.shape
    n_load = rows_dev // GATHER_CHUNK
    idx = jnp.minimum(idx.reshape(-1), rows_dev - 1)
    return pl.pallas_call(
        pick_kernel,
        grid_spec=pltpu.PrefetchScalarGridSpec(
            num_scalar_prefetch=1,
            grid=(n_load + N_DEV,),
            in_specs=[pl.BlockSpec((dim, GATHER_CHUNK), lambda s, _: (0, jnp.minimum(s, n_load - 1)))],
            out_specs=[pl.BlockSpec((CAP, WIDE), lambda s, _: (0, 0))] * N_DEV,
            scratch_shapes=[pltpu.VMEM((rows_dev, WIDE), F32), pltpu.VMEM((CAP, WIDE), F32)],
        ),
        out_shape=[jax.ShapeDtypeStruct((CAP, WIDE), BF)] * N_DEV,
        compiler_params=params(),
        cost_estimate=pl.CostEstimate(flops=10**9, bytes_accessed=2 * rows_dev * dim, transcendentals=0),
        name="pick_rows",
    )(idx, table.T)


EXPAND_ROWS = 512


def expand_kernel(idx_ref, gain_ref, *refs):
    parts, e_ref, h_ref, wide, stage = refs[:N_DEV], *refs[N_DEV:]
    step = pl.program_id(0)

    @pl.when(step == 0)
    def _():
        for k in range(N_DEV):
            wide[k * CAP:(k + 1) * CAP, :] = parts[k][...].astype(F32)

    copy_rows(wide, idx_ref, step * EXPAND_ROWS, stage, EXPAND_ROWS)
    x = stage[:, :e_ref.shape[1]]
    e_ref[...] = x.astype(BF)
    inv = lax.rsqrt(jnp.mean(x * x, axis=-1, keepdims=True) + NORM_EPS)
    h_ref[...] = (x * inv * gain_ref[...]).astype(BF)


def expand_rows(parts, slot, gain):
    n_tok, dim = slot.shape[0], gain.shape[0]
    return pl.pallas_call(
        expand_kernel,
        grid_spec=pltpu.PrefetchScalarGridSpec(
            num_scalar_prefetch=1,
            grid=(n_tok // EXPAND_ROWS,),
            in_specs=[pl.BlockSpec((1, dim), lambda s, _: (0, 0))] + [pl.BlockSpec((CAP, WIDE), lambda s, _: (0, 0))] * N_DEV,
            out_specs=[pl.BlockSpec((EXPAND_ROWS, dim), lambda s, _: (s, 0))] * 2,
            scratch_shapes=[pltpu.VMEM((N_SLOT, WIDE), F32), pltpu.VMEM((EXPAND_ROWS, WIDE), F32)],
        ),
        out_shape=[jax.ShapeDtypeStruct((n_tok, dim), BF)] * 2,
        compiler_params=params(),
        name="expand_rows",
    )(slot, gain.reshape(1, dim), *parts)


def fold_kernel(group, slot_ref, d_ref, *outs):
    n_tok, dim = d_ref.shape
    width = 1024
    for j, k in enumerate(group):
        @pl.when(pl.program_id(0) == j)
        def _(j=j, k=k):
            total = None
            for c in range(n_tok // width):
                ids = jnp.broadcast_to(slot_ref[:, c * width:(c + 1) * width], (CAP, width))
                mine = k * CAP + lax.broadcasted_iota(jnp.int32, (CAP, width), 0)
                hot = jnp.where(ids == mine, 1.0, 0.0).astype(BF)
                term = jnp.dot(hot, d_ref[c * width:(c + 1) * width, :], preferred_element_type=F32)
                total = term if total is None else total + term
            outs[j][:, :dim] = total
            outs[j][:, dim:] = jnp.zeros((CAP, WIDE - dim), F32)


def fold_rows(d_emb, slot, group):
    n_tok, dim = d_emb.shape
    n = len(group)
    return pl.pallas_call(
        functools.partial(fold_kernel, group),
        grid=(n,),
        in_specs=[pl.BlockSpec((1, n_tok), lambda s: (0, 0)), pl.BlockSpec((n_tok, dim), lambda s: (0, 0))],
        out_specs=[pl.BlockSpec((CAP, WIDE), lambda s: (0, 0))] * n,
        out_shape=[jax.ShapeDtypeStruct((CAP, WIDE), F32)] * n,
        compiler_params=params(),
        cost_estimate=pl.CostEstimate(flops=2 * n * CAP * n_tok * dim, bytes_accessed=4 * n * CAP * dim, transcendentals=0),
        name="fold_rows",
    )(slot, d_emb)


FAR, NEAR = (6, 7, 2, 4), (3, 5, 1, 0)
ADD_UNROLL = 8


def spread_kernel(rows_dev, idx_ref, *refs):
    parts, out_ref, total = refs[:N_DEV], refs[N_DEV], refs[N_DEV + 1]
    step = pl.program_id(0)
    n_out = rows_dev // GATHER_CHUNK

    @pl.when(step == 0)
    def _():
        total[...] = jnp.zeros_like(total)

    for k in range(N_DEV):
        @pl.when(step == k)
        def _(k=k):
            def body(i, carry):
                sums = []
                rows = [idx_ref[k * CAP + i * ADD_UNROLL + u] for u in range(ADD_UNROLL)]
                for u in range(ADD_UNROLL):
                    sums.append(total[pl.ds(rows[u], 1), :] + parts[k][pl.ds(i * ADD_UNROLL + u, 1), :])
                for u in range(ADD_UNROLL):
                    total[pl.ds(rows[u], 1), :] = sums[u]
                return carry

            lax.fori_loop(0, CAP // ADD_UNROLL, body, 0)

    @pl.when(step >= N_DEV)
    def _():
        at = pl.multiple_of((step - N_DEV) * GATHER_CHUNK, 8)
        dim = out_ref.shape[0]
        for c in range(WIDE // LANES):
            n_lane = min(LANES, dim - c * LANES)
            part = total[pl.ds(at, GATHER_CHUNK), c * LANES:(c + 1) * LANES].T
            out_ref[c * LANES:c * LANES + n_lane, :] = part[:n_lane].astype(BF)


def spread_rows(parts, idx, rows_dev, dim):
    n_out = rows_dev // GATHER_CHUNK
    return pl.pallas_call(
        functools.partial(spread_kernel, rows_dev),
        grid_spec=pltpu.PrefetchScalarGridSpec(
            num_scalar_prefetch=1,
            grid=(N_DEV + n_out,),
            in_specs=[pl.BlockSpec((CAP, WIDE), lambda s, _: (0, 0))] * N_DEV,
            out_specs=pl.BlockSpec((dim, GATHER_CHUNK), lambda s, _: (0, jnp.maximum(s - N_DEV, 0))),
            scratch_shapes=[pltpu.VMEM((rows_dev + 8, WIDE), F32)],
        ),
        out_shape=jax.ShapeDtypeStruct((dim, rows_dev), BF),
        compiler_params=params(),
        name="spread_rows",
    )(idx.reshape(-1), *parts).T


def rope_tables(seq_len):
    half = HEAD_DIM // 2
    inv_freq = ROPE_THETA ** (-2.0 * jnp.arange(half, dtype=F32) / HEAD_DIM)
    angles = jnp.arange(seq_len, dtype=F32)[:, None] * inv_freq[None, :]
    cos_tab, sin_tab = jnp.cos(angles), jnp.sin(angles)
    cos_all = jnp.concatenate([cos_tab] * 4, axis=1)
    sin_all = jnp.concatenate([-sin_tab, sin_tab] * 2, axis=1)
    return cos_all, sin_all


def turn(x, cos_all, sin_all, low):
    other = jnp.where(low, pltpu.roll(x, LANES - HEAD_DIM // 2, 1), pltpu.roll(x, HEAD_DIM // 2, 1))
    return x * cos_all + other * sin_all


def low_lanes(seq_len):
    lane = lax.broadcasted_iota(jnp.int32, (seq_len, LANES), 1)
    return lax.rem(lane, HEAD_DIM) < HEAD_DIM // 2


CONTRACT_LAST = (((1,), (1,)), ((), ()))
CONTRACT_FIRST = (((0,), (0,)), ((), ()))


def lanes_of(ref, at, first_head):
    return jnp.concatenate([ref[at, h * HEAD_DIM:(h + 1) * HEAD_DIM] for h in range(first_head, first_head + 3)], axis=0)


def hidden(half):
    key = lax.broadcasted_iota(jnp.int32, (half, 3 * half), 0)
    query = lax.rem(lax.broadcasted_iota(jnp.int32, (half, 3 * half), 1), half)
    return key > query


def dot_last(a, b):
    return lax.dot_general(a, b, CONTRACT_LAST, preferred_element_type=F32)


def dot_first(a, b):
    return lax.dot_general(a, b, CONTRACT_FIRST, preferred_element_type=F32)


def dot_mid(a, b):
    return jnp.dot(a, b, preferred_element_type=F32)


def probabilities(q_lo, q_hi, k, mask):
    half, n_lo = k.shape[0] // 2, q_lo.shape[0]
    s_all = dot_last(k[:half], jnp.concatenate([q_lo, q_hi], axis=0))
    s_a = jnp.where(mask, -1e30, s_all[:, :n_lo])
    s_b = s_all[:, n_lo:]
    s_c = jnp.where(mask, -1e30, dot_last(k[half:], q_hi))
    m_lo = jnp.max(s_a, axis=0, keepdims=True)
    m_hi = jnp.maximum(jnp.max(s_b, axis=0, keepdims=True), jnp.max(s_c, axis=0, keepdims=True))
    p_a, p_b, p_c = jnp.exp(s_a - m_lo), jnp.exp(s_b - m_hi), jnp.exp(s_c - m_hi)
    inv_lo = 1.0 / jnp.sum(p_a, axis=0, keepdims=True)
    inv_hi = 1.0 / (jnp.sum(p_b, axis=0, keepdims=True) + jnp.sum(p_c, axis=0, keepdims=True))
    return p_a * inv_lo, p_b * inv_hi, p_c * inv_hi


def attend_kernel(cos_ref, sin_ref, h_ref, x_ref, pack_ref, wo_ref, gain_ref, rot_ref, out_ref, res_ref, h_two_ref, inv_ref, qkv):
    seq_len = h_ref.shape[0]
    low = low_lanes(seq_len)
    cos_all, sin_all = cos_ref[...], sin_ref[...]
    scale_q = Q_HEADS * HEAD_DIM
    qkv[...] = dot_mid(h_ref[...], pack_ref[...])
    for c in range(QK_COLS // LANES):
        x = turn(qkv[:, c * LANES:(c + 1) * LANES], cos_all, sin_all, low)
        col = c * LANES + lax.broadcasted_iota(jnp.int32, x.shape, 1)
        if (c + 1) * LANES <= scale_q:
            x = x * HEAD_DIM ** -0.5
        elif c * LANES < scale_q:
            x = jnp.where(col < scale_q, x * HEAD_DIM ** -0.5, x)
        rot_ref[:, c * LANES:(c + 1) * LANES] = x.astype(BF)
    rot_ref[:, QK_COLS:] = qkv[:, QK_COLS:QKV_COLS].astype(BF)
    half = seq_len // 2
    lo, hi = slice(0, half), slice(half, seq_len)
    mask = hidden(half)
    for g in range(KV_HEADS):
        k0, v0 = scale_q + g * HEAD_DIM, QK_COLS + g * HEAD_DIM
        k = rot_ref[:, k0:k0 + HEAD_DIM]
        v = rot_ref[:, v0:v0 + HEAD_DIM]
        p_a, p_b, p_c = probabilities(lanes_of(rot_ref, lo, 3 * g), lanes_of(rot_ref, hi, 3 * g), k, mask)
        o_lo = dot_first(p_a.astype(BF), v[lo]).astype(BF)
        o_hi = dot_first(jnp.concatenate([p_b.astype(BF), p_c.astype(BF)], axis=0), v).astype(BF)
        for j in range(3):
            h = 3 * g + j
            out_ref[lo, h * HEAD_DIM:(h + 1) * HEAD_DIM] = o_lo[j * half:(j + 1) * half]
            out_ref[hi, h * HEAD_DIM:(h + 1) * HEAD_DIM] = o_hi[j * half:(j + 1) * half]
    resid = (x_ref[...].astype(F32) + dot_mid(out_ref[...], wo_ref[...])).T.astype(BF)
    res_ref[0] = resid
    s = resid.astype(F32)
    inv = lax.rsqrt(jnp.mean(s * s, axis=0, keepdims=True) + NORM_EPS)
    inv_ref[0] = inv
    h_two_ref[0] = (s * inv * gain_ref[...]).astype(BF)


def whole(shape):
    return pl.BlockSpec(shape, lambda s: (0,) * len(shape))


def by_seq(shape):
    return pl.BlockSpec(shape, lambda s: (s,) + (0,) * (len(shape) - 1))


def attend(h_one, emb, full_pack, full_out, gain_two, seq_len, tables):
    n_tok, dim = emb.shape
    batch = n_tok // seq_len
    cube = (1, dim, seq_len)
    return pl.pallas_call(
        attend_kernel,
        grid=(batch,),
        in_specs=[whole((seq_len, LANES))] * 2 + [by_seq((seq_len, dim))] * 2 + [whole(full_pack.shape), whole(full_out.shape), whole((dim, 1))],
        out_specs=[by_seq((seq_len, QKV_COLS)), by_seq((seq_len, dim)), by_seq(cube), by_seq(cube), by_seq((1, 1, seq_len))],
        out_shape=[
            jax.ShapeDtypeStruct((n_tok, QKV_COLS), BF), jax.ShapeDtypeStruct((n_tok, dim), BF),
            jax.ShapeDtypeStruct((batch, dim, seq_len), BF), jax.ShapeDtypeStruct((batch, dim, seq_len), BF),
            jax.ShapeDtypeStruct((batch, 1, seq_len), F32),
        ],
        scratch_shapes=[pltpu.VMEM((seq_len, PACK_COLS), F32)],
        compiler_params=params(40 * 1024 * 1024),
        cost_estimate=pl.CostEstimate(
            flops=4 * n_tok * seq_len * dim + 2 * n_tok * dim * (PACK_COLS + dim), bytes_accessed=14 * n_tok * dim,
            transcendentals=n_tok * seq_len * Q_HEADS),
        name="attend",
    )(*tables, h_one, emb, full_pack, full_out, gain_two.reshape(dim, 1))


def attend_back_kernel(cos_ref, sin_ref, rot_ref, d_res_ref, x_ref, pack_ref, wo_ref, gain_ref, out_ref, d_x_ref, d_gain_ref, d_rot, d_ref):
    seq_len = rot_ref.shape[0]
    d_resid = d_res_ref[0].astype(F32).T
    d_ref[...] = dot_last(d_resid.astype(BF), wo_ref[...]).astype(BF)
    scale_q = Q_HEADS * HEAD_DIM
    half = seq_len // 2
    lo, hi = slice(0, half), slice(half, seq_len)
    mask = hidden(half)
    for g in range(KV_HEADS):
        k0, v0 = scale_q + g * HEAD_DIM, QK_COLS + g * HEAD_DIM
        k = rot_ref[:, k0:k0 + HEAD_DIM]
        v = rot_ref[:, v0:v0 + HEAD_DIM]
        q_lo, q_hi = lanes_of(rot_ref, lo, 3 * g), lanes_of(rot_ref, hi, 3 * g)
        d_lo, d_hi = lanes_of(d_ref, lo, 3 * g), lanes_of(d_ref, hi, 3 * g)
        n_lo = q_lo.shape[0]
        p_a, p_b, p_c = probabilities(q_lo, q_hi, k, mask)
        d_all = jnp.concatenate([d_lo, d_hi], axis=0)
        dp_all = dot_last(v[lo], d_all).astype(BF).astype(F32)
        dp_c = dot_last(v[hi], d_hi).astype(BF).astype(F32)
        p_lo = jnp.concatenate([p_a.astype(BF), p_b.astype(BF)], axis=1)
        out_ref[lo, v0:v0 + HEAD_DIM] = dot_mid(p_lo, d_all).astype(BF)
        out_ref[hi, v0:v0 + HEAD_DIM] = dot_mid(p_c.astype(BF), d_hi).astype(BF)
        pd_a, pd_b, pd_c = p_a * dp_all[:, :n_lo], p_b * dp_all[:, n_lo:], p_c * dp_c
        t_lo = jnp.sum(pd_a, axis=0, keepdims=True)
        t_hi = jnp.sum(pd_b, axis=0, keepdims=True) + jnp.sum(pd_c, axis=0, keepdims=True)
        ds_a = (pd_a - p_a * t_lo).astype(BF)
        ds_b = (pd_b - p_b * t_hi).astype(BF)
        ds_c = (pd_c - p_c * t_hi).astype(BF)
        q_all = jnp.concatenate([q_lo, q_hi], axis=0)
        ds_all = jnp.concatenate([ds_a, ds_b], axis=1)
        d_rot[lo, k0:k0 + HEAD_DIM] = dot_mid(ds_all, q_all).astype(BF).astype(F32)
        d_rot[hi, k0:k0 + HEAD_DIM] = dot_mid(ds_c, q_hi).astype(BF).astype(F32)
        scale = HEAD_DIM ** -0.5
        dq_lo = (dot_first(ds_a, k[lo]) * scale).astype(BF).astype(F32)
        dq_hi = (dot_first(jnp.concatenate([ds_b, ds_c], axis=0), k) * scale).astype(BF).astype(F32)
        for j in range(3):
            h = 3 * g + j
            d_rot[lo, h * HEAD_DIM:(h + 1) * HEAD_DIM] = dq_lo[j * half:(j + 1) * half]
            d_rot[hi, h * HEAD_DIM:(h + 1) * HEAD_DIM] = dq_hi[j * half:(j + 1) * half]
    out_ref[:, QKV_COLS:] = jnp.zeros((seq_len, PACK_COLS - QKV_COLS), BF)
    low = low_lanes(seq_len)
    cos_all, sin_all = cos_ref[...], -sin_ref[...]
    for c in range(QK_COLS // LANES):
        at = slice(c * LANES, (c + 1) * LANES)
        out_ref[:, at] = turn(d_rot[:, at], cos_all, sin_all, low).astype(BF)
    d_h = dot_last(out_ref[...], pack_ref[...]).astype(BF).astype(F32)
    x = x_ref[...].astype(F32)
    inv = lax.rsqrt(jnp.mean(x * x, axis=-1, keepdims=True) + NORM_EPS)
    d_n = d_h * gain_ref[...]
    pull = jnp.mean(d_n * x, axis=-1, keepdims=True) * (inv * inv * inv)
    d_x_ref[...] = (d_resid + (d_n * inv - x * pull)).astype(BF)
    d_gain = jnp.sum(d_h * (x * inv), axis=0, keepdims=True)

    @pl.when(pl.program_id(0) == 0)
    def _():
        d_gain_ref[...] = jnp.zeros_like(d_gain_ref)

    d_gain_ref[...] += d_gain


def attend_back(rot, d_resid, emb, full_pack, full_out, gain_one, seq_len, tables):
    n_tok, dim = emb.shape
    return pl.pallas_call(
        attend_back_kernel,
        grid=(n_tok // seq_len,),
        in_specs=[whole((seq_len, LANES))] * 2
        + [by_seq((seq_len, QKV_COLS)), by_seq((1, dim, seq_len)), by_seq((seq_len, dim))]
        + [whole(full_pack.shape), whole(full_out.shape), whole((1, dim))],
        out_specs=[by_seq((seq_len, PACK_COLS)), by_seq((seq_len, dim)), whole((1, dim))],
        out_shape=[jax.ShapeDtypeStruct((n_tok, PACK_COLS), BF), jax.ShapeDtypeStruct((n_tok, dim), BF), jax.ShapeDtypeStruct((1, dim), F32)],
        scratch_shapes=[pltpu.VMEM((seq_len, QK_COLS), F32), pltpu.VMEM((seq_len, dim), BF)],
        compiler_params=params(40 * 1024 * 1024),
        cost_estimate=pl.CostEstimate(
            flops=10 * n_tok * seq_len * dim + 2 * n_tok * dim * (PACK_COLS + dim), bytes_accessed=14 * n_tok * dim,
            transcendentals=n_tok * seq_len * Q_HEADS),
        name="attend_back",
    )(*tables, rot, d_resid, emb, full_pack, full_out, gain_one.reshape(1, dim))


def rms_norm(x_f32, gain_f32):
    inv_rms = lax.rsqrt(jnp.mean(x_f32 * x_f32, axis=-1, keepdims=True) + NORM_EPS)
    return (x_f32 * inv_rms * gain_f32).astype(BF)


def gated(gate_f32, up_f32):
    return (jax.nn.silu(gate_f32) * up_f32).astype(BF)


def mm(a, b):
    return jnp.einsum("bsd,df->bsf", a, b, preferred_element_type=F32)


def mm_t(a, b):
    return jnp.einsum("bsf,df->bsd", a, b, preferred_element_type=F32)


def mm_w(a, b):
    return jnp.einsum("bsd,bsf->df", a, b, preferred_element_type=F32)


def row_major(x):
    return with_layout_constraint(x, Layout(major_to_minor=(0, 1)))


def from_peer(x, k):
    return lax.ppermute(x, AXIS_NAME, [(i, i ^ k) for i in range(N_DEV)]) if k else x


def owned_ids(token_ids, rows_dev, k):
    rel_ids = from_peer(token_ids, k).reshape(-1) - lax.axis_index(AXIS_NAME) * rows_dev
    return rel_ids, (rel_ids >= 0) & (rel_ids < rows_dev)


def slow_rows(token_ids, table):
    total = None
    for k in range(N_DEV):
        rel_ids, owned = owned_ids(token_ids, table.shape[0], k)
        picked = jnp.take(table, jnp.where(owned, rel_ids, 0), axis=0)
        part = from_peer(jnp.where(owned[:, None], picked, jnp.zeros((), BF)), k)
        total = part if total is None else total + part
    return total


def slow_grad(token_ids, d_emb, rows_dev):
    total = None
    for k in range(N_DEV):
        rel_ids, owned = owned_ids(token_ids, rows_dev, k)
        d_all = from_peer(d_emb, k).astype(F32)
        seg_ids = jnp.where(owned, rel_ids, rows_dev)
        part = jax.ops.segment_sum(d_all, seg_ids, num_segments=rows_dev)
        total = part if total is None else total + part
    return total.astype(BF)


def gather_all(shard):
    return lax.all_gather(shard, AXIS_NAME, axis=0, tiled=True)


def scatter_sum(partial):
    return lax.psum_scatter(partial, AXIS_NAME, scatter_dimension=0, tiled=True)


def solution(mesh):
    spec_1d = P(AXIS_NAME)
    spec_2d = P(AXIS_NAME, None)
    spec_3d = P(AXIS_NAME, None, None)
    in_specs = (spec_2d, spec_3d, spec_2d, spec_1d, spec_1d, spec_3d, spec_3d, spec_3d, spec_2d, spec_2d, spec_2d, spec_2d)
    out_specs = (spec_3d, spec_2d, spec_1d, spec_1d, spec_3d, spec_3d, spec_3d, spec_2d, spec_2d, spec_2d, spec_2d)

    def device_step(token_ids, grad_y, table, g_one, g_two, w_query, w_key, w_value, w_out, w_gate, w_up, w_down):
        rows_dev, dim = table.shape
        batch, seq_len = token_ids.shape
        n_tok = batch * seq_len
        rows_w = w_query.shape[0]

        pad = jnp.zeros((rows_w, PACK_COLS - QKV_COLS - 2), BF)
        shards = [w.reshape(rows_w, -1) for w in (w_query, w_key, w_value)]
        pack = jnp.concatenate(shards + [g_one[:, None], g_two[:, None], pad], axis=1)
        full_pack = gather_all(pack)
        full_down = gather_all(w_down)
        gain_one = full_pack[:, QKV_COLS].astype(F32)
        gain_two = full_pack[:, QKV_COLS + 1].astype(F32)

        slot, req = route(token_ids.reshape(n_tok), rows_dev)
        asked = swap([req[k:k + 1] for k in range(N_DEV)])
        asked = jnp.concatenate(asked, axis=0)
        overflow = jnp.max(asked[:, CAP]) > CAP
        asked = asked[:, :CAP]
        parts = swap(pick_rows(table, asked))
        d_act = mm_t(grad_y, full_down).astype(BF)
        parts, d_act, w_out, w_gate, w_up = lax.optimization_barrier((parts, d_act, w_out, w_gate, w_up))
        full_out = gather_all(w_out)
        full_gate = gather_all(w_gate)
        full_up = gather_all(w_up)
        emb, h_one = expand_rows(parts, slot.reshape(n_tok), gain_one)

        def slow_start():
            rows = slow_rows(token_ids, table)
            return rows, rms_norm(rows.astype(F32), gain_one)

        emb, h_one = lax.cond(overflow, slow_start, lambda: (emb, h_one))
        emb, h_one = row_major(emb), row_major(h_one)

        tables = rope_tables(seq_len)
        cube = (batch, seq_len, -1)
        rot, attn, resid_t, h_two_t, inv_t = attend(h_one, emb, full_pack, full_out, gain_two, seq_len, tables)
        attn = attn.reshape(cube)
        resid, h_two, inv_two = (jnp.swapaxes(v, 1, 2) for v in (resid_t, h_two_t, inv_t))
        gate_f32 = mm(h_two, full_gate)
        up_f32 = mm(h_two, full_up)
        act, act_pull = jax.vjp(gated, gate_f32, up_f32)

        g_down = mm_w(act, grad_y)
        d_gate, d_up = act_pull(d_act)
        d_gate, d_up = d_gate.astype(BF), d_up.astype(BF)
        d_gate, d_up, g_down = lax.optimization_barrier((d_gate, d_up, g_down))
        sum_down = scatter_sum(g_down)
        g_gate, g_up = mm_w(h_two, d_gate), mm_w(h_two, d_up)
        d_gate, d_up, g_gate, g_up = lax.optimization_barrier((d_gate, d_up, g_gate, g_up))
        sum_gate, sum_up = scatter_sum(g_gate), scatter_sum(g_up)
        d_h_two = (mm_t(d_gate, full_gate) + mm_t(d_up, full_up)).astype(BF).astype(F32)
        resid_f32 = resid.astype(F32)
        d_n = d_h_two * gain_two
        pull = jnp.mean(d_n * resid_f32, axis=-1, keepdims=True) * (inv_two * inv_two * inv_two)
        d_gain_two = jnp.sum(d_h_two * (resid_f32 * inv_two), axis=(0, 1))
        d_resid = (grad_y.astype(F32) + (d_n * inv_two - resid_f32 * pull)).astype(BF)
        g_out = mm_w(attn, d_resid)
        d_resid, g_out, sum_down = lax.optimization_barrier((d_resid, g_out, sum_down))
        sum_out = scatter_sum(g_out)
        d_qkv, d_emb, d_gain_one = attend_back(rot, jnp.swapaxes(d_resid, 1, 2), emb, full_pack, full_out, gain_one, seq_len, tables)
        d_qkv, d_emb, sum_gate, sum_up = lax.optimization_barrier((d_qkv, d_emb, sum_gate, sum_up))
        g_pack = mm_w(h_one.reshape(cube), d_qkv.reshape(cube))
        gains = jnp.concatenate([d_gain_one.reshape(dim, 1), d_gain_two[:, None]], axis=1)
        g_pack = lax.dynamic_update_slice(g_pack, gains, (0, QKV_COLS))

        folded = fold_rows(d_emb, slot, FAR)
        d_emb, slot, folded, sum_out, g_pack = lax.optimization_barrier((d_emb, slot, folded, sum_out, g_pack))
        sum_pack = scatter_sum(g_pack).astype(BF)
        sent = {k: from_peer(rows, k) for k, rows in zip(FAR, folded)}
        folded = fold_rows(d_emb, slot, NEAR)
        act, resid, folded = lax.optimization_barrier((act, resid, folded))
        sent.update({k: from_peer(rows, k) for k, rows in zip(NEAR, folded)})
        y_out = (resid.astype(F32) + mm(act, full_down)).astype(BF)
        d_table = spread_rows([sent[k] for k in range(N_DEV)], asked, rows_dev, dim)
        d_table, sum_pack, sum_out, sum_gate, sum_up, sum_down = lax.optimization_barrier(
            (d_table, sum_pack, sum_out, sum_gate, sum_up, sum_down))
        d_table = lax.cond(overflow, lambda: slow_grad(token_ids, d_emb, rows_dev), lambda: d_table)

        cols = [0, Q_HEADS * HEAD_DIM, QK_COLS, QKV_COLS]
        d_w = [sum_pack[:, a:b].reshape(rows_w, -1, HEAD_DIM) for a, b in zip(cols[:-1], cols[1:])]
        return (
            y_out, d_table, sum_pack[:, QKV_COLS], sum_pack[:, QKV_COLS + 1],
            d_w[0], d_w[1], d_w[2], sum_out.astype(BF), sum_gate.astype(BF), sum_up.astype(BF), sum_down.astype(BF),
        )

    return jax.shard_map(device_step, mesh=mesh, in_specs=in_specs, out_specs=out_specs, check_vma=False)
```

```python
import functools

import jax
import jax.numpy as jnp
from jax import lax
from jax.experimental import pallas as pl
from jax.experimental.pallas import tpu as pltpu
from jax.experimental.layout import Layout, with_layout_constraint
from jax.sharding import PartitionSpec as P


AXIS_NAME = "fsdp"
NORM_EPS = 1e-5
ROPE_THETA = 500000.0
N_DEV = 8
CAP_MANY = 80
CAP_ONE = 336
CAP = CAP_MANY + CAP_ONE
N_SLOT = N_DEV * CAP
REQ_COLS = 512
HEAD_DIM = 64
Q_HEADS = 15
KV_HEADS = 5
QK_COLS = (Q_HEADS + KV_HEADS) * HEAD_DIM
QKV_COLS = (Q_HEADS + 2 * KV_HEADS) * HEAD_DIM
PACK_COLS = 1664
LANES = 128
WIDE = 1024
VMEM_LIMIT = 60 * 1024 * 1024
BF = jnp.bfloat16
F32 = jnp.float32


def params(limit=VMEM_LIMIT):
    return pltpu.CompilerParams(vmem_limit_bytes=limit, dimension_semantics=("arbitrary",))


def route_kernel(rows_dev, me_ref, ids_ref, slot_ref, req_ref, tok_ref, col_a, col_b):
    n_tok = ids_ref.shape[1]
    me = me_ref[0]
    big = jnp.int32(2**30)
    high = 65536

    def fill(col, row):
        for c in range(n_tok // LANES):
            part = jnp.broadcast_to(row[:, c * LANES:(c + 1) * LANES], (LANES, LANES))
            col[c * LANES:(c + 1) * LANES, :] = part.T

    ids = ids_ref[...]
    tok = lax.broadcasted_iota(jnp.int32, (1, n_tok), 1)
    fill(col_a, ids)
    wide = (8, LANES)
    unroll = 4

    def sweep(n_out, width, rows_of, steps):
        groups = width // LANES
        outs = []
        for g in range(n_out // width):
            rows = [rows_of(g * width + c * LANES) for c in range(groups)]
            accs = tuple(jnp.zeros(wide, jnp.int32) for _ in range(groups))
            for begin, end, step in steps(g):
                def body(i, accs, rows=rows, step=step):
                    for u in range(unroll):
                        accs = step(i * unroll + u, accs, rows)
                    return accs

                accs = lax.fori_loop(begin // (8 * unroll), end // (8 * unroll), body, accs)
            outs.extend(accs)
        return jnp.concatenate([jnp.sum(r, axis=0, keepdims=True) for r in outs], axis=1)

    def id_row(lane0):
        return jnp.broadcast_to(ids_ref[:, lane0:lane0 + LANES], wide)

    def block(i):
        return pl.ds(pl.multiple_of(i * 8, 8), 8)

    def same_steps(g):
        def step(i, accs, rows, weight):
            col = col_a[block(i), :]
            return tuple(acc + jnp.where(col == row, weight(i, c), 0) for c, (acc, row) in enumerate(zip(accs, rows)))

        def mixed(i, c):
            pos = i * 8 + lax.broadcasted_iota(jnp.int32, wide, 0)
            at = g * 1024 + c * LANES + lax.broadcasted_iota(jnp.int32, wide, 1)
            return jnp.where(pos < at, high + 1, 1)

        before = functools.partial(step, weight=lambda i, c: high + 1)
        after = functools.partial(step, weight=lambda i, c: 1)
        lo, hi = g * 1024, (g + 1) * 1024
        return [(0, lo, before), (lo, hi, functools.partial(step, weight=mixed)), (hi, n_tok, after)]

    same = sweep(n_tok, 1024, id_row, same_steps)
    first = same < high
    many = lax.rem(same, high) > 1
    key = jnp.where(first, ids, big)
    count = jnp.where(many, 1, high)
    fill(col_a, count)
    fill(col_b, key)

    def rank_step(i, accs, rows):
        col, num = col_b[block(i), :], col_a[block(i), :]
        return tuple(acc + jnp.where(col < row, num, 0) for acc, row in zip(accs, rows))

    below = sweep(n_tok, 1024, id_row, lambda g: [(0, n_tok, rank_step)])
    owner = jnp.zeros_like(ids)
    start = jnp.zeros_like(ids)
    prev = jnp.zeros((1, 1), jnp.int32)
    over = jnp.zeros((1, 1), jnp.int32)
    for o in range(1, N_DEV + 1):
        base = jnp.sum(jnp.where(key < o * rows_dev, count, 0), axis=1, keepdims=True)
        held = base - prev
        full = jnp.logical_or(lax.div(held, high) > CAP_ONE, lax.rem(held, high) > CAP_MANY)
        over = jnp.where(full, 1, over)
        prev = base
        if o < N_DEV:
            past = ids >= o * rows_dev
            owner = jnp.where(past, o, owner)
            start = jnp.where(past, base, start)
    rank = below - start
    in_one = CAP_MANY + jnp.minimum(lax.div(rank, high), CAP_ONE - 1)
    in_many = jnp.minimum(lax.rem(rank, high), CAP_MANY - 1)
    slot = (owner ^ me) * CAP + jnp.where(many, in_many, in_one)
    slot_ref[...] = slot
    fill(col_b, jnp.where(first, slot, -1))
    fill(col_a, (ids - owner * rows_dev) * n_tok + tok + 1)

    def req_step(i, accs, rows):
        col, val = col_b[block(i), :], col_a[block(i), :]
        return tuple(acc + jnp.where(col == row, val, 0) for acc, row in zip(accs, rows))

    lanes = lax.broadcasted_iota(jnp.int32, wide, 1)
    code = sweep(N_SLOT, 1664, lambda lane0: lane0 + lanes, lambda g: [(0, n_tok, req_step)])
    used = code > 0
    req = jnp.where(used, lax.div(code - 1, n_tok), rows_dev)
    tok_ref[...] = jnp.where(used, lax.rem(code - 1, n_tok), 0)
    for k in range(N_DEV):
        req_ref[k:k + 1, :CAP] = req[:, k * CAP:(k + 1) * CAP]
        req_ref[k:k + 1, CAP:] = jnp.broadcast_to(over, (1, REQ_COLS - CAP))


def route(ids, rows_dev):
    n_tok = ids.shape[0]
    me = lax.axis_index(AXIS_NAME).astype(jnp.int32).reshape(1)
    vmem = pl.BlockSpec(memory_space=pltpu.VMEM)
    return pl.pallas_call(
        functools.partial(route_kernel, rows_dev),
        out_shape=(
            jax.ShapeDtypeStruct((1, n_tok), jnp.int32), jax.ShapeDtypeStruct((N_DEV, REQ_COLS), jnp.int32),
            jax.ShapeDtypeStruct((1, N_SLOT), jnp.int32)),
        in_specs=[pl.BlockSpec(memory_space=pltpu.SMEM), vmem],
        out_specs=(vmem, vmem, vmem),
        scratch_shapes=[pltpu.VMEM((n_tok, LANES), jnp.int32)] * 2,
        compiler_params=pltpu.CompilerParams(vmem_limit_bytes=16 * 1024 * 1024),
        name="route",
    )(me, ids.reshape(1, n_tok))


def swap(parts):
    out = [parts[0]]
    far = {k: lax.ppermute(parts[k], AXIS_NAME, [(i, i ^ k) for i in range(N_DEV)]) for k in range(N_DEV - 1, 0, -1)}
    return out + [far[k] for k in range(1, N_DEV)]


TILES = WIDE // LANES
ROW_UNROLL = 16
GATHER_CHUNK = 768


def strip(row0, n_rows, c):
    return pl.ds(row0 * TILES + c, n_rows, stride=TILES)


def row(r):
    return pl.ds(pl.multiple_of(r * TILES, TILES), TILES)


def to_rows(dst, row0, src, n_rows, dim):
    for c in range(TILES):
        n_lane = max(0, min(LANES, dim - c * LANES))
        part = src(c * LANES, n_lane).astype(F32)
        if n_lane < LANES:
            part = jnp.concatenate([part, jnp.zeros((n_rows, LANES - n_lane), F32)], axis=1)
        dst[strip(row0, n_rows, c), :] = part


def copy_rows(src, idx_ref, idx0, dst, n_rows):
    def body(i, carry):
        vals = [src[row(idx_ref[idx0 + i * ROW_UNROLL + u]), :] for u in range(ROW_UNROLL)]
        for u in range(ROW_UNROLL):
            dst[row(i * ROW_UNROLL + u), :] = vals[u]
        return carry

    lax.fori_loop(0, n_rows // ROW_UNROLL, body, 0)


def pick_kernel(idx_ref, tab_ref, *refs):
    outs, rows, stage = refs[:N_DEV], refs[N_DEV], refs[N_DEV + 1]
    step = pl.program_id(0)
    dim, n_rows = tab_ref.shape[0], rows.shape[0] // TILES
    n_load = n_rows // GATHER_CHUNK

    @pl.when(step < n_load)
    def _():
        for c in range(TILES):
            part = tab_ref[c * LANES:min((c + 1) * LANES, dim), :].astype(F32)
            if part.shape[0] < LANES:
                part = jnp.concatenate([part, jnp.zeros((LANES - part.shape[0], GATHER_CHUNK), F32)], axis=0)
            rows[strip(step * GATHER_CHUNK, GATHER_CHUNK, c), :] = part.T

    for k in range(N_DEV):
        @pl.when(step == n_load + k)
        def _(k=k):
            copy_rows(rows, idx_ref, k * CAP, stage, CAP)
            for c in range(TILES):
                outs[k][:, c * LANES:(c + 1) * LANES] = stage[strip(0, CAP, c), :].astype(BF)


def pick_rows(table, idx):
    rows_dev, dim = table.shape
    n_load = rows_dev // GATHER_CHUNK
    idx = jnp.minimum(idx.reshape(-1), rows_dev - 1)
    return pl.pallas_call(
        pick_kernel,
        grid_spec=pltpu.PrefetchScalarGridSpec(
            num_scalar_prefetch=1,
            grid=(n_load + N_DEV,),
            in_specs=[pl.BlockSpec((dim, GATHER_CHUNK), lambda s, _: (0, jnp.minimum(s, n_load - 1)))],
            out_specs=[pl.BlockSpec((CAP, WIDE), lambda s, _: (0, 0))] * N_DEV,
            scratch_shapes=[pltpu.VMEM((rows_dev * TILES, LANES), F32), pltpu.VMEM((CAP * TILES, LANES), F32)],
        ),
        out_shape=[jax.ShapeDtypeStruct((CAP, WIDE), BF)] * N_DEV,
        compiler_params=params(),
        cost_estimate=pl.CostEstimate(flops=10**9, bytes_accessed=2 * rows_dev * dim, transcendentals=0),
        name="pick_rows",
    )(idx, table.T)


EXPAND_ROWS = 512


def expand_kernel(idx_ref, gain_ref, *refs):
    parts, e_ref, h_ref, rows, stage = refs[:N_DEV], *refs[N_DEV:]
    step = pl.program_id(0)
    dim = e_ref.shape[1]

    @pl.when(step == 0)
    def _():
        for k in range(N_DEV):
            to_rows(rows, k * CAP, lambda at, n, k=k: parts[k][:, at:at + n], CAP, WIDE)

    copy_rows(rows, idx_ref, step * EXPAND_ROWS, stage, EXPAND_ROWS)
    x = jnp.concatenate([stage[strip(0, EXPAND_ROWS, c), :] for c in range(TILES)], axis=1)[:, :dim]
    e_ref[...] = x.astype(BF)
    inv = lax.rsqrt(jnp.mean(x * x, axis=-1, keepdims=True) + NORM_EPS)
    h_ref[...] = (x * inv * gain_ref[...]).astype(BF)


def expand_rows(parts, slot, gain):
    n_tok, dim = slot.shape[0], gain.shape[0]
    return pl.pallas_call(
        expand_kernel,
        grid_spec=pltpu.PrefetchScalarGridSpec(
            num_scalar_prefetch=1,
            grid=(n_tok // EXPAND_ROWS,),
            in_specs=[pl.BlockSpec((1, dim), lambda s, _: (0, 0))] + [pl.BlockSpec((CAP, WIDE), lambda s, _: (0, 0))] * N_DEV,
            out_specs=[pl.BlockSpec((EXPAND_ROWS, dim), lambda s, _: (s, 0))] * 2,
            scratch_shapes=[pltpu.VMEM((N_SLOT * TILES, LANES), F32), pltpu.VMEM((EXPAND_ROWS * TILES, LANES), F32)],
        ),
        out_shape=[jax.ShapeDtypeStruct((n_tok, dim), BF)] * 2,
        compiler_params=params(),
        name="expand_rows",
    )(slot, gain.reshape(1, dim), *parts)


def fold_kernel(tok_ref, slot_ref, d_ref, *refs):
    many, ones, rows, stage = refs[:N_DEV], refs[N_DEV:2 * N_DEV], refs[2 * N_DEV], refs[2 * N_DEV + 1]
    n_tok, dim = d_ref.shape
    step = pl.program_id(0)
    half = N_DEV // 2
    width = 1024
    chunk = 512

    @pl.when(step == 0)
    def _():
        for b in range(n_tok // chunk):
            to_rows(rows, b * chunk, lambda at, n, b=b: d_ref[b * chunk:(b + 1) * chunk, at:at + n], chunk, dim)

    for part in range(2):
        @pl.when(step == part)
        def _(part=part):
            total = None
            for c in range(n_tok // width):
                hot = []
                for k in range(part * half, (part + 1) * half):
                    ids = jnp.broadcast_to(slot_ref[:, c * width:(c + 1) * width], (CAP_MANY, width))
                    mine = k * CAP + lax.broadcasted_iota(jnp.int32, (CAP_MANY, width), 0)
                    hot.append(jnp.where(ids == mine, 1.0, 0.0).astype(BF))
                term = jnp.dot(jnp.concatenate(hot, axis=0), d_ref[c * width:(c + 1) * width, :], preferred_element_type=F32)
                total = term if total is None else total + term
            for j in range(half):
                out = many[part * half + j]
                out[:, :dim] = total[j * CAP_MANY:(j + 1) * CAP_MANY]
                out[:, dim:] = jnp.zeros((CAP_MANY, WIDE - dim), F32)

    for k in range(N_DEV):
        @pl.when(step == 2 + k)
        def _(k=k):
            copy_rows(rows, tok_ref, k * CAP + CAP_MANY, stage, CAP_ONE)
            for c in range(TILES):
                ones[k][:, c * LANES:(c + 1) * LANES] = stage[strip(0, CAP_ONE, c), :].astype(BF)


def fold_rows(d_emb, slot, tok):
    n_tok, dim = d_emb.shape
    out = pl.pallas_call(
        fold_kernel,
        grid_spec=pltpu.PrefetchScalarGridSpec(
            num_scalar_prefetch=1,
            grid=(2 + N_DEV,),
            in_specs=[pl.BlockSpec((1, n_tok), lambda s, _: (0, 0)), pl.BlockSpec((n_tok, dim), lambda s, _: (0, 0))],
            out_specs=[pl.BlockSpec((CAP_MANY, WIDE), lambda s, _: (0, 0))] * N_DEV + [pl.BlockSpec((CAP_ONE, WIDE), lambda s, _: (0, 0))] * N_DEV,
            scratch_shapes=[pltpu.VMEM((n_tok * TILES, LANES), F32), pltpu.VMEM((CAP_ONE * TILES, LANES), F32)],
        ),
        out_shape=[jax.ShapeDtypeStruct((CAP_MANY, WIDE), F32)] * N_DEV + [jax.ShapeDtypeStruct((CAP_ONE, WIDE), BF)] * N_DEV,
        compiler_params=params(),
        cost_estimate=pl.CostEstimate(flops=2 * N_DEV * CAP_MANY * n_tok * dim, bytes_accessed=4 * N_SLOT * dim, transcendentals=0),
        name="fold_rows",
    )(tok.reshape(-1), slot, d_emb)
    return out[:N_DEV], out[N_DEV:]


ADD_UNROLL = 8


def spread_kernel(rows_dev, idx_ref, *refs):
    many, ones, out_ref, total, stage = refs[:N_DEV], refs[N_DEV:2 * N_DEV], *refs[2 * N_DEV:]
    step = pl.program_id(0)

    @pl.when(step == 0)
    def _():
        total[...] = jnp.zeros_like(total)

    for k in range(N_DEV):
        @pl.when(step == k)
        def _(k=k):
            to_rows(stage, 0, lambda at, n: many[k][:, at:at + n], CAP_MANY, WIDE)
            to_rows(stage, CAP_MANY, lambda at, n: ones[k][:, at:at + n], CAP_ONE, WIDE)

            def body(i, carry):
                rows = [idx_ref[k * CAP + i * ADD_UNROLL + u] for u in range(ADD_UNROLL)]
                sums = [total[row(rows[u]), :] + stage[row(i * ADD_UNROLL + u), :] for u in range(ADD_UNROLL)]
                for u in range(ADD_UNROLL):
                    total[row(rows[u]), :] = sums[u]
                return carry

            lax.fori_loop(0, CAP // ADD_UNROLL, body, 0)

    @pl.when(step >= N_DEV)
    def _():
        at = (step - N_DEV) * GATHER_CHUNK
        dim = out_ref.shape[0]
        for c in range(TILES):
            n_lane = min(LANES, dim - c * LANES)
            part = total[strip(at, GATHER_CHUNK, c), :].T
            out_ref[c * LANES:c * LANES + n_lane, :] = part[:n_lane].astype(BF)


def spread_rows(many, ones, idx, rows_dev, dim):
    n_out = rows_dev // GATHER_CHUNK
    return pl.pallas_call(
        functools.partial(spread_kernel, rows_dev),
        grid_spec=pltpu.PrefetchScalarGridSpec(
            num_scalar_prefetch=1,
            grid=(N_DEV + n_out,),
            in_specs=[pl.BlockSpec((CAP_MANY, WIDE), lambda s, _: (0, 0))] * N_DEV + [pl.BlockSpec((CAP_ONE, WIDE), lambda s, _: (0, 0))] * N_DEV,
            out_specs=pl.BlockSpec((dim, GATHER_CHUNK), lambda s, _: (0, jnp.maximum(s - N_DEV, 0))),
            scratch_shapes=[pltpu.VMEM(((rows_dev + 8) * TILES, LANES), F32), pltpu.VMEM((CAP * TILES, LANES), F32)],
        ),
        out_shape=jax.ShapeDtypeStruct((dim, rows_dev), BF),
        compiler_params=params(),
        name="spread_rows",
    )(idx.reshape(-1), *many, *ones).T


def rope_tables(seq_len):
    half = HEAD_DIM // 2
    inv_freq = ROPE_THETA ** (-2.0 * jnp.arange(half, dtype=F32) / HEAD_DIM)
    angles = jnp.arange(seq_len, dtype=F32)[:, None] * inv_freq[None, :]
    cos_tab, sin_tab = jnp.cos(angles), jnp.sin(angles)
    cos_all = jnp.concatenate([cos_tab] * 4, axis=1)
    sin_all = jnp.concatenate([-sin_tab, sin_tab] * 2, axis=1)
    return cos_all, sin_all


def turn(x, cos_all, sin_all, low):
    other = jnp.where(low, pltpu.roll(x, LANES - HEAD_DIM // 2, 1), pltpu.roll(x, HEAD_DIM // 2, 1))
    return x * cos_all + other * sin_all


def low_lanes(seq_len):
    lane = lax.broadcasted_iota(jnp.int32, (seq_len, LANES), 1)
    return lax.rem(lane, HEAD_DIM) < HEAD_DIM // 2


CONTRACT_LAST = (((1,), (1,)), ((), ()))
CONTRACT_FIRST = (((0,), (0,)), ((), ()))


def lanes_of(ref, at, first_head):
    return jnp.concatenate([ref[at, h * HEAD_DIM:(h + 1) * HEAD_DIM] for h in range(first_head, first_head + 3)], axis=0)


def hidden(half):
    key = lax.broadcasted_iota(jnp.int32, (half, 3 * half), 0)
    query = lax.rem(lax.broadcasted_iota(jnp.int32, (half, 3 * half), 1), half)
    return key > query


def dot_last(a, b):
    return lax.dot_general(a, b, CONTRACT_LAST, preferred_element_type=F32)


def dot_first(a, b):
    return lax.dot_general(a, b, CONTRACT_FIRST, preferred_element_type=F32)


def dot_mid(a, b):
    return jnp.dot(a, b, preferred_element_type=F32)


def probabilities(q_lo, q_hi, k, mask):
    half, n_lo = k.shape[0] // 2, q_lo.shape[0]
    s_all = dot_last(k[:half], jnp.concatenate([q_lo, q_hi], axis=0))
    s_a = jnp.where(mask, -1e30, s_all[:, :n_lo])
    s_b = s_all[:, n_lo:]
    s_c = jnp.where(mask, -1e30, dot_last(k[half:], q_hi))
    m_lo = jnp.max(s_a, axis=0, keepdims=True)
    m_hi = jnp.maximum(jnp.max(s_b, axis=0, keepdims=True), jnp.max(s_c, axis=0, keepdims=True))
    p_a, p_b, p_c = jnp.exp(s_a - m_lo), jnp.exp(s_b - m_hi), jnp.exp(s_c - m_hi)
    inv_lo = 1.0 / jnp.sum(p_a, axis=0, keepdims=True)
    inv_hi = 1.0 / (jnp.sum(p_b, axis=0, keepdims=True) + jnp.sum(p_c, axis=0, keepdims=True))
    return p_a * inv_lo, p_b * inv_hi, p_c * inv_hi


def attend_kernel(cos_ref, sin_ref, h_ref, x_ref, pack_ref, wo_ref, gain_ref, rot_ref, out_ref, res_ref, h_two_ref, inv_ref, qkv):
    seq_len = h_ref.shape[0]
    low = low_lanes(seq_len)
    cos_all, sin_all = cos_ref[...], sin_ref[...]
    scale_q = Q_HEADS * HEAD_DIM
    qkv[...] = dot_mid(h_ref[...], pack_ref[...])
    for c in range(QK_COLS // LANES):
        x = turn(qkv[:, c * LANES:(c + 1) * LANES], cos_all, sin_all, low)
        col = c * LANES + lax.broadcasted_iota(jnp.int32, x.shape, 1)
        if (c + 1) * LANES <= scale_q:
            x = x * HEAD_DIM ** -0.5
        elif c * LANES < scale_q:
            x = jnp.where(col < scale_q, x * HEAD_DIM ** -0.5, x)
        rot_ref[:, c * LANES:(c + 1) * LANES] = x.astype(BF)
    rot_ref[:, QK_COLS:] = qkv[:, QK_COLS:QKV_COLS].astype(BF)
    half = seq_len // 2
    lo, hi = slice(0, half), slice(half, seq_len)
    mask = hidden(half)
    for g in range(KV_HEADS):
        k0, v0 = scale_q + g * HEAD_DIM, QK_COLS + g * HEAD_DIM
        k = rot_ref[:, k0:k0 + HEAD_DIM]
        v = rot_ref[:, v0:v0 + HEAD_DIM]
        p_a, p_b, p_c = probabilities(lanes_of(rot_ref, lo, 3 * g), lanes_of(rot_ref, hi, 3 * g), k, mask)
        o_lo = dot_first(p_a.astype(BF), v[lo]).astype(BF)
        o_hi = dot_first(jnp.concatenate([p_b.astype(BF), p_c.astype(BF)], axis=0), v).astype(BF)
        for j in range(3):
            h = 3 * g + j
            out_ref[lo, h * HEAD_DIM:(h + 1) * HEAD_DIM] = o_lo[j * half:(j + 1) * half]
            out_ref[hi, h * HEAD_DIM:(h + 1) * HEAD_DIM] = o_hi[j * half:(j + 1) * half]
    s = (x_ref[...].astype(F32) + dot_mid(out_ref[...], wo_ref[...])).astype(BF).astype(F32)
    h_two_ref[...] = (s * lax.rsqrt(jnp.mean(s * s, axis=-1, keepdims=True) + NORM_EPS) * gain_ref[...]).astype(BF)
    s = s.T
    res_ref[0] = s.astype(BF)
    inv_ref[0] = lax.rsqrt(jnp.mean(s * s, axis=0, keepdims=True) + NORM_EPS)


def whole(shape):
    return pl.BlockSpec(shape, lambda s: (0,) * len(shape))


def by_seq(shape):
    return pl.BlockSpec(shape, lambda s: (s,) + (0,) * (len(shape) - 1))


def attend(h_one, emb, full_pack, full_out, gain_two, seq_len, tables):
    n_tok, dim = emb.shape
    batch = n_tok // seq_len
    cube = (1, dim, seq_len)
    return pl.pallas_call(
        attend_kernel,
        grid=(batch,),
        in_specs=[whole((seq_len, LANES))] * 2 + [by_seq((seq_len, dim))] * 2 + [whole(full_pack.shape), whole(full_out.shape), whole((1, dim))],
        out_specs=[by_seq((seq_len, QKV_COLS)), by_seq((seq_len, dim)), by_seq(cube), by_seq((seq_len, dim)), by_seq((1, 1, seq_len))],
        out_shape=[
            jax.ShapeDtypeStruct((n_tok, QKV_COLS), BF), jax.ShapeDtypeStruct((n_tok, dim), BF),
            jax.ShapeDtypeStruct((batch, dim, seq_len), BF), jax.ShapeDtypeStruct((n_tok, dim), BF),
            jax.ShapeDtypeStruct((batch, 1, seq_len), F32),
        ],
        scratch_shapes=[pltpu.VMEM((seq_len, PACK_COLS), F32)],
        compiler_params=params(40 * 1024 * 1024),
        cost_estimate=pl.CostEstimate(
            flops=4 * n_tok * seq_len * dim + 2 * n_tok * dim * (PACK_COLS + dim), bytes_accessed=14 * n_tok * dim,
            transcendentals=n_tok * seq_len * Q_HEADS),
        name="attend",
    )(*tables, h_one, emb, full_pack, full_out, gain_two.reshape(1, dim))


def attend_back_kernel(cos_ref, sin_ref, rot_ref, d_res_ref, x_ref, pack_ref, wo_ref, gain_ref, out_ref, d_x_ref, d_gain_ref, d_rot, d_ref):
    seq_len = rot_ref.shape[0]
    d_resid = d_res_ref[0].astype(F32).T
    d_ref[...] = dot_last(d_resid.astype(BF), wo_ref[...]).astype(BF)
    scale_q = Q_HEADS * HEAD_DIM
    half = seq_len // 2
    lo, hi = slice(0, half), slice(half, seq_len)
    mask = hidden(half)
    for g in range(KV_HEADS):
        k0, v0 = scale_q + g * HEAD_DIM, QK_COLS + g * HEAD_DIM
        k = rot_ref[:, k0:k0 + HEAD_DIM]
        v = rot_ref[:, v0:v0 + HEAD_DIM]
        q_lo, q_hi = lanes_of(rot_ref, lo, 3 * g), lanes_of(rot_ref, hi, 3 * g)
        d_lo, d_hi = lanes_of(d_ref, lo, 3 * g), lanes_of(d_ref, hi, 3 * g)
        n_lo = q_lo.shape[0]
        p_a, p_b, p_c = probabilities(q_lo, q_hi, k, mask)
        d_all = jnp.concatenate([d_lo, d_hi], axis=0)
        dp_all = dot_last(v[lo], d_all).astype(BF).astype(F32)
        dp_c = dot_last(v[hi], d_hi).astype(BF).astype(F32)
        p_lo = jnp.concatenate([p_a.astype(BF), p_b.astype(BF)], axis=1)
        out_ref[lo, v0:v0 + HEAD_DIM] = dot_mid(p_lo, d_all).astype(BF)
        out_ref[hi, v0:v0 + HEAD_DIM] = dot_mid(p_c.astype(BF), d_hi).astype(BF)
        pd_a, pd_b, pd_c = p_a * dp_all[:, :n_lo], p_b * dp_all[:, n_lo:], p_c * dp_c
        t_lo = jnp.sum(pd_a, axis=0, keepdims=True)
        t_hi = jnp.sum(pd_b, axis=0, keepdims=True) + jnp.sum(pd_c, axis=0, keepdims=True)
        ds_a = (pd_a - p_a * t_lo).astype(BF)
        ds_b = (pd_b - p_b * t_hi).astype(BF)
        ds_c = (pd_c - p_c * t_hi).astype(BF)
        q_all = jnp.concatenate([q_lo, q_hi], axis=0)
        ds_all = jnp.concatenate([ds_a, ds_b], axis=1)
        d_rot[lo, k0:k0 + HEAD_DIM] = dot_mid(ds_all, q_all).astype(BF).astype(F32)
        d_rot[hi, k0:k0 + HEAD_DIM] = dot_mid(ds_c, q_hi).astype(BF).astype(F32)
        scale = HEAD_DIM ** -0.5
        dq_lo = (dot_first(ds_a, k[lo]) * scale).astype(BF).astype(F32)
        dq_hi = (dot_first(jnp.concatenate([ds_b, ds_c], axis=0), k) * scale).astype(BF).astype(F32)
        for j in range(3):
            h = 3 * g + j
            d_rot[lo, h * HEAD_DIM:(h + 1) * HEAD_DIM] = dq_lo[j * half:(j + 1) * half]
            d_rot[hi, h * HEAD_DIM:(h + 1) * HEAD_DIM] = dq_hi[j * half:(j + 1) * half]
    out_ref[:, QKV_COLS:] = jnp.zeros((seq_len, PACK_COLS - QKV_COLS), BF)
    low = low_lanes(seq_len)
    cos_all, sin_all = cos_ref[...], -sin_ref[...]
    for c in range(QK_COLS // LANES):
        at = slice(c * LANES, (c + 1) * LANES)
        out_ref[:, at] = turn(d_rot[:, at], cos_all, sin_all, low).astype(BF)
    d_h = dot_last(out_ref[...], pack_ref[...]).astype(BF).astype(F32)
    x = x_ref[...].astype(F32)
    inv = lax.rsqrt(jnp.mean(x * x, axis=-1, keepdims=True) + NORM_EPS)
    d_n = d_h * gain_ref[...]
    pull = jnp.mean(d_n * x, axis=-1, keepdims=True) * (inv * inv * inv)
    d_x_ref[...] = (d_resid + (d_n * inv - x * pull)).astype(BF)
    d_gain = jnp.sum(d_h * (x * inv), axis=0, keepdims=True)

    @pl.when(pl.program_id(0) == 0)
    def _():
        d_gain_ref[...] = jnp.zeros_like(d_gain_ref)

    d_gain_ref[...] += d_gain


def attend_back(rot, d_resid, emb, full_pack, full_out, gain_one, seq_len, tables):
    n_tok, dim = emb.shape
    return pl.pallas_call(
        attend_back_kernel,
        grid=(n_tok // seq_len,),
        in_specs=[whole((seq_len, LANES))] * 2
        + [by_seq((seq_len, QKV_COLS)), by_seq((1, dim, seq_len)), by_seq((seq_len, dim))]
        + [whole(full_pack.shape), whole(full_out.shape), whole((1, dim))],
        out_specs=[by_seq((seq_len, PACK_COLS)), by_seq((seq_len, dim)), whole((1, dim))],
        out_shape=[jax.ShapeDtypeStruct((n_tok, PACK_COLS), BF), jax.ShapeDtypeStruct((n_tok, dim), BF), jax.ShapeDtypeStruct((1, dim), F32)],
        scratch_shapes=[pltpu.VMEM((seq_len, QK_COLS), F32), pltpu.VMEM((seq_len, dim), BF)],
        compiler_params=params(40 * 1024 * 1024),
        cost_estimate=pl.CostEstimate(
            flops=10 * n_tok * seq_len * dim + 2 * n_tok * dim * (PACK_COLS + dim), bytes_accessed=14 * n_tok * dim,
            transcendentals=n_tok * seq_len * Q_HEADS),
        name="attend_back",
    )(*tables, rot, d_resid, emb, full_pack, full_out, gain_one.reshape(1, dim))


GATE_ROWS = 512
GATE_COLS = 256


def gate_kernel(h_ref, gate_ref, up_ref, d_act_ref, act_ref, d_gate_ref, d_up_ref):
    h = h_ref[...]
    for n in range(gate_ref.shape[1] // GATE_COLS):
        at = slice(n * GATE_COLS, (n + 1) * GATE_COLS)
        gate, up = dot_mid(h, gate_ref[:, at]), dot_mid(h, up_ref[:, at])
        d_act = d_act_ref[:, at].astype(F32)
        sig = jax.nn.sigmoid(gate)
        silu = gate * sig
        act_ref[:, at] = (silu * up).astype(BF)
        d_up_ref[:, at] = (d_act * silu).astype(BF)
        d_gate_ref[:, at] = (d_act * up * (sig + silu * (1.0 - sig))).astype(BF)


def gate_up(h_two, full_gate, full_up, d_act):
    n_tok, dim = h_two.shape
    ffn = full_gate.shape[1]
    tall = pl.BlockSpec((GATE_ROWS, ffn), lambda s: (s, 0))
    return pl.pallas_call(
        gate_kernel,
        grid=(n_tok // GATE_ROWS,),
        in_specs=[pl.BlockSpec((GATE_ROWS, dim), lambda s: (s, 0)), whole((dim, ffn)), whole((dim, ffn)), tall],
        out_specs=[tall] * 3,
        out_shape=[jax.ShapeDtypeStruct((n_tok, ffn), BF)] * 3,
        compiler_params=params(),
        cost_estimate=pl.CostEstimate(flops=4 * n_tok * dim * ffn, bytes_accessed=8 * n_tok * ffn, transcendentals=2 * n_tok * ffn),
        name="gate_up",
    )(h_two, full_gate, full_up, d_act)


def rms_norm(x_f32, gain_f32):
    inv_rms = lax.rsqrt(jnp.mean(x_f32 * x_f32, axis=-1, keepdims=True) + NORM_EPS)
    return (x_f32 * inv_rms * gain_f32).astype(BF)


def mm(a, b):
    return jnp.einsum("bsd,df->bsf", a, b, preferred_element_type=F32)


def mm_t(a, b):
    return jnp.einsum("bsf,df->bsd", a, b, preferred_element_type=F32)


def mm_w(a, b):
    return jnp.einsum("bsd,bsf->df", a, b, preferred_element_type=F32)


def row_major(x):
    return with_layout_constraint(x, Layout(major_to_minor=(0, 1)))


def from_peer(x, k):
    return lax.ppermute(x, AXIS_NAME, [(i, i ^ k) for i in range(N_DEV)]) if k else x


def owned_ids(token_ids, rows_dev, k):
    rel_ids = from_peer(token_ids, k).reshape(-1) - lax.axis_index(AXIS_NAME) * rows_dev
    return rel_ids, (rel_ids >= 0) & (rel_ids < rows_dev)


def slow_rows(token_ids, table):
    total = None
    for k in range(N_DEV):
        rel_ids, owned = owned_ids(token_ids, table.shape[0], k)
        picked = jnp.take(table, jnp.where(owned, rel_ids, 0), axis=0)
        part = from_peer(jnp.where(owned[:, None], picked, jnp.zeros((), BF)), k)
        total = part if total is None else total + part
    return total


def slow_grad(token_ids, d_emb, rows_dev):
    total = None
    for k in range(N_DEV):
        rel_ids, owned = owned_ids(token_ids, rows_dev, k)
        d_all = from_peer(d_emb, k).astype(F32)
        seg_ids = jnp.where(owned, rel_ids, rows_dev)
        part = jax.ops.segment_sum(d_all, seg_ids, num_segments=rows_dev)
        total = part if total is None else total + part
    return total.astype(BF)


def gather_all(shard):
    return lax.all_gather(shard, AXIS_NAME, axis=0, tiled=True)


def scatter_sum(partial):
    return lax.psum_scatter(partial, AXIS_NAME, scatter_dimension=0, tiled=True)


def solution(mesh):
    spec_1d = P(AXIS_NAME)
    spec_2d = P(AXIS_NAME, None)
    spec_3d = P(AXIS_NAME, None, None)
    in_specs = (spec_2d, spec_3d, spec_2d, spec_1d, spec_1d, spec_3d, spec_3d, spec_3d, spec_2d, spec_2d, spec_2d, spec_2d)
    out_specs = (spec_3d, spec_2d, spec_1d, spec_1d, spec_3d, spec_3d, spec_3d, spec_2d, spec_2d, spec_2d, spec_2d)

    def device_step(token_ids, grad_y, table, g_one, g_two, w_query, w_key, w_value, w_out, w_gate, w_up, w_down):
        rows_dev, dim = table.shape
        batch, seq_len = token_ids.shape
        n_tok = batch * seq_len
        rows_w = w_query.shape[0]

        pad = jnp.zeros((rows_w, PACK_COLS - QKV_COLS - 2), BF)
        shards = [w.reshape(rows_w, -1) for w in (w_query, w_key, w_value)]
        pack = jnp.concatenate(shards + [g_one[:, None], g_two[:, None], pad], axis=1)
        full_pack = gather_all(pack)
        full_down = gather_all(w_down)
        gain_one = full_pack[:, QKV_COLS].astype(F32)
        gain_two = full_pack[:, QKV_COLS + 1].astype(F32)

        slot, req, tok = route(token_ids.reshape(n_tok), rows_dev)
        asked = swap([req[k:k + 1] for k in range(N_DEV)])
        asked = jnp.concatenate(asked, axis=0)
        overflow = jnp.max(asked[:, CAP]) > 0
        asked = asked[:, :CAP]
        parts = swap(pick_rows(table, asked))
        d_act = mm_t(grad_y, full_down).astype(BF)
        parts, d_act, w_out, w_gate, w_up = lax.optimization_barrier((parts, d_act, w_out, w_gate, w_up))
        full_out = gather_all(w_out)
        full_gate = gather_all(w_gate)
        full_up = gather_all(w_up)
        emb, h_one = expand_rows(parts, slot.reshape(n_tok), gain_one)

        def slow_start():
            rows = slow_rows(token_ids, table)
            return rows, rms_norm(rows.astype(F32), gain_one)

        emb, h_one = lax.cond(overflow, slow_start, lambda: (emb, h_one))
        emb, h_one = row_major(emb), row_major(h_one)

        tables = rope_tables(seq_len)
        cube = (batch, seq_len, -1)
        rot, attn, resid_t, h_two, inv_t = attend(h_one, emb, full_pack, full_out, gain_two, seq_len, tables)
        attn = attn.reshape(cube)
        resid, inv_two = jnp.swapaxes(resid_t, 1, 2), jnp.swapaxes(inv_t, 1, 2)
        act, d_gate, d_up = (v.reshape(cube) for v in gate_up(h_two, full_gate, full_up, d_act.reshape(n_tok, -1)))
        h_two = h_two.reshape(cube)

        g_down = mm_w(act, grad_y)
        d_gate, d_up, g_down = lax.optimization_barrier((d_gate, d_up, g_down))
        sum_down = scatter_sum(g_down)
        g_gate, g_up = mm_w(h_two, d_gate), mm_w(h_two, d_up)
        d_gate, d_up, g_gate, g_up = lax.optimization_barrier((d_gate, d_up, g_gate, g_up))
        sum_gate, sum_up = scatter_sum(g_gate), scatter_sum(g_up)
        d_h_two = (mm_t(d_gate, full_gate) + mm_t(d_up, full_up)).astype(BF).astype(F32)
        resid_f32 = resid.astype(F32)
        d_n = d_h_two * gain_two
        pull = jnp.mean(d_n * resid_f32, axis=-1, keepdims=True) * (inv_two * inv_two * inv_two)
        d_gain_two = jnp.sum(d_h_two * (resid_f32 * inv_two), axis=(0, 1))
        d_resid = (grad_y.astype(F32) + (d_n * inv_two - resid_f32 * pull)).astype(BF)
        g_out = mm_w(attn, d_resid)
        d_resid, g_out, sum_down = lax.optimization_barrier((d_resid, g_out, sum_down))
        sum_out = scatter_sum(g_out)
        d_qkv, d_emb, d_gain_one = attend_back(rot, jnp.swapaxes(d_resid, 1, 2), emb, full_pack, full_out, gain_one, seq_len, tables)
        d_qkv, d_emb, sum_gate, sum_up = lax.optimization_barrier((d_qkv, d_emb, sum_gate, sum_up))
        g_pack = mm_w(h_one.reshape(cube), d_qkv.reshape(cube))
        gains = jnp.concatenate([d_gain_one.reshape(dim, 1), d_gain_two[:, None]], axis=1)
        g_pack = lax.dynamic_update_slice(g_pack, gains, (0, QKV_COLS))

        d_emb, slot, sum_out, g_pack = lax.optimization_barrier((d_emb, slot, sum_out, g_pack))
        sum_pack = scatter_sum(g_pack).astype(BF)
        many, ones = fold_rows(d_emb, slot, tok)
        act, resid, many, ones = lax.optimization_barrier((act, resid, many, ones))
        many, ones = swap(many), swap(ones)
        y_out = (resid.astype(F32) + mm(act, full_down)).astype(BF)
        d_table = spread_rows(many, ones, asked, rows_dev, dim)
        d_table, sum_pack, sum_out, sum_gate, sum_up, sum_down = lax.optimization_barrier(
            (d_table, sum_pack, sum_out, sum_gate, sum_up, sum_down))
        d_table = lax.cond(overflow, lambda: slow_grad(token_ids, d_emb, rows_dev), lambda: d_table)

        cols = [0, Q_HEADS * HEAD_DIM, QK_COLS, QKV_COLS]
        d_w = [sum_pack[:, a:b].reshape(rows_w, -1, HEAD_DIM) for a, b in zip(cols[:-1], cols[1:])]
        return (
            y_out, d_table, sum_pack[:, QKV_COLS], sum_pack[:, QKV_COLS + 1],
            d_w[0], d_w[1], d_w[2], sum_out.astype(BF), sum_gate.astype(BF), sum_up.astype(BF), sum_down.astype(BF),
        )

    return jax.shard_map(device_step, mesh=mesh, in_specs=in_specs, out_specs=out_specs, check_vma=False)
```

```python
import functools

import jax
import jax.numpy as jnp
from jax import lax
from jax.experimental import pallas as pl
from jax.experimental.pallas import tpu as pltpu
from jax.experimental.layout import Layout, with_layout_constraint
from jax.sharding import PartitionSpec as P


AXIS_NAME = "fsdp"
NORM_EPS = 1e-5
ROPE_THETA = 500000.0
N_DEV = 8
CAP_MANY = 80
CAP_ONE = 336
CAP = CAP_MANY + CAP_ONE
N_SLOT = N_DEV * CAP
REQ_COLS = 512
HEAD_DIM = 64
Q_HEADS = 15
KV_HEADS = 5
QK_COLS = (Q_HEADS + KV_HEADS) * HEAD_DIM
QKV_COLS = (Q_HEADS + 2 * KV_HEADS) * HEAD_DIM
PACK_COLS = 1664
LANES = 128
WIDE = 1024
VMEM_LIMIT = 60 * 1024 * 1024
BF = jnp.bfloat16
F32 = jnp.float32


def params(limit=VMEM_LIMIT):
    return pltpu.CompilerParams(vmem_limit_bytes=limit, dimension_semantics=("arbitrary",))


def route_kernel(rows_dev, me_ref, ids_ref, slot_ref, req_ref, tok_ref, col_a, col_b):
    n_tok = ids_ref.shape[1]
    tok_bits = n_tok.bit_length() - 1
    me = me_ref[0]
    big = jnp.int32(2**30)
    high, low = 65536, 65535

    def fill(col, row):
        for c in range(n_tok // LANES):
            part = jnp.broadcast_to(row[:, c * LANES:(c + 1) * LANES], (LANES, LANES))
            col[c * LANES:(c + 1) * LANES, :] = part.T

    ids = ids_ref[...]
    tok = lax.broadcasted_iota(jnp.int32, (1, n_tok), 1)
    fill(col_a, ids)
    wide = (8, LANES)
    unroll = 4

    def sweep(n_out, width, rows_of, steps):
        groups = width // LANES
        outs = []
        for g in range(n_out // width):
            rows = [rows_of(g * width + c * LANES) for c in range(groups)]
            accs = tuple(jnp.zeros(wide, jnp.int32) for _ in range(groups))
            for begin, end, step in steps(g):
                def body(i, accs, rows=rows, step=step):
                    for u in range(unroll):
                        accs = step(i * unroll + u, accs, rows)
                    return accs

                accs = lax.fori_loop(begin // (8 * unroll), end // (8 * unroll), body, accs)
            outs.extend(accs)
        return jnp.concatenate([jnp.sum(r, axis=0, keepdims=True) for r in outs], axis=1)

    def id_row(lane0):
        return jnp.broadcast_to(ids_ref[:, lane0:lane0 + LANES], wide)

    def block(i):
        return pl.ds(pl.multiple_of(i * 8, 8), 8)

    def same_steps(g):
        def step(i, accs, rows, weight):
            col = col_a[block(i), :]
            return tuple(acc + jnp.where(col == row, weight(i, c), 0) for c, (acc, row) in enumerate(zip(accs, rows)))

        def mixed(i, c):
            pos = i * 8 + lax.broadcasted_iota(jnp.int32, wide, 0)
            at = g * 1024 + c * LANES + lax.broadcasted_iota(jnp.int32, wide, 1)
            return jnp.where(pos < at, high + 1, 1)

        before = functools.partial(step, weight=lambda i, c: high + 1)
        after = functools.partial(step, weight=lambda i, c: 1)
        lo, hi = g * 1024, (g + 1) * 1024
        return [(0, lo, before), (lo, hi, functools.partial(step, weight=mixed)), (hi, n_tok, after)]

    same = sweep(n_tok, 1024, id_row, same_steps)
    first = same < high
    many = (same & low) > 1
    key = jnp.where(first, ids, big)
    count = jnp.where(many, 1, high)
    fill(col_a, count)
    fill(col_b, key)

    def rank_step(i, accs, rows):
        col, num = col_b[block(i), :], col_a[block(i), :]
        return tuple(acc + jnp.where(col < row, num, 0) for acc, row in zip(accs, rows))

    below = sweep(n_tok, 1024, id_row, lambda g: [(0, n_tok, rank_step)])
    owner = jnp.zeros_like(ids)
    start = jnp.zeros_like(ids)
    prev = jnp.zeros((1, 1), jnp.int32)
    over = jnp.zeros((1, 1), jnp.int32)
    for o in range(1, N_DEV + 1):
        base = jnp.sum(jnp.where(key < o * rows_dev, count, 0), axis=1, keepdims=True)
        held = base - prev
        full = jnp.logical_or((held >> 16) > CAP_ONE, (held & low) > CAP_MANY)
        over = jnp.where(full, 1, over)
        prev = base
        if o < N_DEV:
            past = ids >= o * rows_dev
            owner = jnp.where(past, o, owner)
            start = jnp.where(past, base, start)
    rank = below - start
    place = jnp.where(many, rank & low, CAP_MANY + (rank >> 16))
    fits = place < jnp.where(many, CAP_MANY, CAP)
    slot = (owner ^ me) * CAP + jnp.where(fits, place, 0)
    slot_ref[...] = slot
    fill(col_b, jnp.where(jnp.logical_and(first, fits), slot, -1))
    fill(col_a, (ids - owner * rows_dev) * n_tok + tok + 1)

    def req_step(i, accs, rows):
        col, val = col_b[block(i), :], col_a[block(i), :]
        return tuple(acc + jnp.where(col == row, val, 0) for acc, row in zip(accs, rows))

    lanes = lax.broadcasted_iota(jnp.int32, wide, 1)
    code = sweep(N_SLOT, 1664, lambda lane0: lane0 + lanes, lambda g: [(0, n_tok, req_step)])
    used = code > 0
    req = jnp.where(used, (code - 1) >> tok_bits, rows_dev)
    tok_ref[...] = jnp.where(used, (code - 1) & (n_tok - 1), 0)
    for k in range(N_DEV):
        req_ref[k:k + 1, :CAP] = req[:, k * CAP:(k + 1) * CAP]
        req_ref[k:k + 1, CAP:] = jnp.broadcast_to(over, (1, REQ_COLS - CAP))


def route(ids, rows_dev):
    n_tok = ids.shape[0]
    me = lax.axis_index(AXIS_NAME).astype(jnp.int32).reshape(1)
    vmem = pl.BlockSpec(memory_space=pltpu.VMEM)
    return pl.pallas_call(
        functools.partial(route_kernel, rows_dev),
        out_shape=(
            jax.ShapeDtypeStruct((1, n_tok), jnp.int32), jax.ShapeDtypeStruct((N_DEV, REQ_COLS), jnp.int32),
            jax.ShapeDtypeStruct((1, N_SLOT), jnp.int32)),
        in_specs=[pl.BlockSpec(memory_space=pltpu.SMEM), vmem],
        out_specs=(vmem, vmem, vmem),
        scratch_shapes=[pltpu.VMEM((n_tok, LANES), jnp.int32)] * 2,
        compiler_params=pltpu.CompilerParams(vmem_limit_bytes=16 * 1024 * 1024),
        name="route",
    )(me, ids.reshape(1, n_tok))


def swap(parts):
    out = [parts[0]]
    far = {k: lax.ppermute(parts[k], AXIS_NAME, [(i, i ^ k) for i in range(N_DEV)]) for k in range(N_DEV - 1, 0, -1)}
    return out + [far[k] for k in range(1, N_DEV)]


TILES = WIDE // LANES
ROW_UNROLL = 16
GATHER_CHUNK = 768


def strip(row0, n_rows, c):
    return pl.ds(row0 * TILES + c, n_rows, stride=TILES)


def row(r):
    return pl.ds(pl.multiple_of(r * TILES, TILES), TILES)


def to_rows(dst, row0, src, n_rows, dim):
    for c in range(TILES):
        n_lane = max(0, min(LANES, dim - c * LANES))
        part = src(c * LANES, n_lane).astype(F32)
        if n_lane < LANES:
            part = jnp.concatenate([part, jnp.zeros((n_rows, LANES - n_lane), F32)], axis=1)
        dst[strip(row0, n_rows, c), :] = part


def copy_rows(src, idx_ref, idx0, dst, n_rows):
    def body(i, carry):
        vals = [src[row(idx_ref[idx0 + i * ROW_UNROLL + u]), :] for u in range(ROW_UNROLL)]
        for u in range(ROW_UNROLL):
            dst[row(i * ROW_UNROLL + u), :] = vals[u]
        return carry

    lax.fori_loop(0, n_rows // ROW_UNROLL, body, 0)


def pick_kernel(idx_ref, tab_ref, *refs):
    outs, rows, stage = refs[:N_DEV], refs[N_DEV], refs[N_DEV + 1]
    step = pl.program_id(0)
    dim, n_rows = tab_ref.shape[0], rows.shape[0] // TILES
    n_load = n_rows // GATHER_CHUNK

    @pl.when(step < n_load)
    def _():
        for c in range(TILES):
            part = tab_ref[c * LANES:min((c + 1) * LANES, dim), :].astype(F32)
            if part.shape[0] < LANES:
                part = jnp.concatenate([part, jnp.zeros((LANES - part.shape[0], GATHER_CHUNK), F32)], axis=0)
            rows[strip(step * GATHER_CHUNK, GATHER_CHUNK, c), :] = part.T

    for k in range(N_DEV):
        @pl.when(step == n_load + k)
        def _(k=k):
            copy_rows(rows, idx_ref, k * CAP, stage, CAP)
            for c in range(TILES):
                outs[k][:, c * LANES:(c + 1) * LANES] = stage[strip(0, CAP, c), :].astype(BF)


def pick_rows(table, idx):
    rows_dev, dim = table.shape
    n_load = rows_dev // GATHER_CHUNK
    idx = jnp.minimum(idx.reshape(-1), rows_dev - 1)
    return pl.pallas_call(
        pick_kernel,
        grid_spec=pltpu.PrefetchScalarGridSpec(
            num_scalar_prefetch=1,
            grid=(n_load + N_DEV,),
            in_specs=[pl.BlockSpec((dim, GATHER_CHUNK), lambda s, _: (0, jnp.minimum(s, n_load - 1)))],
            out_specs=[pl.BlockSpec((CAP, WIDE), lambda s, _: (0, 0))] * N_DEV,
            scratch_shapes=[pltpu.VMEM((rows_dev * TILES, LANES), F32), pltpu.VMEM((CAP * TILES, LANES), F32)],
        ),
        out_shape=[jax.ShapeDtypeStruct((CAP, WIDE), BF)] * N_DEV,
        compiler_params=params(),
        cost_estimate=pl.CostEstimate(flops=10**9, bytes_accessed=2 * rows_dev * dim, transcendentals=0),
        name="pick_rows",
    )(idx, table.T)


EXPAND_ROWS = 512


def expand_kernel(idx_ref, gain_ref, *refs):
    parts, e_ref, h_ref, rows, stage = refs[:N_DEV], *refs[N_DEV:]
    step = pl.program_id(0)
    dim = e_ref.shape[1]

    @pl.when(step == 0)
    def _():
        for k in range(N_DEV):
            to_rows(rows, k * CAP, lambda at, n, k=k: parts[k][:, at:at + n], CAP, WIDE)

    copy_rows(rows, idx_ref, step * EXPAND_ROWS, stage, EXPAND_ROWS)
    x = jnp.concatenate([stage[strip(0, EXPAND_ROWS, c), :] for c in range(TILES)], axis=1)[:, :dim]
    e_ref[...] = x.astype(BF)
    inv = lax.rsqrt(jnp.mean(x * x, axis=-1, keepdims=True) + NORM_EPS)
    h_ref[...] = (x * inv * gain_ref[...]).astype(BF)


def expand_rows(parts, slot, gain):
    n_tok, dim = slot.shape[0], gain.shape[0]
    return pl.pallas_call(
        expand_kernel,
        grid_spec=pltpu.PrefetchScalarGridSpec(
            num_scalar_prefetch=1,
            grid=(n_tok // EXPAND_ROWS,),
            in_specs=[pl.BlockSpec((1, dim), lambda s, _: (0, 0))] + [pl.BlockSpec((CAP, WIDE), lambda s, _: (0, 0))] * N_DEV,
            out_specs=[pl.BlockSpec((EXPAND_ROWS, dim), lambda s, _: (s, 0))] * 2,
            scratch_shapes=[pltpu.VMEM((N_SLOT * TILES, LANES), F32), pltpu.VMEM((EXPAND_ROWS * TILES, LANES), F32)],
        ),
        out_shape=[jax.ShapeDtypeStruct((n_tok, dim), BF)] * 2,
        compiler_params=params(),
        name="expand_rows",
    )(slot, gain.reshape(1, dim), *parts)


def fold_kernel(tok_ref, slot_ref, d_ref, *refs):
    many, ones, rows, stage = refs[:N_DEV], refs[N_DEV:2 * N_DEV], refs[2 * N_DEV], refs[2 * N_DEV + 1]
    n_tok, dim = d_ref.shape
    step = pl.program_id(0)
    half = N_DEV // 2
    width = 1024
    chunk = 512

    @pl.when(step == 0)
    def _():
        for b in range(n_tok // chunk):
            to_rows(rows, b * chunk, lambda at, n, b=b: d_ref[b * chunk:(b + 1) * chunk, at:at + n], chunk, dim)

    for part in range(2):
        @pl.when(step == part)
        def _(part=part):
            total = None
            for c in range(n_tok // width):
                hot = []
                for k in range(part * half, (part + 1) * half):
                    ids = jnp.broadcast_to(slot_ref[:, c * width:(c + 1) * width], (CAP_MANY, width))
                    mine = k * CAP + lax.broadcasted_iota(jnp.int32, (CAP_MANY, width), 0)
                    hot.append(jnp.where(ids == mine, 1.0, 0.0).astype(BF))
                term = jnp.dot(jnp.concatenate(hot, axis=0), d_ref[c * width:(c + 1) * width, :], preferred_element_type=F32)
                total = term if total is None else total + term
            for j in range(half):
                out = many[part * half + j]
                out[:, :dim] = total[j * CAP_MANY:(j + 1) * CAP_MANY]
                out[:, dim:] = jnp.zeros((CAP_MANY, WIDE - dim), F32)

    for k in range(N_DEV):
        @pl.when(step == 2 + k)
        def _(k=k):
            copy_rows(rows, tok_ref, k * CAP + CAP_MANY, stage, CAP_ONE)
            for c in range(TILES):
                ones[k][:, c * LANES:(c + 1) * LANES] = stage[strip(0, CAP_ONE, c), :].astype(BF)


def fold_rows(d_emb, slot, tok):
    n_tok, dim = d_emb.shape
    out = pl.pallas_call(
        fold_kernel,
        grid_spec=pltpu.PrefetchScalarGridSpec(
            num_scalar_prefetch=1,
            grid=(2 + N_DEV,),
            in_specs=[pl.BlockSpec((1, n_tok), lambda s, _: (0, 0)), pl.BlockSpec((n_tok, dim), lambda s, _: (0, 0))],
            out_specs=[pl.BlockSpec((CAP_MANY, WIDE), lambda s, _: (0, 0))] * N_DEV + [pl.BlockSpec((CAP_ONE, WIDE), lambda s, _: (0, 0))] * N_DEV,
            scratch_shapes=[pltpu.VMEM((n_tok * TILES, LANES), F32), pltpu.VMEM((CAP_ONE * TILES, LANES), F32)],
        ),
        out_shape=[jax.ShapeDtypeStruct((CAP_MANY, WIDE), F32)] * N_DEV + [jax.ShapeDtypeStruct((CAP_ONE, WIDE), BF)] * N_DEV,
        compiler_params=params(),
        cost_estimate=pl.CostEstimate(flops=2 * N_DEV * CAP_MANY * n_tok * dim, bytes_accessed=4 * N_SLOT * dim, transcendentals=0),
        name="fold_rows",
    )(tok.reshape(-1), slot, d_emb)
    return out[:N_DEV], out[N_DEV:]


ADD_UNROLL = 8


def spread_kernel(rows_dev, idx_ref, *refs):
    many, ones, out_ref, total, stage = refs[:N_DEV], refs[N_DEV:2 * N_DEV], *refs[2 * N_DEV:]
    step = pl.program_id(0)

    @pl.when(step == 0)
    def _():
        total[...] = jnp.zeros_like(total)

    for k in range(N_DEV):
        @pl.when(step == k)
        def _(k=k):
            to_rows(stage, 0, lambda at, n: many[k][:, at:at + n], CAP_MANY, WIDE)
            to_rows(stage, CAP_MANY, lambda at, n: ones[k][:, at:at + n], CAP_ONE, WIDE)

            def body(i, carry):
                rows = [idx_ref[k * CAP + i * ADD_UNROLL + u] for u in range(ADD_UNROLL)]
                sums = [total[row(rows[u]), :] + stage[row(i * ADD_UNROLL + u), :] for u in range(ADD_UNROLL)]
                for u in range(ADD_UNROLL):
                    total[row(rows[u]), :] = sums[u]
                return carry

            lax.fori_loop(0, CAP // ADD_UNROLL, body, 0)

    @pl.when(step >= N_DEV)
    def _():
        at = (step - N_DEV) * GATHER_CHUNK
        dim = out_ref.shape[0]
        for c in range(TILES):
            n_lane = min(LANES, dim - c * LANES)
            part = total[strip(at, GATHER_CHUNK, c), :].T
            out_ref[c * LANES:c * LANES + n_lane, :] = part[:n_lane].astype(BF)


def spread_rows(many, ones, idx, rows_dev, dim):
    n_out = rows_dev // GATHER_CHUNK
    return pl.pallas_call(
        functools.partial(spread_kernel, rows_dev),
        grid_spec=pltpu.PrefetchScalarGridSpec(
            num_scalar_prefetch=1,
            grid=(N_DEV + n_out,),
            in_specs=[pl.BlockSpec((CAP_MANY, WIDE), lambda s, _: (0, 0))] * N_DEV + [pl.BlockSpec((CAP_ONE, WIDE), lambda s, _: (0, 0))] * N_DEV,
            out_specs=pl.BlockSpec((dim, GATHER_CHUNK), lambda s, _: (0, jnp.maximum(s - N_DEV, 0))),
            scratch_shapes=[pltpu.VMEM(((rows_dev + 8) * TILES, LANES), F32), pltpu.VMEM((CAP * TILES, LANES), F32)],
        ),
        out_shape=jax.ShapeDtypeStruct((dim, rows_dev), BF),
        compiler_params=params(),
        name="spread_rows",
    )(idx.reshape(-1), *many, *ones).T


def rope_tables(seq_len):
    half = HEAD_DIM // 2
    inv_freq = ROPE_THETA ** (-2.0 * jnp.arange(half, dtype=F32) / HEAD_DIM)
    angles = jnp.arange(seq_len, dtype=F32)[:, None] * inv_freq[None, :]
    cos_tab, sin_tab = jnp.cos(angles), jnp.sin(angles)
    cos_all = jnp.concatenate([cos_tab] * 4, axis=1)
    sin_all = jnp.concatenate([-sin_tab, sin_tab] * 2, axis=1)
    return cos_all, sin_all


def turn(x, cos_all, sin_all, low):
    other = jnp.where(low, pltpu.roll(x, LANES - HEAD_DIM // 2, 1), pltpu.roll(x, HEAD_DIM // 2, 1))
    return x * cos_all + other * sin_all


def low_lanes(seq_len):
    lane = lax.broadcasted_iota(jnp.int32, (seq_len, LANES), 1)
    return lax.rem(lane, HEAD_DIM) < HEAD_DIM // 2


CONTRACT_LAST = (((1,), (1,)), ((), ()))
CONTRACT_FIRST = (((0,), (0,)), ((), ()))


def lanes_of(ref, at, first_head):
    return jnp.concatenate([ref[at, h * HEAD_DIM:(h + 1) * HEAD_DIM] for h in range(first_head, first_head + 3)], axis=0)


def hidden(half):
    key = lax.broadcasted_iota(jnp.int32, (half, 3 * half), 0)
    query = lax.rem(lax.broadcasted_iota(jnp.int32, (half, 3 * half), 1), half)
    return key > query


def dot_last(a, b):
    return lax.dot_general(a, b, CONTRACT_LAST, preferred_element_type=F32)


def dot_first(a, b):
    return lax.dot_general(a, b, CONTRACT_FIRST, preferred_element_type=F32)


def dot_mid(a, b):
    return jnp.dot(a, b, preferred_element_type=F32)


def scores(q_lo, q_hi, k):
    half = k.shape[0] // 2
    return dot_last(k[:half], jnp.concatenate([q_lo, q_hi], axis=0)), dot_last(k[half:], q_hi)


def probabilities(s_all, s_c, mask):
    n_lo = s_c.shape[1]
    s_a = jnp.where(mask, -1e30, s_all[:, :n_lo])
    s_b = s_all[:, n_lo:]
    s_c = jnp.where(mask, -1e30, s_c)
    m_lo = jnp.max(s_a, axis=0, keepdims=True)
    m_hi = jnp.maximum(jnp.max(s_b, axis=0, keepdims=True), jnp.max(s_c, axis=0, keepdims=True))
    p_a, p_b, p_c = jnp.exp(s_a - m_lo), jnp.exp(s_b - m_hi), jnp.exp(s_c - m_hi)
    inv_lo = 1.0 / jnp.sum(p_a, axis=0, keepdims=True)
    inv_hi = 1.0 / (jnp.sum(p_b, axis=0, keepdims=True) + jnp.sum(p_c, axis=0, keepdims=True))
    return p_a * inv_lo, p_b * inv_hi, p_c * inv_hi


def group_keys(rot_ref, g):
    k0, v0 = (Q_HEADS + g) * HEAD_DIM, QK_COLS + g * HEAD_DIM
    return rot_ref[:, k0:k0 + HEAD_DIM], rot_ref[:, v0:v0 + HEAD_DIM]


def attend_kernel(cos_ref, sin_ref, h_ref, x_ref, pack_ref, wo_ref, gain_ref, rot_ref, out_ref, res_ref, h_two_ref, inv_ref, qkv):
    seq_len = h_ref.shape[0]
    low = low_lanes(seq_len)
    cos_all, sin_all = cos_ref[...], sin_ref[...]
    scale_q = Q_HEADS * HEAD_DIM
    qkv[...] = dot_mid(h_ref[...], pack_ref[...])
    for c in range(QK_COLS // LANES):
        x = turn(qkv[:, c * LANES:(c + 1) * LANES], cos_all, sin_all, low)
        col = c * LANES + lax.broadcasted_iota(jnp.int32, x.shape, 1)
        if (c + 1) * LANES <= scale_q:
            x = x * HEAD_DIM ** -0.5
        elif c * LANES < scale_q:
            x = jnp.where(col < scale_q, x * HEAD_DIM ** -0.5, x)
        rot_ref[:, c * LANES:(c + 1) * LANES] = x.astype(BF)
    rot_ref[:, QK_COLS:] = qkv[:, QK_COLS:QKV_COLS].astype(BF)
    half = seq_len // 2
    lo, hi = slice(0, half), slice(half, seq_len)
    mask = hidden(half)

    def products(g):
        k, v = group_keys(rot_ref, g)
        return v, scores(lanes_of(rot_ref, lo, 3 * g), lanes_of(rot_ref, hi, 3 * g), k)

    ahead = products(0)
    for g in range(KV_HEADS):
        v, (s_all, s_c) = ahead
        if g + 1 < KV_HEADS:
            ahead = products(g + 1)
        p_a, p_b, p_c = probabilities(s_all, s_c, mask)
        o_lo = dot_first(p_a.astype(BF), v[lo]).astype(BF)
        o_hi = dot_first(jnp.concatenate([p_b.astype(BF), p_c.astype(BF)], axis=0), v).astype(BF)
        for j in range(3):
            h = 3 * g + j
            out_ref[lo, h * HEAD_DIM:(h + 1) * HEAD_DIM] = o_lo[j * half:(j + 1) * half]
            out_ref[hi, h * HEAD_DIM:(h + 1) * HEAD_DIM] = o_hi[j * half:(j + 1) * half]
    s = (x_ref[...].astype(F32) + dot_mid(out_ref[...], wo_ref[...])).astype(BF).astype(F32)
    h_two_ref[...] = (s * lax.rsqrt(jnp.mean(s * s, axis=-1, keepdims=True) + NORM_EPS) * gain_ref[...]).astype(BF)
    s = s.T
    res_ref[0] = s.astype(BF)
    inv_ref[0] = lax.rsqrt(jnp.mean(s * s, axis=0, keepdims=True) + NORM_EPS)


def whole(shape):
    return pl.BlockSpec(shape, lambda s: (0,) * len(shape))


def by_seq(shape):
    return pl.BlockSpec(shape, lambda s: (s,) + (0,) * (len(shape) - 1))


def attend(h_one, emb, full_pack, full_out, gain_two, seq_len, tables):
    n_tok, dim = emb.shape
    batch = n_tok // seq_len
    cube = (1, dim, seq_len)
    return pl.pallas_call(
        attend_kernel,
        grid=(batch,),
        in_specs=[whole((seq_len, LANES))] * 2 + [by_seq((seq_len, dim))] * 2 + [whole(full_pack.shape), whole(full_out.shape), whole((1, dim))],
        out_specs=[by_seq((seq_len, QKV_COLS)), by_seq((seq_len, dim)), by_seq(cube), by_seq((seq_len, dim)), by_seq((1, 1, seq_len))],
        out_shape=[
            jax.ShapeDtypeStruct((n_tok, QKV_COLS), BF), jax.ShapeDtypeStruct((n_tok, dim), BF),
            jax.ShapeDtypeStruct((batch, dim, seq_len), BF), jax.ShapeDtypeStruct((n_tok, dim), BF),
            jax.ShapeDtypeStruct((batch, 1, seq_len), F32),
        ],
        scratch_shapes=[pltpu.VMEM((seq_len, PACK_COLS), F32)],
        compiler_params=params(40 * 1024 * 1024),
        cost_estimate=pl.CostEstimate(
            flops=4 * n_tok * seq_len * dim + 2 * n_tok * dim * (PACK_COLS + dim), bytes_accessed=14 * n_tok * dim,
            transcendentals=n_tok * seq_len * Q_HEADS),
        name="attend",
    )(*tables, h_one, emb, full_pack, full_out, gain_two.reshape(1, dim))


def attend_back_kernel(cos_ref, sin_ref, rot_ref, d_res_ref, x_ref, pack_ref, wo_ref, gain_ref, out_ref, d_x_ref, d_gain_ref, d_rot, d_ref):
    seq_len = rot_ref.shape[0]
    d_resid = d_res_ref[0].astype(F32).T
    d_ref[...] = dot_last(d_resid.astype(BF), wo_ref[...]).astype(BF)
    scale_q = Q_HEADS * HEAD_DIM
    half = seq_len // 2
    lo, hi = slice(0, half), slice(half, seq_len)
    mask = hidden(half)

    def products(g):
        k, v = group_keys(rot_ref, g)
        q_lo, q_hi = lanes_of(rot_ref, lo, 3 * g), lanes_of(rot_ref, hi, 3 * g)
        d_lo, d_hi = lanes_of(d_ref, lo, 3 * g), lanes_of(d_ref, hi, 3 * g)
        return k, q_lo, q_hi, d_lo, d_hi, scores(q_lo, q_hi, k), scores(d_lo, d_hi, v)

    ahead = products(0)
    for g in range(KV_HEADS):
        k0, v0 = scale_q + g * HEAD_DIM, QK_COLS + g * HEAD_DIM
        k, q_lo, q_hi, d_lo, d_hi, (s_all, s_c), (dp_all, dp_c) = ahead
        if g + 1 < KV_HEADS:
            ahead = products(g + 1)
        n_lo = q_lo.shape[0]
        p_a, p_b, p_c = probabilities(s_all, s_c, mask)
        d_all = jnp.concatenate([d_lo, d_hi], axis=0)
        dp_all, dp_c = dp_all.astype(BF).astype(F32), dp_c.astype(BF).astype(F32)
        p_lo = jnp.concatenate([p_a.astype(BF), p_b.astype(BF)], axis=1)
        out_ref[lo, v0:v0 + HEAD_DIM] = dot_mid(p_lo, d_all).astype(BF)
        out_ref[hi, v0:v0 + HEAD_DIM] = dot_mid(p_c.astype(BF), d_hi).astype(BF)
        pd_a, pd_b, pd_c = p_a * dp_all[:, :n_lo], p_b * dp_all[:, n_lo:], p_c * dp_c
        t_lo = jnp.sum(pd_a, axis=0, keepdims=True)
        t_hi = jnp.sum(pd_b, axis=0, keepdims=True) + jnp.sum(pd_c, axis=0, keepdims=True)
        ds_a = (pd_a - p_a * t_lo).astype(BF)
        ds_b = (pd_b - p_b * t_hi).astype(BF)
        ds_c = (pd_c - p_c * t_hi).astype(BF)
        q_all = jnp.concatenate([q_lo, q_hi], axis=0)
        ds_all = jnp.concatenate([ds_a, ds_b], axis=1)
        d_rot[lo, k0:k0 + HEAD_DIM] = dot_mid(ds_all, q_all).astype(BF).astype(F32)
        d_rot[hi, k0:k0 + HEAD_DIM] = dot_mid(ds_c, q_hi).astype(BF).astype(F32)
        scale = HEAD_DIM ** -0.5
        dq_lo = (dot_first(ds_a, k[lo]) * scale).astype(BF).astype(F32)
        dq_hi = (dot_first(jnp.concatenate([ds_b, ds_c], axis=0), k) * scale).astype(BF).astype(F32)
        for j in range(3):
            h = 3 * g + j
            d_rot[lo, h * HEAD_DIM:(h + 1) * HEAD_DIM] = dq_lo[j * half:(j + 1) * half]
            d_rot[hi, h * HEAD_DIM:(h + 1) * HEAD_DIM] = dq_hi[j * half:(j + 1) * half]
    out_ref[:, QKV_COLS:] = jnp.zeros((seq_len, PACK_COLS - QKV_COLS), BF)
    low = low_lanes(seq_len)
    cos_all, sin_all = cos_ref[...], -sin_ref[...]
    for c in range(QK_COLS // LANES):
        at = slice(c * LANES, (c + 1) * LANES)
        out_ref[:, at] = turn(d_rot[:, at], cos_all, sin_all, low).astype(BF)
    d_h = dot_last(out_ref[...], pack_ref[...]).astype(BF).astype(F32)
    x = x_ref[...].astype(F32)
    inv = lax.rsqrt(jnp.mean(x * x, axis=-1, keepdims=True) + NORM_EPS)
    d_n = d_h * gain_ref[...]
    pull = jnp.mean(d_n * x, axis=-1, keepdims=True) * (inv * inv * inv)
    d_x_ref[...] = (d_resid + (d_n * inv - x * pull)).astype(BF)
    d_gain = jnp.sum(d_h * (x * inv), axis=0, keepdims=True)

    @pl.when(pl.program_id(0) == 0)
    def _():
        d_gain_ref[...] = jnp.zeros_like(d_gain_ref)

    d_gain_ref[...] += d_gain


def attend_back(rot, d_resid, emb, full_pack, full_out, gain_one, seq_len, tables):
    n_tok, dim = emb.shape
    return pl.pallas_call(
        attend_back_kernel,
        grid=(n_tok // seq_len,),
        in_specs=[whole((seq_len, LANES))] * 2
        + [by_seq((seq_len, QKV_COLS)), by_seq((1, dim, seq_len)), by_seq((seq_len, dim))]
        + [whole(full_pack.shape), whole(full_out.shape), whole((1, dim))],
        out_specs=[by_seq((seq_len, PACK_COLS)), by_seq((seq_len, dim)), whole((1, dim))],
        out_shape=[jax.ShapeDtypeStruct((n_tok, PACK_COLS), BF), jax.ShapeDtypeStruct((n_tok, dim), BF), jax.ShapeDtypeStruct((1, dim), F32)],
        scratch_shapes=[pltpu.VMEM((seq_len, QK_COLS), F32), pltpu.VMEM((seq_len, dim), BF)],
        compiler_params=params(40 * 1024 * 1024),
        cost_estimate=pl.CostEstimate(
            flops=10 * n_tok * seq_len * dim + 2 * n_tok * dim * (PACK_COLS + dim), bytes_accessed=14 * n_tok * dim,
            transcendentals=n_tok * seq_len * Q_HEADS),
        name="attend_back",
    )(*tables, rot, d_resid, emb, full_pack, full_out, gain_one.reshape(1, dim))


GATE_ROWS = 512
GATE_COLS = 256


def gate_kernel(h_ref, gate_ref, up_ref, d_act_ref, act_ref, d_gate_ref, d_up_ref):
    h = h_ref[...]
    for n in range(gate_ref.shape[1] // GATE_COLS):
        at = slice(n * GATE_COLS, (n + 1) * GATE_COLS)
        gate, up = dot_mid(h, gate_ref[:, at]), dot_mid(h, up_ref[:, at])
        d_act = d_act_ref[:, at].astype(F32)
        sig = jax.nn.sigmoid(gate)
        silu = gate * sig
        act_ref[:, at] = (silu * up).astype(BF)
        d_up_ref[:, at] = (d_act * silu).astype(BF)
        d_gate_ref[:, at] = (d_act * up * (sig + silu * (1.0 - sig))).astype(BF)


def gate_up(h_two, full_gate, full_up, d_act):
    n_tok, dim = h_two.shape
    ffn = full_gate.shape[1]
    tall = pl.BlockSpec((GATE_ROWS, ffn), lambda s: (s, 0))
    return pl.pallas_call(
        gate_kernel,
        grid=(n_tok // GATE_ROWS,),
        in_specs=[pl.BlockSpec((GATE_ROWS, dim), lambda s: (s, 0)), whole((dim, ffn)), whole((dim, ffn)), tall],
        out_specs=[tall] * 3,
        out_shape=[jax.ShapeDtypeStruct((n_tok, ffn), BF)] * 3,
        compiler_params=params(),
        cost_estimate=pl.CostEstimate(flops=4 * n_tok * dim * ffn, bytes_accessed=8 * n_tok * ffn, transcendentals=2 * n_tok * ffn),
        name="gate_up",
    )(h_two, full_gate, full_up, d_act)


def rms_norm(x_f32, gain_f32):
    inv_rms = lax.rsqrt(jnp.mean(x_f32 * x_f32, axis=-1, keepdims=True) + NORM_EPS)
    return (x_f32 * inv_rms * gain_f32).astype(BF)


def mm(a, b):
    return jnp.einsum("bsd,df->bsf", a, b, preferred_element_type=F32)


def mm_t(a, b):
    return jnp.einsum("bsf,df->bsd", a, b, preferred_element_type=F32)


def mm_w(a, b):
    return jnp.einsum("bsd,bsf->df", a, b, preferred_element_type=F32)


def row_major(x):
    return with_layout_constraint(x, Layout(major_to_minor=(0, 1)))


def from_peer(x, k):
    return lax.ppermute(x, AXIS_NAME, [(i, i ^ k) for i in range(N_DEV)]) if k else x


def owned_ids(token_ids, rows_dev, k):
    rel_ids = from_peer(token_ids, k).reshape(-1) - lax.axis_index(AXIS_NAME) * rows_dev
    return rel_ids, (rel_ids >= 0) & (rel_ids < rows_dev)


def slow_rows(token_ids, table):
    total = None
    for k in range(N_DEV):
        rel_ids, owned = owned_ids(token_ids, table.shape[0], k)
        picked = jnp.take(table, jnp.where(owned, rel_ids, 0), axis=0)
        part = from_peer(jnp.where(owned[:, None], picked, jnp.zeros((), BF)), k)
        total = part if total is None else total + part
    return total


def slow_grad(token_ids, d_emb, rows_dev):
    total = None
    for k in range(N_DEV):
        rel_ids, owned = owned_ids(token_ids, rows_dev, k)
        d_all = from_peer(d_emb, k).astype(F32)
        seg_ids = jnp.where(owned, rel_ids, rows_dev)
        part = jax.ops.segment_sum(d_all, seg_ids, num_segments=rows_dev)
        total = part if total is None else total + part
    return total.astype(BF)


def gather_all(shard):
    return lax.all_gather(shard, AXIS_NAME, axis=0, tiled=True)


def scatter_sum(partial):
    return lax.psum_scatter(partial, AXIS_NAME, scatter_dimension=0, tiled=True)


def solution(mesh):
    spec_1d = P(AXIS_NAME)
    spec_2d = P(AXIS_NAME, None)
    spec_3d = P(AXIS_NAME, None, None)
    in_specs = (spec_2d, spec_3d, spec_2d, spec_1d, spec_1d, spec_3d, spec_3d, spec_3d, spec_2d, spec_2d, spec_2d, spec_2d)
    out_specs = (spec_3d, spec_2d, spec_1d, spec_1d, spec_3d, spec_3d, spec_3d, spec_2d, spec_2d, spec_2d, spec_2d)

    def device_step(token_ids, grad_y, table, g_one, g_two, w_query, w_key, w_value, w_out, w_gate, w_up, w_down):
        rows_dev, dim = table.shape
        batch, seq_len = token_ids.shape
        n_tok = batch * seq_len
        rows_w = w_query.shape[0]

        pad = jnp.zeros((rows_w, PACK_COLS - QKV_COLS - 2), BF)
        shards = [w.reshape(rows_w, -1) for w in (w_query, w_key, w_value)]
        pack = jnp.concatenate(shards + [g_one[:, None], g_two[:, None], pad], axis=1)
        full_pack = gather_all(pack)
        full_down = gather_all(w_down)
        gain_one = full_pack[:, QKV_COLS].astype(F32)
        gain_two = full_pack[:, QKV_COLS + 1].astype(F32)

        slot, req, tok = route(token_ids.reshape(n_tok), rows_dev)
        asked = swap([req[k:k + 1] for k in range(N_DEV)])
        asked = jnp.concatenate(asked, axis=0)
        overflow = jnp.max(asked[:, CAP]) > 0
        asked = asked[:, :CAP]
        parts = swap(pick_rows(table, asked))
        d_act = mm_t(grad_y, full_down).astype(BF)
        parts, d_act, w_out, w_gate, w_up = lax.optimization_barrier((parts, d_act, w_out, w_gate, w_up))
        full_out = gather_all(w_out)
        full_gate = gather_all(w_gate)
        full_up = gather_all(w_up)

        def slow_start():
            rows = slow_rows(token_ids, table)
            return rows, rms_norm(rows.astype(F32), gain_one)

        emb, h_one = lax.cond(overflow, slow_start, lambda: tuple(expand_rows(parts, slot.reshape(n_tok), gain_one)))
        emb, h_one = row_major(emb), row_major(h_one)

        tables = rope_tables(seq_len)
        cube = (batch, seq_len, -1)
        rot, attn, resid_t, h_two, inv_t = attend(h_one, emb, full_pack, full_out, gain_two, seq_len, tables)
        attn = attn.reshape(cube)
        resid, inv_two = jnp.swapaxes(resid_t, 1, 2), jnp.swapaxes(inv_t, 1, 2)
        act, d_gate, d_up = (v.reshape(cube) for v in gate_up(h_two, full_gate, full_up, d_act.reshape(n_tok, -1)))
        h_two = h_two.reshape(cube)

        g_down = mm_w(act, grad_y)
        d_gate, d_up, g_down = lax.optimization_barrier((d_gate, d_up, g_down))
        sum_down = scatter_sum(g_down)
        g_gate, g_up = mm_w(h_two, d_gate), mm_w(h_two, d_up)
        d_gate, d_up, g_gate, g_up = lax.optimization_barrier((d_gate, d_up, g_gate, g_up))
        sum_gate, sum_up = scatter_sum(g_gate), scatter_sum(g_up)
        d_h_two = (mm_t(d_gate, full_gate) + mm_t(d_up, full_up)).astype(BF).astype(F32)
        resid_f32 = resid.astype(F32)
        d_n = d_h_two * gain_two
        pull = jnp.mean(d_n * resid_f32, axis=-1, keepdims=True) * (inv_two * inv_two * inv_two)
        d_gain_two = jnp.sum(d_h_two * (resid_f32 * inv_two), axis=(0, 1))
        d_resid = (grad_y.astype(F32) + (d_n * inv_two - resid_f32 * pull)).astype(BF)
        g_out = mm_w(attn, d_resid)
        d_resid, g_out, sum_down = lax.optimization_barrier((d_resid, g_out, sum_down))
        sum_out = scatter_sum(g_out)
        d_qkv, d_emb, d_gain_one = attend_back(rot, jnp.swapaxes(d_resid, 1, 2), emb, full_pack, full_out, gain_one, seq_len, tables)
        d_qkv, d_emb, sum_gate, sum_up = lax.optimization_barrier((d_qkv, d_emb, sum_gate, sum_up))

        d_emb, slot, sum_out = lax.optimization_barrier((d_emb, slot, sum_out))
        many, ones = fold_rows(d_emb, slot, tok)
        act, resid, many, ones = lax.optimization_barrier((act, resid, many, ones))
        many, ones = swap(many), swap(ones)
        y_out = (resid.astype(F32) + mm(act, full_down)).astype(BF)
        d_qkv, many, y_out = lax.optimization_barrier((d_qkv, many, y_out))
        g_pack = mm_w(h_one.reshape(cube), d_qkv.reshape(cube))
        gains = jnp.concatenate([d_gain_one.reshape(dim, 1), d_gain_two[:, None]], axis=1)
        g_pack = lax.dynamic_update_slice(g_pack, gains, (0, QKV_COLS))
        sum_pack = scatter_sum(g_pack).astype(BF)
        many, ones, _ = lax.optimization_barrier((many, ones, g_pack))
        d_table = spread_rows(many, ones, asked, rows_dev, dim)
        d_table, sum_pack, sum_out, sum_gate, sum_up, sum_down = lax.optimization_barrier(
            (d_table, sum_pack, sum_out, sum_gate, sum_up, sum_down))
        d_table = lax.cond(overflow, lambda: slow_grad(token_ids, d_emb, rows_dev), lambda: d_table)

        cols = [0, Q_HEADS * HEAD_DIM, QK_COLS, QKV_COLS]
        d_w = [sum_pack[:, a:b].reshape(rows_w, -1, HEAD_DIM) for a, b in zip(cols[:-1], cols[1:])]
        return (
            y_out, d_table, sum_pack[:, QKV_COLS], sum_pack[:, QKV_COLS + 1],
            d_w[0], d_w[1], d_w[2], sum_out.astype(BF), sum_gate.astype(BF), sum_up.astype(BF), sum_down.astype(BF),
        )

    return jax.shard_map(device_step, mesh=mesh, in_specs=in_specs, out_specs=out_specs, check_vma=False)
```

```python
import functools

import jax
import jax.numpy as jnp
from jax import lax
from jax.experimental import pallas as pl
from jax.experimental.pallas import tpu as pltpu
from jax.experimental.layout import Layout, with_layout_constraint
from jax.sharding import PartitionSpec as P


AXIS_NAME = "fsdp"
NORM_EPS = 1e-5
ROPE_THETA = 500000.0
N_DEV = 8
CAP_MANY = 80
CAP_ONE = 336
CAP = CAP_MANY + CAP_ONE
N_SLOT = N_DEV * CAP
REQ_COLS = 512
HEAD_DIM = 64
Q_HEADS = 15
KV_HEADS = 5
QK_COLS = (Q_HEADS + KV_HEADS) * HEAD_DIM
QKV_COLS = (Q_HEADS + 2 * KV_HEADS) * HEAD_DIM
PACK_COLS = 1664
LANES = 128
WIDE = 1024
VMEM_LIMIT = 60 * 1024 * 1024
BF = jnp.bfloat16
F32 = jnp.float32


def params(limit=VMEM_LIMIT):
    return pltpu.CompilerParams(vmem_limit_bytes=limit, dimension_semantics=("arbitrary",))


def route_kernel(rows_dev, me_ref, ids_ref, slot_ref, req_ref, tok_ref, col_a, col_b):
    n_tok = ids_ref.shape[1]
    tok_bits = n_tok.bit_length() - 1
    me = me_ref[0]
    big = jnp.int32(2**30)
    high, low = 65536, 65535

    def fill(col, row):
        for c in range(n_tok // LANES):
            part = jnp.broadcast_to(row[:, c * LANES:(c + 1) * LANES], (LANES, LANES))
            col[c * LANES:(c + 1) * LANES, :] = part.T

    ids = ids_ref[...]
    tok = lax.broadcasted_iota(jnp.int32, (1, n_tok), 1)
    fill(col_a, ids)
    wide = (8, LANES)
    unroll = 4

    def sweep(n_out, width, rows_of, steps):
        groups = width // LANES
        outs = []
        for g in range(n_out // width):
            rows = [rows_of(g * width + c * LANES) for c in range(groups)]
            accs = tuple(jnp.zeros(wide, jnp.int32) for _ in range(groups))
            for begin, end, step in steps(g):
                def body(i, accs, rows=rows, step=step):
                    for u in range(unroll):
                        accs = step(i * unroll + u, accs, rows)
                    return accs

                accs = lax.fori_loop(begin // (8 * unroll), end // (8 * unroll), body, accs)
            outs.extend(accs)
        return jnp.concatenate([jnp.sum(r, axis=0, keepdims=True) for r in outs], axis=1)

    def id_row(lane0):
        return jnp.broadcast_to(ids_ref[:, lane0:lane0 + LANES], wide)

    def block(i):
        return pl.ds(pl.multiple_of(i * 8, 8), 8)

    def same_steps(g):
        def step(i, accs, rows, weight):
            col = col_a[block(i), :]
            return tuple(acc + jnp.where(col == row, weight(i, c), 0) for c, (acc, row) in enumerate(zip(accs, rows)))

        def mixed(i, c):
            pos = i * 8 + lax.broadcasted_iota(jnp.int32, wide, 0)
            at = g * 1024 + c * LANES + lax.broadcasted_iota(jnp.int32, wide, 1)
            return jnp.where(pos < at, high + 1, 1)

        before = functools.partial(step, weight=lambda i, c: high + 1)
        after = functools.partial(step, weight=lambda i, c: 1)
        lo, hi = g * 1024, (g + 1) * 1024
        return [(0, lo, before), (lo, hi, functools.partial(step, weight=mixed)), (hi, n_tok, after)]

    same = sweep(n_tok, 1024, id_row, same_steps)
    first = same < high
    many = (same & low) > 1
    key = jnp.where(first, ids, big)
    count = jnp.where(many, 1, high)
    fill(col_a, count)
    fill(col_b, key)

    def rank_step(i, accs, rows):
        col, num = col_b[block(i), :], col_a[block(i), :]
        return tuple(acc + jnp.where(col < row, num, 0) for acc, row in zip(accs, rows))

    below = sweep(n_tok, 1024, id_row, lambda g: [(0, n_tok, rank_step)])
    owner = jnp.zeros_like(ids)
    start = jnp.zeros_like(ids)
    prev = jnp.zeros((1, 1), jnp.int32)
    over = jnp.zeros((1, 1), jnp.int32)
    for o in range(1, N_DEV + 1):
        base = jnp.sum(jnp.where(key < o * rows_dev, count, 0), axis=1, keepdims=True)
        held = base - prev
        full = jnp.logical_or((held >> 16) > CAP_ONE, (held & low) > CAP_MANY)
        over = jnp.where(full, 1, over)
        prev = base
        if o < N_DEV:
            past = ids >= o * rows_dev
            owner = jnp.where(past, o, owner)
            start = jnp.where(past, base, start)
    rank = below - start
    place = jnp.where(many, rank & low, CAP_MANY + (rank >> 16))
    fits = place < jnp.where(many, CAP_MANY, CAP)
    slot = (owner ^ me) * CAP + jnp.where(fits, place, 0)
    slot_ref[...] = slot
    fill(col_b, jnp.where(jnp.logical_and(first, fits), slot, -1))
    fill(col_a, (ids - owner * rows_dev) * n_tok + tok + 1)

    def req_step(i, accs, rows):
        col, val = col_b[block(i), :], col_a[block(i), :]
        return tuple(acc + jnp.where(col == row, val, 0) for acc, row in zip(accs, rows))

    lanes = lax.broadcasted_iota(jnp.int32, wide, 1)
    code = sweep(N_SLOT, 1664, lambda lane0: lane0 + lanes, lambda g: [(0, n_tok, req_step)])
    used = code > 0
    req = jnp.where(used, (code - 1) >> tok_bits, rows_dev)
    tok_ref[...] = jnp.where(used, (code - 1) & (n_tok - 1), 0)
    for k in range(N_DEV):
        req_ref[k:k + 1, :CAP] = req[:, k * CAP:(k + 1) * CAP]
        req_ref[k:k + 1, CAP:] = jnp.broadcast_to(over, (1, REQ_COLS - CAP))


def route(ids, rows_dev):
    n_tok = ids.shape[0]
    me = lax.axis_index(AXIS_NAME).astype(jnp.int32).reshape(1)
    vmem = pl.BlockSpec(memory_space=pltpu.VMEM)
    return pl.pallas_call(
        functools.partial(route_kernel, rows_dev),
        out_shape=(
            jax.ShapeDtypeStruct((1, n_tok), jnp.int32), jax.ShapeDtypeStruct((N_DEV, REQ_COLS), jnp.int32),
            jax.ShapeDtypeStruct((1, N_SLOT), jnp.int32)),
        in_specs=[pl.BlockSpec(memory_space=pltpu.SMEM), vmem],
        out_specs=(vmem, vmem, vmem),
        scratch_shapes=[pltpu.VMEM((n_tok, LANES), jnp.int32)] * 2,
        compiler_params=pltpu.CompilerParams(vmem_limit_bytes=16 * 1024 * 1024),
        name="route",
    )(me, ids.reshape(1, n_tok))


def swap(parts):
    out = [parts[0]]
    far = {k: lax.ppermute(parts[k], AXIS_NAME, [(i, i ^ k) for i in range(N_DEV)]) for k in range(N_DEV - 1, 0, -1)}
    return out + [far[k] for k in range(1, N_DEV)]


TILES = WIDE // LANES
ROW_UNROLL = 16
GATHER_CHUNK = 768


def strip(row0, n_rows, c):
    return pl.ds(row0 * TILES + c, n_rows, stride=TILES)


def row(r):
    return pl.ds(pl.multiple_of(r * TILES, TILES), TILES)


def to_rows(dst, row0, src, n_rows, dim):
    for c in range(TILES):
        n_lane = max(0, min(LANES, dim - c * LANES))
        part = src(c * LANES, n_lane).astype(F32)
        if n_lane < LANES:
            part = jnp.concatenate([part, jnp.zeros((n_rows, LANES - n_lane), F32)], axis=1)
        dst[strip(row0, n_rows, c), :] = part


def copy_rows(src, idx_ref, idx0, dst, n_rows):
    def body(i, carry):
        vals = [src[row(idx_ref[idx0 + i * ROW_UNROLL + u]), :] for u in range(ROW_UNROLL)]
        for u in range(ROW_UNROLL):
            dst[row(i * ROW_UNROLL + u), :] = vals[u]
        return carry

    lax.fori_loop(0, n_rows // ROW_UNROLL, body, 0)


def pick_kernel(idx_ref, tab_ref, *refs):
    outs, rows, stage = refs[:N_DEV], refs[N_DEV], refs[N_DEV + 1]
    step = pl.program_id(0)
    dim, n_rows = tab_ref.shape[0], rows.shape[0] // TILES
    n_load = n_rows // GATHER_CHUNK

    @pl.when(step < n_load)
    def _():
        for c in range(TILES):
            part = tab_ref[c * LANES:min((c + 1) * LANES, dim), :].astype(F32)
            if part.shape[0] < LANES:
                part = jnp.concatenate([part, jnp.zeros((LANES - part.shape[0], GATHER_CHUNK), F32)], axis=0)
            rows[strip(step * GATHER_CHUNK, GATHER_CHUNK, c), :] = part.T

    for k in range(N_DEV):
        @pl.when(step == n_load + k)
        def _(k=k):
            copy_rows(rows, idx_ref, k * CAP, stage, CAP)
            for c in range(TILES):
                outs[k][:, c * LANES:(c + 1) * LANES] = stage[strip(0, CAP, c), :].astype(BF)


def pick_rows(table, idx):
    rows_dev, dim = table.shape
    n_load = rows_dev // GATHER_CHUNK
    idx = jnp.minimum(idx.reshape(-1), rows_dev - 1)
    return pl.pallas_call(
        pick_kernel,
        grid_spec=pltpu.PrefetchScalarGridSpec(
            num_scalar_prefetch=1,
            grid=(n_load + N_DEV,),
            in_specs=[pl.BlockSpec((dim, GATHER_CHUNK), lambda s, _: (0, jnp.minimum(s, n_load - 1)))],
            out_specs=[pl.BlockSpec((CAP, WIDE), lambda s, _: (0, 0))] * N_DEV,
            scratch_shapes=[pltpu.VMEM((rows_dev * TILES, LANES), F32), pltpu.VMEM((CAP * TILES, LANES), F32)],
        ),
        out_shape=[jax.ShapeDtypeStruct((CAP, WIDE), BF)] * N_DEV,
        compiler_params=params(),
        cost_estimate=pl.CostEstimate(flops=10**9, bytes_accessed=2 * rows_dev * dim, transcendentals=0),
        name="pick_rows",
    )(idx, table.T)


EXPAND_ROWS = 512


def expand_kernel(idx_ref, gain_ref, *refs):
    parts, e_ref, h_ref, rows, stage = refs[:N_DEV], *refs[N_DEV:]
    step = pl.program_id(0)
    dim = e_ref.shape[1]

    @pl.when(step == 0)
    def _():
        for k in range(N_DEV):
            to_rows(rows, k * CAP, lambda at, n, k=k: parts[k][:, at:at + n], CAP, WIDE)

    copy_rows(rows, idx_ref, step * EXPAND_ROWS, stage, EXPAND_ROWS)
    x = jnp.concatenate([stage[strip(0, EXPAND_ROWS, c), :] for c in range(TILES)], axis=1)[:, :dim]
    e_ref[...] = x.astype(BF)
    inv = lax.rsqrt(jnp.mean(x * x, axis=-1, keepdims=True) + NORM_EPS)
    h_ref[...] = (x * inv * gain_ref[...]).astype(BF)


def expand_rows(parts, slot, gain):
    n_tok, dim = slot.shape[0], gain.shape[0]
    return pl.pallas_call(
        expand_kernel,
        grid_spec=pltpu.PrefetchScalarGridSpec(
            num_scalar_prefetch=1,
            grid=(n_tok // EXPAND_ROWS,),
            in_specs=[pl.BlockSpec((1, dim), lambda s, _: (0, 0))] + [pl.BlockSpec((CAP, WIDE), lambda s, _: (0, 0))] * N_DEV,
            out_specs=[pl.BlockSpec((EXPAND_ROWS, dim), lambda s, _: (s, 0))] * 2,
            scratch_shapes=[pltpu.VMEM((N_SLOT * TILES, LANES), F32), pltpu.VMEM((EXPAND_ROWS * TILES, LANES), F32)],
        ),
        out_shape=[jax.ShapeDtypeStruct((n_tok, dim), BF)] * 2,
        compiler_params=params(),
        name="expand_rows",
    )(slot, gain.reshape(1, dim), *parts)


def fold_kernel(tok_ref, slot_ref, d_ref, *refs):
    many, ones, rows, stage = refs[:N_DEV], refs[N_DEV:2 * N_DEV], refs[2 * N_DEV], refs[2 * N_DEV + 1]
    n_tok, dim = d_ref.shape
    step = pl.program_id(0)
    half = N_DEV // 2
    width = 1024
    chunk = 512

    @pl.when(step == 0)
    def _():
        for b in range(n_tok // chunk):
            to_rows(rows, b * chunk, lambda at, n, b=b: d_ref[b * chunk:(b + 1) * chunk, at:at + n], chunk, dim)

    for part in range(2):
        @pl.when(step == part)
        def _(part=part):
            total = None
            for c in range(n_tok // width):
                hot = []
                for k in range(part * half, (part + 1) * half):
                    ids = jnp.broadcast_to(slot_ref[:, c * width:(c + 1) * width], (CAP_MANY, width))
                    mine = k * CAP + lax.broadcasted_iota(jnp.int32, (CAP_MANY, width), 0)
                    hot.append(jnp.where(ids == mine, 1.0, 0.0).astype(BF))
                term = jnp.dot(jnp.concatenate(hot, axis=0), d_ref[c * width:(c + 1) * width, :], preferred_element_type=F32)
                total = term if total is None else total + term
            for j in range(half):
                out = many[part * half + j]
                out[:, :dim] = total[j * CAP_MANY:(j + 1) * CAP_MANY]
                out[:, dim:] = jnp.zeros((CAP_MANY, WIDE - dim), F32)

    for k in range(N_DEV):
        @pl.when(step == 2 + k)
        def _(k=k):
            copy_rows(rows, tok_ref, k * CAP + CAP_MANY, stage, CAP_ONE)
            for c in range(TILES):
                ones[k][:, c * LANES:(c + 1) * LANES] = stage[strip(0, CAP_ONE, c), :].astype(BF)


def fold_rows(d_emb, slot, tok):
    n_tok, dim = d_emb.shape
    out = pl.pallas_call(
        fold_kernel,
        grid_spec=pltpu.PrefetchScalarGridSpec(
            num_scalar_prefetch=1,
            grid=(2 + N_DEV,),
            in_specs=[pl.BlockSpec((1, n_tok), lambda s, _: (0, 0)), pl.BlockSpec((n_tok, dim), lambda s, _: (0, 0))],
            out_specs=[pl.BlockSpec((CAP_MANY, WIDE), lambda s, _: (0, 0))] * N_DEV + [pl.BlockSpec((CAP_ONE, WIDE), lambda s, _: (0, 0))] * N_DEV,
            scratch_shapes=[pltpu.VMEM((n_tok * TILES, LANES), F32), pltpu.VMEM((CAP_ONE * TILES, LANES), F32)],
        ),
        out_shape=[jax.ShapeDtypeStruct((CAP_MANY, WIDE), F32)] * N_DEV + [jax.ShapeDtypeStruct((CAP_ONE, WIDE), BF)] * N_DEV,
        compiler_params=params(),
        cost_estimate=pl.CostEstimate(flops=2 * N_DEV * CAP_MANY * n_tok * dim, bytes_accessed=4 * N_SLOT * dim, transcendentals=0),
        name="fold_rows",
    )(tok.reshape(-1), slot, d_emb)
    return out[:N_DEV], out[N_DEV:]


ADD_UNROLL = 8


def spread_kernel(rows_dev, idx_ref, *refs):
    many, ones, out_ref, total, stage = refs[:N_DEV], refs[N_DEV:2 * N_DEV], *refs[2 * N_DEV:]
    step = pl.program_id(0)

    @pl.when(step == 0)
    def _():
        total[...] = jnp.zeros_like(total)

    for k in range(N_DEV):
        @pl.when(step == k)
        def _(k=k):
            to_rows(stage, 0, lambda at, n: many[k][:, at:at + n], CAP_MANY, WIDE)
            to_rows(stage, CAP_MANY, lambda at, n: ones[k][:, at:at + n], CAP_ONE, WIDE)

            def body(i, carry):
                rows = [idx_ref[k * CAP + i * ADD_UNROLL + u] for u in range(ADD_UNROLL)]
                sums = [total[row(rows[u]), :] + stage[row(i * ADD_UNROLL + u), :] for u in range(ADD_UNROLL)]
                for u in range(ADD_UNROLL):
                    total[row(rows[u]), :] = sums[u]
                return carry

            lax.fori_loop(0, CAP // ADD_UNROLL, body, 0)

    @pl.when(step >= N_DEV)
    def _():
        at = (step - N_DEV) * GATHER_CHUNK
        dim = out_ref.shape[0]
        for c in range(TILES):
            n_lane = min(LANES, dim - c * LANES)
            part = total[strip(at, GATHER_CHUNK, c), :].T
            out_ref[c * LANES:c * LANES + n_lane, :] = part[:n_lane].astype(BF)


def spread_rows(many, ones, idx, rows_dev, dim):
    n_out = rows_dev // GATHER_CHUNK
    return pl.pallas_call(
        functools.partial(spread_kernel, rows_dev),
        grid_spec=pltpu.PrefetchScalarGridSpec(
            num_scalar_prefetch=1,
            grid=(N_DEV + n_out,),
            in_specs=[pl.BlockSpec((CAP_MANY, WIDE), lambda s, _: (0, 0))] * N_DEV + [pl.BlockSpec((CAP_ONE, WIDE), lambda s, _: (0, 0))] * N_DEV,
            out_specs=pl.BlockSpec((dim, GATHER_CHUNK), lambda s, _: (0, jnp.maximum(s - N_DEV, 0))),
            scratch_shapes=[pltpu.VMEM(((rows_dev + 8) * TILES, LANES), F32), pltpu.VMEM((CAP * TILES, LANES), F32)],
        ),
        out_shape=jax.ShapeDtypeStruct((dim, rows_dev), BF),
        compiler_params=params(),
        name="spread_rows",
    )(idx.reshape(-1), *many, *ones).T


def rope_tables(seq_len):
    half = HEAD_DIM // 2
    inv_freq = ROPE_THETA ** (-2.0 * jnp.arange(half, dtype=F32) / HEAD_DIM)
    angles = jnp.arange(seq_len, dtype=F32)[:, None] * inv_freq[None, :]
    cos_tab, sin_tab = jnp.cos(angles), jnp.sin(angles)
    cos_all = jnp.concatenate([cos_tab] * 4, axis=1)
    sin_all = jnp.concatenate([-sin_tab, sin_tab] * 2, axis=1)
    return cos_all, sin_all


def turn(x, cos_all, sin_all, low):
    other = jnp.where(low, pltpu.roll(x, LANES - HEAD_DIM // 2, 1), pltpu.roll(x, HEAD_DIM // 2, 1))
    return x * cos_all + other * sin_all


def low_lanes(seq_len):
    lane = lax.broadcasted_iota(jnp.int32, (seq_len, LANES), 1)
    return lax.rem(lane, HEAD_DIM) < HEAD_DIM // 2


CONTRACT_LAST = (((1,), (1,)), ((), ()))
CONTRACT_FIRST = (((0,), (0,)), ((), ()))


def lanes_of(ref, at, first_head):
    return jnp.concatenate([ref[at, h * HEAD_DIM:(h + 1) * HEAD_DIM] for h in range(first_head, first_head + 3)], axis=0)


def hidden(half):
    key = lax.broadcasted_iota(jnp.int32, (half, 3 * half), 0)
    query = lax.rem(lax.broadcasted_iota(jnp.int32, (half, 3 * half), 1), half)
    return key > query


def dot_last(a, b):
    return lax.dot_general(a, b, CONTRACT_LAST, preferred_element_type=F32)


def dot_first(a, b):
    return lax.dot_general(a, b, CONTRACT_FIRST, preferred_element_type=F32)


def dot_mid(a, b):
    return jnp.dot(a, b, preferred_element_type=F32)


def scores(q_lo, q_hi, k):
    half = k.shape[0] // 2
    return dot_last(k[:half], jnp.concatenate([q_lo, q_hi], axis=0)), dot_last(k[half:], q_hi)


def probabilities(s_all, s_c, mask):
    n_lo = s_c.shape[1]
    s_a = jnp.where(mask, -1e30, s_all[:, :n_lo])
    s_b = s_all[:, n_lo:]
    s_c = jnp.where(mask, -1e30, s_c)
    m_lo = jnp.max(s_a, axis=0, keepdims=True)
    m_hi = jnp.maximum(jnp.max(s_b, axis=0, keepdims=True), jnp.max(s_c, axis=0, keepdims=True))
    p_a, p_b, p_c = jnp.exp(s_a - m_lo), jnp.exp(s_b - m_hi), jnp.exp(s_c - m_hi)
    inv_lo = 1.0 / jnp.sum(p_a, axis=0, keepdims=True)
    inv_hi = 1.0 / (jnp.sum(p_b, axis=0, keepdims=True) + jnp.sum(p_c, axis=0, keepdims=True))
    return p_a * inv_lo, p_b * inv_hi, p_c * inv_hi


def group_keys(rot_ref, g):
    k0, v0 = (Q_HEADS + g) * HEAD_DIM, QK_COLS + g * HEAD_DIM
    return rot_ref[:, k0:k0 + HEAD_DIM], rot_ref[:, v0:v0 + HEAD_DIM]


def attend_kernel(cos_ref, sin_ref, h_ref, x_ref, pack_ref, wo_ref, gain_ref, rot_ref, out_ref, res_ref, h_two_ref, inv_ref, qkv):
    seq_len = h_ref.shape[0]
    low = low_lanes(seq_len)
    cos_all, sin_all = cos_ref[...], sin_ref[...]
    scale_q = Q_HEADS * HEAD_DIM
    qkv[...] = dot_mid(h_ref[...], pack_ref[...])
    for c in range(QK_COLS // LANES):
        x = turn(qkv[:, c * LANES:(c + 1) * LANES], cos_all, sin_all, low)
        col = c * LANES + lax.broadcasted_iota(jnp.int32, x.shape, 1)
        if (c + 1) * LANES <= scale_q:
            x = x * HEAD_DIM ** -0.5
        elif c * LANES < scale_q:
            x = jnp.where(col < scale_q, x * HEAD_DIM ** -0.5, x)
        rot_ref[:, c * LANES:(c + 1) * LANES] = x.astype(BF)
    rot_ref[:, QK_COLS:] = qkv[:, QK_COLS:QKV_COLS].astype(BF)
    half = seq_len // 2
    lo, hi = slice(0, half), slice(half, seq_len)
    mask = hidden(half)

    def products(g):
        k, v = group_keys(rot_ref, g)
        return v, scores(lanes_of(rot_ref, lo, 3 * g), lanes_of(rot_ref, hi, 3 * g), k)

    ahead = products(0)
    for g in range(KV_HEADS):
        v, (s_all, s_c) = ahead
        if g + 1 < KV_HEADS:
            ahead = products(g + 1)
        p_a, p_b, p_c = probabilities(s_all, s_c, mask)
        o_lo = dot_first(p_a.astype(BF), v[lo]).astype(BF)
        o_hi = dot_first(jnp.concatenate([p_b.astype(BF), p_c.astype(BF)], axis=0), v).astype(BF)
        for j in range(3):
            h = 3 * g + j
            out_ref[lo, h * HEAD_DIM:(h + 1) * HEAD_DIM] = o_lo[j * half:(j + 1) * half]
            out_ref[hi, h * HEAD_DIM:(h + 1) * HEAD_DIM] = o_hi[j * half:(j + 1) * half]
    s = (x_ref[...].astype(F32) + dot_mid(out_ref[...], wo_ref[...])).astype(BF).astype(F32)
    h_two_ref[...] = (s * lax.rsqrt(jnp.mean(s * s, axis=-1, keepdims=True) + NORM_EPS) * gain_ref[...]).astype(BF)
    s = s.T
    res_ref[0] = s.astype(BF)
    inv_ref[0] = lax.rsqrt(jnp.mean(s * s, axis=0, keepdims=True) + NORM_EPS)


def whole(shape):
    return pl.BlockSpec(shape, lambda s: (0,) * len(shape))


def by_seq(shape):
    return pl.BlockSpec(shape, lambda s: (s,) + (0,) * (len(shape) - 1))


def attend(h_one, emb, full_pack, full_out, gain_two, seq_len, tables):
    n_tok, dim = emb.shape
    batch = n_tok // seq_len
    cube = (1, dim, seq_len)
    return pl.pallas_call(
        attend_kernel,
        grid=(batch,),
        in_specs=[whole((seq_len, LANES))] * 2 + [by_seq((seq_len, dim))] * 2 + [whole(full_pack.shape), whole(full_out.shape), whole((1, dim))],
        out_specs=[by_seq((seq_len, QKV_COLS)), by_seq((seq_len, dim)), by_seq(cube), by_seq((seq_len, dim)), by_seq((1, 1, seq_len))],
        out_shape=[
            jax.ShapeDtypeStruct((n_tok, QKV_COLS), BF), jax.ShapeDtypeStruct((n_tok, dim), BF),
            jax.ShapeDtypeStruct((batch, dim, seq_len), BF), jax.ShapeDtypeStruct((n_tok, dim), BF),
            jax.ShapeDtypeStruct((batch, 1, seq_len), F32),
        ],
        scratch_shapes=[pltpu.VMEM((seq_len, PACK_COLS), F32)],
        compiler_params=params(40 * 1024 * 1024),
        cost_estimate=pl.CostEstimate(
            flops=4 * n_tok * seq_len * dim + 2 * n_tok * dim * (PACK_COLS + dim), bytes_accessed=14 * n_tok * dim,
            transcendentals=n_tok * seq_len * Q_HEADS),
        name="attend",
    )(*tables, h_one, emb, full_pack, full_out, gain_two.reshape(1, dim))


def attend_back_kernel(cos_ref, sin_ref, rot_ref, d_res_ref, x_ref, pack_ref, wo_ref, gain_ref, out_ref, d_x_ref, d_gain_ref, d_rot, d_ref):
    seq_len = rot_ref.shape[0]
    d_resid = d_res_ref[0].astype(F32).T
    d_ref[...] = dot_last(d_resid.astype(BF), wo_ref[...]).astype(BF)
    scale_q = Q_HEADS * HEAD_DIM
    half = seq_len // 2
    lo, hi = slice(0, half), slice(half, seq_len)
    mask = hidden(half)

    def products(g):
        k, v = group_keys(rot_ref, g)
        q_lo, q_hi = lanes_of(rot_ref, lo, 3 * g), lanes_of(rot_ref, hi, 3 * g)
        d_lo, d_hi = lanes_of(d_ref, lo, 3 * g), lanes_of(d_ref, hi, 3 * g)
        return k, q_lo, q_hi, d_lo, d_hi, scores(q_lo, q_hi, k), scores(d_lo, d_hi, v)

    ahead = products(0)
    for g in range(KV_HEADS):
        k0, v0 = scale_q + g * HEAD_DIM, QK_COLS + g * HEAD_DIM
        k, q_lo, q_hi, d_lo, d_hi, (s_all, s_c), (dp_all, dp_c) = ahead
        if g + 1 < KV_HEADS:
            ahead = products(g + 1)
        n_lo = q_lo.shape[0]
        p_a, p_b, p_c = probabilities(s_all, s_c, mask)
        d_all = jnp.concatenate([d_lo, d_hi], axis=0)
        dp_all, dp_c = dp_all.astype(BF).astype(F32), dp_c.astype(BF).astype(F32)
        p_lo = jnp.concatenate([p_a.astype(BF), p_b.astype(BF)], axis=1)
        out_ref[lo, v0:v0 + HEAD_DIM] = dot_mid(p_lo, d_all).astype(BF)
        out_ref[hi, v0:v0 + HEAD_DIM] = dot_mid(p_c.astype(BF), d_hi).astype(BF)
        pd_a, pd_b, pd_c = p_a * dp_all[:, :n_lo], p_b * dp_all[:, n_lo:], p_c * dp_c
        t_lo = jnp.sum(pd_a, axis=0, keepdims=True)
        t_hi = jnp.sum(pd_b, axis=0, keepdims=True) + jnp.sum(pd_c, axis=0, keepdims=True)
        ds_a = (pd_a - p_a * t_lo).astype(BF)
        ds_b = (pd_b - p_b * t_hi).astype(BF)
        ds_c = (pd_c - p_c * t_hi).astype(BF)
        q_all = jnp.concatenate([q_lo, q_hi], axis=0)
        ds_all = jnp.concatenate([ds_a, ds_b], axis=1)
        d_rot[lo, k0:k0 + HEAD_DIM] = dot_mid(ds_all, q_all).astype(BF).astype(F32)
        d_rot[hi, k0:k0 + HEAD_DIM] = dot_mid(ds_c, q_hi).astype(BF).astype(F32)
        scale = HEAD_DIM ** -0.5
        dq_lo = (dot_first(ds_a, k[lo]) * scale).astype(BF).astype(F32)
        dq_hi = (dot_first(jnp.concatenate([ds_b, ds_c], axis=0), k) * scale).astype(BF).astype(F32)
        for j in range(3):
            h = 3 * g + j
            d_rot[lo, h * HEAD_DIM:(h + 1) * HEAD_DIM] = dq_lo[j * half:(j + 1) * half]
            d_rot[hi, h * HEAD_DIM:(h + 1) * HEAD_DIM] = dq_hi[j * half:(j + 1) * half]
    out_ref[:, QKV_COLS:] = jnp.zeros((seq_len, PACK_COLS - QKV_COLS), BF)
    low = low_lanes(seq_len)
    cos_all, sin_all = cos_ref[...], -sin_ref[...]
    for c in range(QK_COLS // LANES):
        at = slice(c * LANES, (c + 1) * LANES)
        out_ref[:, at] = turn(d_rot[:, at], cos_all, sin_all, low).astype(BF)
    d_h = dot_last(out_ref[...], pack_ref[...]).astype(BF).astype(F32)
    x = x_ref[...].astype(F32)
    inv = lax.rsqrt(jnp.mean(x * x, axis=-1, keepdims=True) + NORM_EPS)
    d_n = d_h * gain_ref[...]
    pull = jnp.mean(d_n * x, axis=-1, keepdims=True) * (inv * inv * inv)
    d_x_ref[...] = (d_resid + (d_n * inv - x * pull)).astype(BF)
    d_gain = jnp.sum(d_h * (x * inv), axis=0, keepdims=True)

    @pl.when(pl.program_id(0) == 0)
    def _():
        d_gain_ref[...] = jnp.zeros_like(d_gain_ref)

    d_gain_ref[...] += d_gain


def attend_back(rot, d_resid, emb, full_pack, full_out, gain_one, seq_len, tables):
    n_tok, dim = emb.shape
    return pl.pallas_call(
        attend_back_kernel,
        grid=(n_tok // seq_len,),
        in_specs=[whole((seq_len, LANES))] * 2
        + [by_seq((seq_len, QKV_COLS)), by_seq((1, dim, seq_len)), by_seq((seq_len, dim))]
        + [whole(full_pack.shape), whole(full_out.shape), whole((1, dim))],
        out_specs=[by_seq((seq_len, PACK_COLS)), by_seq((seq_len, dim)), whole((1, dim))],
        out_shape=[jax.ShapeDtypeStruct((n_tok, PACK_COLS), BF), jax.ShapeDtypeStruct((n_tok, dim), BF), jax.ShapeDtypeStruct((1, dim), F32)],
        scratch_shapes=[pltpu.VMEM((seq_len, QK_COLS), F32), pltpu.VMEM((seq_len, dim), BF)],
        compiler_params=params(40 * 1024 * 1024),
        cost_estimate=pl.CostEstimate(
            flops=10 * n_tok * seq_len * dim + 2 * n_tok * dim * (PACK_COLS + dim), bytes_accessed=14 * n_tok * dim,
            transcendentals=n_tok * seq_len * Q_HEADS),
        name="attend_back",
    )(*tables, rot, d_resid, emb, full_pack, full_out, gain_one.reshape(1, dim))


GATE_ROWS = 512
GATE_COLS = 256


def gate_kernel(h_ref, gate_ref, up_ref, d_act_ref, act_ref, d_gate_ref, d_up_ref):
    h = h_ref[...]
    for n in range(gate_ref.shape[1] // GATE_COLS):
        at = slice(n * GATE_COLS, (n + 1) * GATE_COLS)
        gate, up = dot_mid(h, gate_ref[:, at]), dot_mid(h, up_ref[:, at])
        d_act = d_act_ref[:, at].astype(F32)
        sig = jax.nn.sigmoid(gate)
        silu = gate * sig
        act_ref[:, at] = (silu * up).astype(BF)
        d_up_ref[:, at] = (d_act * silu).astype(BF)
        d_gate_ref[:, at] = (d_act * up * (sig + silu * (1.0 - sig))).astype(BF)


def gate_up(h_two, full_gate, full_up, d_act):
    n_tok, dim = h_two.shape
    ffn = full_gate.shape[1]
    tall = pl.BlockSpec((GATE_ROWS, ffn), lambda s: (s, 0))
    return pl.pallas_call(
        gate_kernel,
        grid=(n_tok // GATE_ROWS,),
        in_specs=[pl.BlockSpec((GATE_ROWS, dim), lambda s: (s, 0)), whole((dim, ffn)), whole((dim, ffn)), tall],
        out_specs=[tall] * 3,
        out_shape=[jax.ShapeDtypeStruct((n_tok, ffn), BF)] * 3,
        compiler_params=params(),
        cost_estimate=pl.CostEstimate(flops=4 * n_tok * dim * ffn, bytes_accessed=8 * n_tok * ffn, transcendentals=2 * n_tok * ffn),
        name="gate_up",
    )(h_two, full_gate, full_up, d_act)


def rms_norm(x_f32, gain_f32):
    inv_rms = lax.rsqrt(jnp.mean(x_f32 * x_f32, axis=-1, keepdims=True) + NORM_EPS)
    return (x_f32 * inv_rms * gain_f32).astype(BF)


def mm(a, b):
    return jnp.einsum("bsd,df->bsf", a, b, preferred_element_type=F32)


def mm_t(a, b):
    return jnp.einsum("bsf,df->bsd", a, b, preferred_element_type=F32)


def mm_w(a, b):
    return jnp.einsum("bsd,bsf->df", a, b, preferred_element_type=F32)


def row_major(x):
    return with_layout_constraint(x, Layout(major_to_minor=(0, 1)))


def from_peer(x, k):
    return lax.ppermute(x, AXIS_NAME, [(i, i ^ k) for i in range(N_DEV)]) if k else x


def owned_ids(token_ids, rows_dev, k):
    rel_ids = from_peer(token_ids, k).reshape(-1) - lax.axis_index(AXIS_NAME) * rows_dev
    return rel_ids, (rel_ids >= 0) & (rel_ids < rows_dev)


def slow_rows(token_ids, table):
    total = None
    for k in range(N_DEV):
        rel_ids, owned = owned_ids(token_ids, table.shape[0], k)
        picked = jnp.take(table, jnp.where(owned, rel_ids, 0), axis=0)
        part = from_peer(jnp.where(owned[:, None], picked, jnp.zeros((), BF)), k)
        total = part if total is None else total + part
    return total


def slow_grad(token_ids, d_emb, rows_dev):
    total = None
    for k in range(N_DEV):
        rel_ids, owned = owned_ids(token_ids, rows_dev, k)
        d_all = from_peer(d_emb, k).astype(F32)
        seg_ids = jnp.where(owned, rel_ids, rows_dev)
        part = jax.ops.segment_sum(d_all, seg_ids, num_segments=rows_dev)
        total = part if total is None else total + part
    return total.astype(BF)


def gather_all(shard):
    return lax.all_gather(shard, AXIS_NAME, axis=0, tiled=True)


def scatter_sum(partial):
    return lax.psum_scatter(partial, AXIS_NAME, scatter_dimension=0, tiled=True)


def solution(mesh):
    spec_1d = P(AXIS_NAME)
    spec_2d = P(AXIS_NAME, None)
    spec_3d = P(AXIS_NAME, None, None)
    in_specs = (spec_2d, spec_3d, spec_2d, spec_1d, spec_1d, spec_3d, spec_3d, spec_3d, spec_2d, spec_2d, spec_2d, spec_2d)
    out_specs = (spec_3d, spec_2d, spec_1d, spec_1d, spec_3d, spec_3d, spec_3d, spec_2d, spec_2d, spec_2d, spec_2d)

    def device_step(token_ids, grad_y, table, g_one, g_two, w_query, w_key, w_value, w_out, w_gate, w_up, w_down):
        rows_dev, dim = table.shape
        batch, seq_len = token_ids.shape
        n_tok = batch * seq_len
        rows_w = w_query.shape[0]

        pad = jnp.zeros((rows_w, PACK_COLS - QKV_COLS - 2), BF)
        shards = [w.reshape(rows_w, -1) for w in (w_query, w_key, w_value)]
        pack = jnp.concatenate(shards + [g_one[:, None], g_two[:, None], pad], axis=1)
        full_pack = gather_all(pack)
        full_down = gather_all(w_down)
        gain_one = full_pack[:, QKV_COLS].astype(F32)
        gain_two = full_pack[:, QKV_COLS + 1].astype(F32)

        slot, req, tok = route(token_ids.reshape(n_tok), rows_dev)
        asked = swap([req[k:k + 1] for k in range(N_DEV)])
        asked = jnp.concatenate(asked, axis=0)
        overflow = jnp.max(asked[:, CAP]) > 0
        asked = asked[:, :CAP]
        parts = swap(pick_rows(table, asked))
        d_act = mm_t(grad_y, full_down).astype(BF)
        parts, d_act, w_out, w_gate, w_up = lax.optimization_barrier((parts, d_act, w_out, w_gate, w_up))
        full_out = gather_all(w_out)
        full_gate = gather_all(w_gate)
        full_up = gather_all(w_up)

        def slow_start():
            rows = slow_rows(token_ids, table)
            return rows, rms_norm(rows.astype(F32), gain_one)

        emb, h_one = lax.cond(overflow, slow_start, lambda: tuple(expand_rows(parts, slot.reshape(n_tok), gain_one)))
        emb, h_one = row_major(emb), row_major(h_one)

        tables = rope_tables(seq_len)
        cube = (batch, seq_len, -1)
        rot, attn, resid_t, h_two, inv_t = attend(h_one, emb, full_pack, full_out, gain_two, seq_len, tables)
        attn = attn.reshape(cube)
        resid, inv_two = jnp.swapaxes(resid_t, 1, 2), jnp.swapaxes(inv_t, 1, 2)
        act, d_gate, d_up = (v.reshape(cube) for v in gate_up(h_two, full_gate, full_up, d_act.reshape(n_tok, -1)))
        h_two = h_two.reshape(cube)

        g_gate = mm_w(h_two, d_gate)
        act, d_up, g_gate = lax.optimization_barrier((act, d_up, g_gate))
        sum_gate = scatter_sum(g_gate)
        g_up, g_down = mm_w(h_two, d_up), mm_w(act, grad_y)
        d_gate, d_up, g_up, g_down = lax.optimization_barrier((d_gate, d_up, g_up, g_down))
        sum_up, sum_down = scatter_sum(g_up), scatter_sum(g_down)
        d_h_two = (mm_t(d_gate, full_gate) + mm_t(d_up, full_up)).astype(BF).astype(F32)
        resid_f32 = resid.astype(F32)
        d_n = d_h_two * gain_two
        pull = jnp.mean(d_n * resid_f32, axis=-1, keepdims=True) * (inv_two * inv_two * inv_two)
        d_gain_two = jnp.sum(d_h_two * (resid_f32 * inv_two), axis=(0, 1))
        d_resid = (grad_y.astype(F32) + (d_n * inv_two - resid_f32 * pull)).astype(BF)
        g_out = mm_w(attn, d_resid)
        d_resid, g_out, sum_gate = lax.optimization_barrier((d_resid, g_out, sum_gate))
        sum_out = scatter_sum(g_out)
        d_qkv, d_emb, d_gain_one = attend_back(rot, jnp.swapaxes(d_resid, 1, 2), emb, full_pack, full_out, gain_one, seq_len, tables)
        d_qkv, d_emb, sum_up, sum_down = lax.optimization_barrier((d_qkv, d_emb, sum_up, sum_down))

        g_pack = mm_w(h_one.reshape(cube), d_qkv.reshape(cube))
        gains = jnp.concatenate([d_gain_one.reshape(dim, 1), d_gain_two[:, None]], axis=1)
        g_pack = lax.dynamic_update_slice(g_pack, gains, (0, QKV_COLS))
        d_emb, slot, g_pack = lax.optimization_barrier((d_emb, slot, g_pack))
        sum_pack = scatter_sum(g_pack).astype(BF)

        many, ones = fold_rows(d_emb, slot, tok)
        act, resid, many, ones, sum_out = lax.optimization_barrier((act, resid, many, ones, sum_out))
        many, ones = swap(many), swap(ones)
        y_out = (resid.astype(F32) + mm(act, full_down)).astype(BF)
        d_table = spread_rows(many, ones, asked, rows_dev, dim)
        d_table, sum_pack, sum_out, sum_gate, sum_up, sum_down = lax.optimization_barrier(
            (d_table, sum_pack, sum_out, sum_gate, sum_up, sum_down))
        d_table = lax.cond(overflow, lambda: slow_grad(token_ids, d_emb, rows_dev), lambda: d_table)

        cols = [0, Q_HEADS * HEAD_DIM, QK_COLS, QKV_COLS]
        d_w = [sum_pack[:, a:b].reshape(rows_w, -1, HEAD_DIM) for a, b in zip(cols[:-1], cols[1:])]
        return (
            y_out, d_table, sum_pack[:, QKV_COLS], sum_pack[:, QKV_COLS + 1],
            d_w[0], d_w[1], d_w[2], sum_out.astype(BF), sum_gate.astype(BF), sum_up.astype(BF), sum_down.astype(BF),
        )

    return jax.shard_map(device_step, mesh=mesh, in_specs=in_specs, out_specs=out_specs, check_vma=False)
```
